512 devices in a mesh: rep: 256 (over y_lo, x, z, core), slab: 2 (over y_hi).
Axes of the slice: x: 4, y: 8 (y_hi: 2, y_lo: 4; y = y_hi * 4 + y_lo), z: 8, core: 2. Of those that a mesh axis runs over, the one named last changes fastest.
Arguments:
- weights: bfloat16 [256, 256, 3072], P('rep', 'slab'), may hold values from -6 to 6
- perms: int32 [256, 8, 256], P('rep'), may hold values from 0 to 255, each once within a row
Outputs:
- merged: bfloat16 [256, 256, 3072], P('rep', 'slab')
The draws below stay inside these ranges and needn't reach their ends.
Inputs may be any that keep to these rules, and one draw needn't show every extreme that they name: `perms`: each row of 256 entries names every neuron of the window once.
All inputs are finite; a program needn't handle non-finite values.
Results may differ from the reference program's by a relative error of at most 0.012.
Values may be sent and summed in bfloat16 or wider, within the bound.
A program may use at most 64 MiB of HBM per device.

```python
import math
import jax
import jax.numpy as jnp
from jax import lax

D = 3072
ROUNDS = 8
FFW = 256
REPLICAS = 256
N_REP = 256


def shard_levels(own_key, dims, cuts, smallest, top_value):
    loudness = 1.0
    for axis_at, parts in cuts:
        heights = jax.random.uniform(jax.random.fold_in(jax.random.fold_in(own_key, 6), axis_at), (parts,), jnp.float32, smallest / len(cuts), top_value / len(cuts))
        loudness = loudness * jnp.repeat(jnp.exp(heights), dims[axis_at] // parts).reshape((-1,) + (1,) * (len(dims) - 1 - axis_at))
    return loudness


def gaussian(own_key, shape, deviation, bound, split=(), kind=jnp.bfloat16):
    array = deviation * jax.random.normal(own_key, shape, jnp.float32)
    if split:
        array = array * shard_levels(own_key, shape, split, -0.22, 0.18)
    return jnp.clip(array, -bound, bound).astype(kind)


def setup_inputs(seed: int = 0) -> dict:
    arg_keys = jax.random.split(jax.random.key(seed), 3)
    weights = gaussian(arg_keys[0], (REPLICAS, FFW, D), 1.0, 6.0, ((0, 256), (1, 2)))
    perms = jax.vmap(lambda own: jax.random.permutation(own, FFW))(jax.random.split(arg_keys[1], REPLICAS * ROUNDS)).reshape((REPLICAS, ROUNDS, FFW)).astype(jnp.int32)
    return dict(weights=weights, perms=perms)


def merge_one(own, partner, perm_row):
    cost = jnp.dot(own, partner.T, preferred_element_type=jnp.float32) * (1.0 / math.sqrt(D))
    squared = cost * cost
    fourth = squared * squared
    soft_plan = fourth / (1.0 + lax.optimization_barrier(jnp.sum(fourth, axis=1, keepdims=True)))
    columns = jnp.arange(partner.shape[0], dtype=jnp.int32)
    onehot = (perm_row[:, None] == columns[None, :]).astype(jnp.float32)
    mixing = (onehot + soft_plan).astype(jnp.bfloat16)
    aligned = 0.5 * jnp.dot(mixing, partner, preferred_element_type=jnp.float32)
    return ((own.astype(jnp.float32) + aligned) * (1.0 / math.sqrt(2.0))).astype(jnp.bfloat16)

def reference(weights, perms):
    bit_count = N_REP.bit_length() - 1
    current = weights
    for round_idx in range(ROUNDS):
        flip = 1 << round_idx % bit_count
        partner_idx = jnp.bitwise_xor(jnp.arange(REPLICAS, dtype=jnp.int32), flip)
        partner = current[partner_idx]
        current = jax.vmap(merge_one)(current, partner, perms[:, round_idx])
    return current
```

```python
import functools
import math

import jax
import jax.numpy as jnp
from jax import lax
from jax.experimental import pallas as pl
from jax.experimental.pallas import tpu as pltpu
from jax.sharding import PartitionSpec as P

D = 3072
N = 256
H = N // 2
F = D // 2
MESH = pl.DeviceIdType.MESH
NEAR, Z0, Z1, Z2, X0, X1, Y0, Y1 = range(8)


def layout(counts):
    at, out = 0, {}
    for name, count in counts:
        out[name] = at
        at += count
    return out, at


SEM, N_SEM = layout([
    ("near_raw", 1), ("in", 16), ("z_raw", 2), ("z_fwd", 16), ("perm", 8),
    ("p2", 4), ("p3z", 8), ("p3x", 4), ("p3f", 8),
    ("p4x", 4), ("p4y", 4), ("p4fx", 2), ("p4fy", 2), ("p5", 4), ("out", 2),
    ("cost", 11 * 4),
])


def kernel(w_hbm, p_ref, o_ref, wv, perms, raw, first, cur, got, mine_g, near_g, mix, ssem, rsem, lsem):
    rep, h = lax.axis_index("rep"), lax.axis_index("slab")
    g = rep % 2
    far = 1 - h

    def flip(bit):
        return rep + (1 << bit) * (1 - 2 * ((rep // (1 << bit)) % 2))

    def core(base, c):
        return base - g + c

    def xor(a, b):
        return a + b - 2 * a * b

    near = (flip(0), h)
    chip = [flip(b) for b in range(8)]
    same = [(chip[b], h) for b in range(8)]

    load = pltpu.make_async_copy(w_hbm.at[0], wv, lsem.at[0])
    load.start()

    peers = [near] + [same[b] for b in (Z1, Z2, X1, Y1)]
    for c in range(2):
        peers.append((core(rep, c), far))
        for b in (Z0, X0, Y0):
            peers.append((core(chip[b], c), h))
    barrier = pltpu.get_barrier_semaphore()
    for peer in peers:
        pl.semaphore_signal(barrier, inc=1, device_id=peer, device_id_type=MESH)
    pl.semaphore_wait(barrier, len(peers))

    sent = []

    def send(src, dst, sem, device):
        copy = pltpu.make_async_remote_copy(
            src_ref=src, dst_ref=dst, send_sem=ssem.at[sem], recv_sem=rsem.at[sem],
            device_id=device, device_id_type=MESH,
        )
        copy.start()
        sent.append(copy)

    def arrived(dst, sem):
        pltpu.make_async_remote_copy(
            src_ref=dst, dst_ref=dst, send_sem=ssem.at[0], recv_sem=rsem.at[sem],
            device_id=near, device_id_type=MESH,
        ).wait_recv()

    def half(c):
        return pl.ds(c * F, F)

    slot, far_slot = xor(g, h), xor(g, far)
    my_rows, far_rows = h * H, far * H
    step = H // 8

    load.wait()
    keep = pltpu.make_async_copy(
        wv.at[:, pl.ds(pl.multiple_of(g * F, F), F)],
        raw.at[0, slot, pl.ds(pl.multiple_of(my_rows, H), H)], lsem.at[1])
    keep.start()

    def send_in(q, c):
        src = wv.at[pl.ds(q * step, step), half(c)]
        dst = raw.at[0, far_slot, pl.ds(pl.multiple_of(my_rows + q * step, step), step)]
        copy = pltpu.make_async_remote_copy(
            src_ref=src, dst_ref=dst, send_sem=ssem.at[SEM["in"] + q * 2 + c],
            recv_sem=rsem.at[SEM["in"] + q * 2 + far_slot],
            device_id=(core(rep, c), far), device_id_type=MESH)
        copy.start()
        sent.append(copy)

    for q in range(8):
        for c in range(2):
            send_in(q, c)
    for c in range(2):
        copy = pltpu.make_async_remote_copy(
            src_ref=wv.at[:, half(c)],
            dst_ref=raw.at[1, slot, pl.ds(pl.multiple_of(my_rows, H), H)],
            send_sem=ssem.at[SEM["z_raw"] + c], recv_sem=rsem.at[SEM["z_raw"] + slot],
            device_id=(core(chip[Z0], c), h), device_id_type=MESH)
        copy.start()
        sent.append(copy)
    send(wv.at[:, pl.ds(pl.multiple_of((1 - g) * F, F), F)],
         raw.at[0, slot, pl.ds(pl.multiple_of(my_rows, H), H)], SEM["near_raw"], near)

    perms[0, slot] = p_ref[0]
    perm_to = [(0, near, 0)]
    for at, b in ((1, Z0), (2, X0), (3, Y0)):
        for c in range(2):
            perm_to.append((at, (core(chip[b], c), h), c))
    for at, device, c in perm_to:
        copy = pltpu.make_async_remote_copy(
            src_ref=p_ref.at[0], dst_ref=perms.at[at, slot],
            send_sem=ssem.at[SEM["perm"] + at * 2 + c], recv_sem=rsem.at[SEM["perm"] + at * 2 + slot],
            device_id=device, device_id_type=MESH)
        copy.start()
        sent.append(copy)

    for q in range(8):
        for s in range(2):
            rows = pl.ds(pl.multiple_of(far_rows + q * step, step), step)
            arrived(raw.at[0, s, rows], SEM["in"] + q * 2 + s)
            send(raw.at[0, s, rows], raw.at[1, s, rows], SEM["z_fwd"] + q * 2 + s, same[Z0])

    keep.wait()
    arrived(raw.at[0, 1 - slot, pl.ds(pl.multiple_of(my_rows, H), H)], SEM["near_raw"])
    arrived(perms.at[0, 1 - slot], SEM["perm"] + (1 - slot))
    for at in range(1, 4):
        for s in range(2):
            arrived(perms.at[at, s], SEM["perm"] + at * 2 + s)

    Q = N // 4

    def rows4(q):
        return pl.ds(q * Q, Q)

    def cost_part(level, q, part, own):
        mine_g[level, rows4(q)] = lax.dot_general(
            part[rows4(q)], own[...], (((1,), (1,)), ((), ())), preferred_element_type=jnp.float32)
        send(mine_g.at[level, rows4(q)], near_g.at[level, rows4(q)], SEM["cost"] + level * 4 + q, near)

    def merge(level, perm_row, part, own, out, then=lambda q: None):
        for q in range(4):
            arrived(near_g.at[level, rows4(q)], SEM["cost"] + level * 4 + q)
        cost = (mine_g[level] + near_g[level]) * (1.0 / math.sqrt(D))
        squared = cost * cost
        fourth = squared * squared
        scale = 1.0 / (1.0 + jnp.sum(fourth, axis=0, keepdims=True))
        neuron = lax.broadcasted_iota(jnp.int32, (N, N), 0)
        onehot = (neuron == perm_row).astype(jnp.float32)
        mixing = onehot + fourth * scale
        mix[...] = mixing.T.astype(jnp.bfloat16)
        for q in range(4):
            aligned = 0.5 * jnp.dot(mix[rows4(q)], part[...], preferred_element_type=jnp.float32)
            out[rows4(q)] = (
                (own[rows4(q)].astype(jnp.float32) + aligned) * (1.0 / math.sqrt(2.0))).astype(jnp.bfloat16)
            then(q)

    def perm_of(at, r):
        return perms[at, 0, r:r + 1]

    for q in range(4):
        cost_part(0, q, raw.at[0, 1], raw.at[0, 0])
    for s in range(2):
        arrived(raw.at[1, s, pl.ds(pl.multiple_of(my_rows, H), H)], SEM["z_raw"] + s)
    for q in range(8):
        for s in range(2):
            rows = pl.ds(pl.multiple_of(far_rows + q * step, step), step)
            arrived(raw.at[1, s, rows], SEM["z_fwd"] + q * 2 + s)
    for q in range(4):
        cost_part(1, q, raw.at[1, 1], raw.at[1, 0])
    merge(0, perm_of(0, 0), raw.at[0, 1], raw.at[0, 0], first.at[0])
    merge(1, perm_of(1, 0), raw.at[1, 1], raw.at[1, 0], first.at[1])
    for q in range(4):
        cost_part(2, q, first.at[1], first.at[0])

    def send2(q):
        send(cur.at[0, rows4(q)], got.at[0, rows4(q)], SEM["p2"] + q, same[Z1])

    merge(2, perm_of(0, 1), first.at[1], first.at[0], cur.at[0], send2)
    for q in range(4):
        arrived(got.at[0, rows4(q)], SEM["p2"] + q)
        cost_part(3, q, got.at[0], cur.at[0])

    O = N // 8

    def rows8(q):
        return pl.ds(q * O, O)

    def send3(q):
        for e in (2 * q, 2 * q + 1):
            send(cur.at[1, rows8(e)], got.at[1, rows8(e)], SEM["p3z"] + e, same[Z2])
        send(cur.at[1, rows4(q)], got.at[2, rows4(q)], SEM["p3x"] + q, same[X0])

    merge(3, perm_of(0, 2), got.at[0], cur.at[0], cur.at[1], send3)
    for q in range(4):
        for e in (2 * q, 2 * q + 1):
            arrived(got.at[1, rows8(e)], SEM["p3z"] + e)
            send(got.at[1, rows8(e)], got.at[3, rows8(e)], SEM["p3f"] + e, same[X0])
        cost_part(4, q, got.at[1], cur.at[1])
    for q in range(4):
        arrived(got.at[2, rows4(q)], SEM["p3x"] + q)
    for q in range(4):
        for e in (2 * q, 2 * q + 1):
            arrived(got.at[3, rows8(e)], SEM["p3f"] + e)
        cost_part(5, q, got.at[3], got.at[2])
    merge(4, perm_of(0, 3), got.at[1], cur.at[1], first.at[2])
    merge(5, perm_of(2, 3), got.at[3], got.at[2], first.at[3])
    for q in range(4):
        cost_part(6, q, first.at[3], first.at[2])

    def send4(q):
        send(cur.at[2, rows4(q)], got.at[5, rows4(q)], SEM["p4y"] + q, same[Y0])
        if q >= 2:
            send(cur.at[2, rows4(q)], got.at[4, rows4(q)], SEM["p4x"] + q, same[X1])
        if q == 3:
            for e in range(2):
                send(cur.at[2, rows4(e)], got.at[4, rows4(e)], SEM["p4x"] + e, same[X1])

    merge(6, perm_of(0, 4), first.at[3], first.at[2], cur.at[2], send4)
    for e in range(2):
        arrived(got.at[5, rows4(e)], SEM["p4y"] + e)
        send(got.at[5, rows4(e)], got.at[6, rows4(e)], SEM["p4fx"] + e, same[X1])
        arrived(got.at[4, rows4(e + 2)], SEM["p4x"] + e + 2)
        send(got.at[4, rows4(e + 2)], got.at[6, rows4(e + 2)], SEM["p4fy"] + e, same[Y0])
        cost_part(7, e + 2, got.at[4], cur.at[2])
    for e in range(2):
        arrived(got.at[4, rows4(e)], SEM["p4x"] + e)
        cost_part(7, e, got.at[4], cur.at[2])
        arrived(got.at[5, rows4(e + 2)], SEM["p4y"] + e + 2)
    for e in range(2):
        arrived(got.at[6, rows4(e)], SEM["p4fx"] + e)
        cost_part(8, e, got.at[6], got.at[5])
        arrived(got.at[6, rows4(e + 2)], SEM["p4fy"] + e)
        cost_part(8, e + 2, got.at[6], got.at[5])
    merge(7, perm_of(0, 5), got.at[4], cur.at[2], first.at[4])
    merge(8, perm_of(3, 5), got.at[6], got.at[5], first.at[5])
    for q in range(4):
        cost_part(9, q, first.at[5], first.at[4])

    def send5(q):
        send(cur.at[3, rows4(q)], got.at[7, rows4(q)], SEM["p5"] + q, same[Y1])

    merge(9, perm_of(0, 6), first.at[5], first.at[4], cur.at[3], send5)
    for q in range(4):
        arrived(got.at[7, rows4(q)], SEM["p5"] + q)
        cost_part(10, q, got.at[7], cur.at[3])
    fin = first.at[6]
    merge(10, perm_of(0, 7), got.at[7], cur.at[3], fin)

    cols = pl.ds(pl.multiple_of(g * F, F), F)
    away = pltpu.make_async_remote_copy(
        src_ref=fin.at[pl.ds(pl.multiple_of(far_rows, H), H)], dst_ref=o_ref.at[0, :, cols],
        send_sem=ssem.at[SEM["out"]], recv_sem=rsem.at[SEM["out"] + g],
        device_id=(core(rep, h), far), device_id_type=MESH)
    away.start()
    home_src = fin.at[pl.ds(pl.multiple_of(my_rows, H), H)]

    @pl.when(slot == 0)
    def _():
        home = pltpu.make_async_copy(home_src, o_ref.at[0, :, cols], lsem.at[2])
        home.start()
        home.wait()
        arrived(o_ref.at[0, :, pl.ds(pl.multiple_of((1 - g) * F, F), F)], SEM["out"] + 1 - g)

    @pl.when(slot == 1)
    def _():
        home = pltpu.make_async_remote_copy(
            src_ref=home_src, dst_ref=o_ref.at[0, :, cols],
            send_sem=ssem.at[SEM["out"] + 1], recv_sem=rsem.at[SEM["out"] + g],
            device_id=near, device_id_type=MESH)
        home.start()
        for c in range(2):
            arrived(o_ref.at[0, :, half(c)], SEM["out"] + c)
        home.wait_send()

    away.wait_send()
    for copy in sent:
        copy.wait_send()


def local(weights, perms):
    rows = (N, F)
    return pl.pallas_call(
        kernel,
        out_shape=jax.ShapeDtypeStruct((1, H, D), jnp.bfloat16),
        in_specs=[pl.BlockSpec(memory_space=pl.ANY), pl.BlockSpec(memory_space=pltpu.VMEM)],
        out_specs=pl.BlockSpec(memory_space=pl.ANY),
        scratch_shapes=[
            pltpu.VMEM((H, D), jnp.bfloat16),
            pltpu.VMEM((4, 2, 8, N), jnp.int32),
            pltpu.VMEM((2, 2, *rows), jnp.bfloat16),
            pltpu.VMEM((7, *rows), jnp.bfloat16),
            pltpu.VMEM((4, *rows), jnp.bfloat16),
            pltpu.VMEM((8, *rows), jnp.bfloat16),
            pltpu.VMEM((11, N, N), jnp.float32),
            pltpu.VMEM((11, N, N), jnp.float32),
            pltpu.VMEM((N, N), jnp.bfloat16),
            pltpu.SemaphoreType.DMA((N_SEM,)),
            pltpu.SemaphoreType.DMA((N_SEM,)),
            pltpu.SemaphoreType.DMA((3,)),
        ],
        compiler_params=pltpu.CompilerParams(
            collective_id=0, has_side_effects=True, vmem_limit_bytes=60 * 1024 * 1024),
    )(weights, perms)


def solution(mesh):
    placed = (P("rep", "slab", None), P("rep", None, None))
    return jax.shard_map(
        local, mesh=mesh, in_specs=placed, out_specs=P("rep", "slab", None), check_vma=False
    )
```

```python
import functools
import math

import jax
import jax.numpy as jnp
from jax import lax
from jax.experimental import pallas as pl
from jax.experimental.pallas import tpu as pltpu
from jax.sharding import PartitionSpec as P

D = 3072
N = 256
H = N // 2
F = D // 2
MESH = pl.DeviceIdType.MESH
NEAR, Z0, Z1, Z2, X0, X1, Y0, Y1 = range(8)


def layout(counts):
    at, out = 0, {}
    for name, count in counts:
        out[name] = at
        at += count
    return out, at


SEM, N_SEM = layout([
    ("near_raw", 1), ("in", 16), ("z_raw", 2), ("z_fwd", 16), ("perm", 8),
    ("z1", 8), ("z2", 8), ("z3", 4), ("z4", 4), ("x1", 8), ("x2", 4), ("y0", 4), ("y1", 4), ("out", 2),
    ("cost", 11 * 4),
])


def kernel(w_hbm, p_ref, o_ref, wv, perms, raw, first, cur, got, relay, relay_half, mine_g, near_g, mix, ssem, rsem, lsem):
    rep, h = lax.axis_index("rep"), lax.axis_index("slab")
    g = rep % 2
    far = 1 - h

    def flip(bit):
        return rep + (1 << bit) * (1 - 2 * ((rep // (1 << bit)) % 2))

    def core(base, c):
        return base - g + c

    def xor(a, b):
        return a + b - 2 * a * b

    near = (flip(0), h)
    chip = [flip(b) for b in range(8)]
    same = [(chip[b], h) for b in range(8)]

    load = pltpu.make_async_copy(w_hbm.at[0], wv, lsem.at[0])
    load.start()

    z, x = (rep // 2) % 8, (rep // 16) % 4
    z_next, z_last = (rep + 2 * ((z + 1) % 8 - z), h), (rep + 2 * ((z + 7) % 8 - z), h)
    x_next, x_last = (rep + 16 * ((x + 1) % 4 - x), h), (rep + 16 * ((x + 3) % 4 - x), h)

    peers = [near, z_next, z_last, x_next, x_last, same[Y0], same[Y1]]
    for c in range(2):
        peers.append((core(rep, c), far))
        for b in (Z0, Z2, X1):
            peers.append((core(chip[b], c), h))
    barrier = pltpu.get_barrier_semaphore()
    for peer in peers:
        pl.semaphore_signal(barrier, inc=1, device_id=peer, device_id_type=MESH)
    pl.semaphore_wait(barrier, len(peers))

    sent = []

    def send(src, dst, sem, device):
        copy = pltpu.make_async_remote_copy(
            src_ref=src, dst_ref=dst, send_sem=ssem.at[sem], recv_sem=rsem.at[sem],
            device_id=device, device_id_type=MESH,
        )
        copy.start()
        sent.append(copy)

    def arrived(dst, sem):
        pltpu.make_async_remote_copy(
            src_ref=dst, dst_ref=dst, send_sem=ssem.at[0], recv_sem=rsem.at[sem],
            device_id=near, device_id_type=MESH,
        ).wait_recv()

    def half(c):
        return pl.ds(c * F, F)

    slot, far_slot = xor(g, h), xor(g, far)
    my_rows, far_rows = h * H, far * H
    step = H // 8

    load.wait()
    keep = pltpu.make_async_copy(
        wv.at[:, pl.ds(pl.multiple_of(g * F, F), F)],
        raw.at[0, slot, pl.ds(pl.multiple_of(my_rows, H), H)], lsem.at[1])
    keep.start()

    def send_in(q, c):
        src = wv.at[pl.ds(q * step, step), half(c)]
        dst = raw.at[0, far_slot, pl.ds(pl.multiple_of(my_rows + q * step, step), step)]
        copy = pltpu.make_async_remote_copy(
            src_ref=src, dst_ref=dst, send_sem=ssem.at[SEM["in"] + q * 2 + c],
            recv_sem=rsem.at[SEM["in"] + q * 2 + far_slot],
            device_id=(core(rep, c), far), device_id_type=MESH)
        copy.start()
        sent.append(copy)

    for q in range(8):
        for c in range(2):
            send_in(q, c)
    for c in range(2):
        copy = pltpu.make_async_remote_copy(
            src_ref=wv.at[:, half(c)],
            dst_ref=raw.at[1, slot, pl.ds(pl.multiple_of(my_rows, H), H)],
            send_sem=ssem.at[SEM["z_raw"] + c], recv_sem=rsem.at[SEM["z_raw"] + slot],
            device_id=(core(chip[Z0], c), h), device_id_type=MESH)
        copy.start()
        sent.append(copy)
    send(wv.at[:, pl.ds(pl.multiple_of((1 - g) * F, F), F)],
         raw.at[0, slot, pl.ds(pl.multiple_of(my_rows, H), H)], SEM["near_raw"], near)

    perms[0, slot] = p_ref[0]
    perm_to = [(0, near, 0)]
    for at, b in ((1, Z0), (2, Z2), (3, X1)):
        for c in range(2):
            perm_to.append((at, (core(chip[b], c), h), c))
    for at, device, c in perm_to:
        copy = pltpu.make_async_remote_copy(
            src_ref=p_ref.at[0], dst_ref=perms.at[at, slot],
            send_sem=ssem.at[SEM["perm"] + at * 2 + c], recv_sem=rsem.at[SEM["perm"] + at * 2 + slot],
            device_id=device, device_id_type=MESH)
        copy.start()
        sent.append(copy)

    for q in range(8):
        for s in range(2):
            rows = pl.ds(pl.multiple_of(far_rows + q * step, step), step)
            arrived(raw.at[0, s, rows], SEM["in"] + q * 2 + s)
            send(raw.at[0, s, rows], raw.at[1, s, rows], SEM["z_fwd"] + q * 2 + s, same[Z0])

    keep.wait()
    arrived(raw.at[0, 1 - slot, pl.ds(pl.multiple_of(my_rows, H), H)], SEM["near_raw"])
    arrived(perms.at[0, 1 - slot], SEM["perm"] + (1 - slot))
    for at in range(1, 4):
        for s in range(2):
            arrived(perms.at[at, s], SEM["perm"] + at * 2 + s)

    Q = N // 4

    def rows4(q):
        return pl.ds(q * Q, Q)

    def cost_part(level, q, part, own):
        mine_g[level, rows4(q)] = lax.dot_general(
            part[rows4(q)], own[...], (((1,), (1,)), ((), ())), preferred_element_type=jnp.float32)
        send(mine_g.at[level, rows4(q)], near_g.at[level, rows4(q)], SEM["cost"] + level * 4 + q, near)

    def merge(level, perm_row, part, own, out, then=lambda q: None):
        for q in range(4):
            arrived(near_g.at[level, rows4(q)], SEM["cost"] + level * 4 + q)
        cost = (mine_g[level] + near_g[level]) * (1.0 / math.sqrt(D))
        squared = cost * cost
        fourth = squared * squared
        scale = 1.0 / (1.0 + jnp.sum(fourth, axis=0, keepdims=True))
        neuron = lax.broadcasted_iota(jnp.int32, (N, N), 0)
        onehot = (neuron == perm_row).astype(jnp.float32)
        mixing = onehot + fourth * scale
        mix[...] = mixing.T.astype(jnp.bfloat16)
        for q in range(4):
            aligned = 0.5 * jnp.dot(mix[rows4(q)], part[...], preferred_element_type=jnp.float32)
            out[rows4(q)] = (
                (own[rows4(q)].astype(jnp.float32) + aligned) * (1.0 / math.sqrt(2.0))).astype(jnp.bfloat16)
            then(q)

    def perm_of(at, r):
        return perms[at, 0, r:r + 1]

    for q in range(4):
        cost_part(0, q, raw.at[0, 1], raw.at[0, 0])
    for s in range(2):
        arrived(raw.at[1, s, pl.ds(pl.multiple_of(my_rows, H), H)], SEM["z_raw"] + s)
    for q in range(8):
        for s in range(2):
            rows = pl.ds(pl.multiple_of(far_rows + q * step, step), step)
            arrived(raw.at[1, s, rows], SEM["z_fwd"] + q * 2 + s)
    for q in range(4):
        cost_part(1, q, raw.at[1, 1], raw.at[1, 0])
    merge(0, perm_of(0, 0), raw.at[0, 1], raw.at[0, 0], first.at[0])
    merge(1, perm_of(1, 0), raw.at[1, 1], raw.at[1, 0], first.at[1])
    for q in range(4):
        cost_part(2, q, first.at[1], first.at[0])

    def quad(level, at, r, own, slots, wait_rings, wait_last, tmp, out, then):
        for q in range(4):
            wait_rings(q)
            cost_part(level, q, slots.at[0], own)
        wait_last()
        for q in range(4):
            cost_part(level + 1, q, slots.at[2], slots.at[1])
        merge(level, perm_of(0, r), slots.at[0], own, tmp.at[0])
        merge(level + 1, perm_of(at, r), slots.at[2], slots.at[1], tmp.at[1])
        for q in range(4):
            cost_part(level + 2, q, tmp.at[1], tmp.at[0])
        merge(level + 2, perm_of(0, r + 1), tmp.at[1], tmp.at[0], out, then)

    zq = got.at[pl.ds(0, 3)]

    def bit1(v):
        return (v // 2) % 2

    def send_z1(q):
        send(cur.at[0, rows4(q)], relay.at[0, rows4(q)], SEM["z1"] + q, z_next)
        send(cur.at[0, rows4(q)], relay.at[1, rows4(q)], SEM["z1"] + 4 + q, z_last)

    to_next, to_last = 2 * (1 - bit1((z + 1) % 8)), 2 * bit1((z + 7) % 8)
    from_last, from_next = 2 * (1 - bit1(z)), 2 * bit1(z)

    merge(2, perm_of(0, 1), first.at[1], first.at[0], cur.at[0], send_z1)
    for q in range(4):
        arrived(relay.at[0, rows4(q)], SEM["z1"] + q)
        send(relay.at[0, rows4(q)], zq.at[to_next, rows4(q)], SEM["z2"] + q, z_next)
        arrived(relay.at[1, rows4(q)], SEM["z1"] + 4 + q)
        send(relay.at[1, rows4(q)], zq.at[to_last, rows4(q)], SEM["z2"] + 4 + q, z_last)

    def rings_z(q):
        arrived(zq.at[from_last, rows4(q)], SEM["z2"] + q)
        if q < 2:
            send(zq.at[from_last, rows4(q)], relay_half.at[0, rows4(q)], SEM["z3"] + q, z_next)
        arrived(zq.at[from_next, rows4(q)], SEM["z2"] + 4 + q)
        if q >= 2:
            send(zq.at[from_next, rows4(q)], relay_half.at[1, rows4(q - 2)], SEM["z3"] + q, z_last)

    def last_z():
        for q in range(2):
            arrived(relay_half.at[0, rows4(q)], SEM["z3"] + q)
            send(relay_half.at[0, rows4(q)], zq.at[1, rows4(q)], SEM["z4"] + q, z_next)
            arrived(relay_half.at[1, rows4(q)], SEM["z3"] + 2 + q)
            send(relay_half.at[1, rows4(q)], zq.at[1, rows4(q + 2)], SEM["z4"] + 2 + q, z_last)
        for q in range(4):
            arrived(zq.at[1, rows4(q)], SEM["z4"] + q)

    def send_x1(q):
        send(cur.at[1, rows4(q)], xq.at[2 * (x % 2), rows4(q)], SEM["x1"] + q, x_next)
        send(cur.at[1, rows4(q)], xq.at[2 * (1 - x % 2), rows4(q)], SEM["x1"] + 4 + q, x_last)

    xq = got.at[pl.ds(3, 3)]
    quad(3, 2, 2, cur.at[0], zq, rings_z, last_z, first.at[pl.ds(2, 2)], cur.at[1], send_x1)

    def rings_x(q):
        arrived(xq.at[2 * (1 - x % 2), rows4(q)], SEM["x1"] + q)
        if q < 2:
            send(xq.at[2 * (1 - x % 2), rows4(q)], xq.at[1, rows4(q)], SEM["x2"] + q, x_next)
        arrived(xq.at[2 * (x % 2), rows4(q)], SEM["x1"] + 4 + q)
        if q >= 2:
            send(xq.at[2 * (x % 2), rows4(q)], xq.at[1, rows4(q)], SEM["x2"] + q, x_last)

    def last_x():
        for q in range(4):
            arrived(xq.at[1, rows4(q)], SEM["x2"] + q)

    def send_y0(q):
        send(cur.at[2, rows4(q)], got.at[6, rows4(q)], SEM["y0"] + q, same[Y0])

    quad(6, 3, 4, cur.at[1], xq, rings_x, last_x, first.at[pl.ds(4, 2)], cur.at[2], send_y0)

    for q in range(4):
        arrived(got.at[6, rows4(q)], SEM["y0"] + q)
        cost_part(9, q, got.at[6], cur.at[2])

    def send_y1(q):
        send(cur.at[3, rows4(q)], got.at[7, rows4(q)], SEM["y1"] + q, same[Y1])

    merge(9, perm_of(0, 6), got.at[6], cur.at[2], cur.at[3], send_y1)
    for q in range(4):
        arrived(got.at[7, rows4(q)], SEM["y1"] + q)
        cost_part(10, q, got.at[7], cur.at[3])
    fin = first.at[6]
    merge(10, perm_of(0, 7), got.at[7], cur.at[3], fin)

    cols = pl.ds(pl.multiple_of(g * F, F), F)
    away = pltpu.make_async_remote_copy(
        src_ref=fin.at[pl.ds(pl.multiple_of(far_rows, H), H)], dst_ref=o_ref.at[0, :, cols],
        send_sem=ssem.at[SEM["out"]], recv_sem=rsem.at[SEM["out"] + g],
        device_id=(core(rep, h), far), device_id_type=MESH)
    away.start()
    home_src = fin.at[pl.ds(pl.multiple_of(my_rows, H), H)]

    @pl.when(slot == 0)
    def _():
        home = pltpu.make_async_copy(home_src, o_ref.at[0, :, cols], lsem.at[2])
        home.start()
        home.wait()
        arrived(o_ref.at[0, :, pl.ds(pl.multiple_of((1 - g) * F, F), F)], SEM["out"] + 1 - g)

    @pl.when(slot == 1)
    def _():
        home = pltpu.make_async_remote_copy(
            src_ref=home_src, dst_ref=o_ref.at[0, :, cols],
            send_sem=ssem.at[SEM["out"] + 1], recv_sem=rsem.at[SEM["out"] + g],
            device_id=near, device_id_type=MESH)
        home.start()
        for c in range(2):
            arrived(o_ref.at[0, :, half(c)], SEM["out"] + c)
        home.wait_send()

    away.wait_send()
    for copy in sent:
        copy.wait_send()


def local(weights, perms):
    rows = (N, F)
    return pl.pallas_call(
        kernel,
        out_shape=jax.ShapeDtypeStruct((1, H, D), jnp.bfloat16),
        in_specs=[pl.BlockSpec(memory_space=pl.ANY), pl.BlockSpec(memory_space=pltpu.VMEM)],
        out_specs=pl.BlockSpec(memory_space=pl.ANY),
        scratch_shapes=[
            pltpu.VMEM((H, D), jnp.bfloat16),
            pltpu.VMEM((4, 2, 8, N), jnp.int32),
            pltpu.VMEM((2, 2, *rows), jnp.bfloat16),
            pltpu.VMEM((7, *rows), jnp.bfloat16),
            pltpu.VMEM((4, *rows), jnp.bfloat16),
            pltpu.VMEM((8, *rows), jnp.bfloat16),
            pltpu.VMEM((2, *rows), jnp.bfloat16),
            pltpu.VMEM((2, H, F), jnp.bfloat16),
            pltpu.VMEM((11, N, N), jnp.float32),
            pltpu.VMEM((11, N, N), jnp.float32),
            pltpu.VMEM((N, N), jnp.bfloat16),
            pltpu.SemaphoreType.DMA((N_SEM,)),
            pltpu.SemaphoreType.DMA((N_SEM,)),
            pltpu.SemaphoreType.DMA((3,)),
        ],
        compiler_params=pltpu.CompilerParams(
            collective_id=0, has_side_effects=True, vmem_limit_bytes=60 * 1024 * 1024),
    )(weights, perms)


def solution(mesh):
    placed = (P("rep", "slab", None), P("rep", None, None))
    return jax.shard_map(
        local, mesh=mesh, in_specs=placed, out_specs=P("rep", "slab", None), check_vma=False
    )
```

```python
import functools
import math

import jax
import jax.numpy as jnp
from jax import lax
from jax.experimental import pallas as pl
from jax.experimental.pallas import tpu as pltpu
from jax.sharding import PartitionSpec as P

D = 3072
N = 256
H = N // 2
F = D // 2
MESH = pl.DeviceIdType.MESH
NEAR, Z0, Z1, Z2, X0, X1, Y0, Y1 = range(8)


def layout(counts):
    at, out = 0, {}
    for name, count in counts:
        out[name] = at
        at += count
    return out, at


SEM, N_SEM = layout([
    ("near_raw", 1), ("in", 16), ("z_raw", 2), ("z_fwd", 16), ("perm", 10),
    ("z1", 8), ("z2", 8), ("z3", 4), ("z4", 4), ("x1", 8), ("x2", 4), ("y1", 4), ("y2", 4), ("y3", 4), ("out", 2), ("away", 4),
    ("cost", 12 * 4),
])


def kernel(w_hbm, p_ref, o_ref, wv, perms, raw, first, cur, got, relay, relay_half, mine_g, near_g, mix, ssem, rsem, lsem):
    rep, h = lax.axis_index("rep"), lax.axis_index("slab")
    g = rep % 2
    far = 1 - h

    def flip(bit):
        return rep + (1 << bit) * (1 - 2 * ((rep // (1 << bit)) % 2))

    def core(base, c):
        return base - g + c

    def xor(a, b):
        return a + b - 2 * a * b

    near = (flip(0), h)
    chip = [flip(b) for b in range(8)]
    same = [(chip[b], h) for b in range(8)]

    load = pltpu.make_async_copy(w_hbm.at[0], wv, lsem.at[0])
    load.start()

    z, x = (rep // 2) % 8, (rep // 16) % 4
    z_next, z_last = (rep + 2 * ((z + 1) % 8 - z), h), (rep + 2 * ((z + 7) % 8 - z), h)
    x_next, x_last = (rep + 16 * ((x + 1) % 4 - x), h), (rep + 16 * ((x + 3) % 4 - x), h)

    y = (rep // 64) % 4
    inner = ((y + 1) // 2) % 2
    y_cross = (rep + 64 * (3 - 2 * y), h)
    peers = [near, z_next, z_last, x_next, x_last, same[Y0], y_cross]
    for c in range(2):
        peers.append((core(rep, c), far))
        peers.append((core(chip[Y1], c), far))
        for b in (Z0, Z2, X1, Y1):
            peers.append((core(chip[b], c), h))
    barrier = pltpu.get_barrier_semaphore()
    for peer in peers:
        pl.semaphore_signal(barrier, inc=1, device_id=peer, device_id_type=MESH)
    pl.semaphore_wait(barrier, len(peers))

    sent = []

    def send(src, dst, sem, device):
        copy = pltpu.make_async_remote_copy(
            src_ref=src, dst_ref=dst, send_sem=ssem.at[sem], recv_sem=rsem.at[sem],
            device_id=device, device_id_type=MESH,
        )
        copy.start()
        sent.append(copy)

    def arrived(dst, sem):
        pltpu.make_async_remote_copy(
            src_ref=dst, dst_ref=dst, send_sem=ssem.at[0], recv_sem=rsem.at[sem],
            device_id=near, device_id_type=MESH,
        ).wait_recv()

    def half(c):
        return pl.ds(c * F, F)

    slot, far_slot = xor(g, h), xor(g, far)
    my_rows, far_rows = h * H, far * H
    step = H // 8

    load.wait()
    keep = pltpu.make_async_copy(
        wv.at[:, pl.ds(pl.multiple_of(g * F, F), F)],
        raw.at[0, slot, pl.ds(pl.multiple_of(my_rows, H), H)], lsem.at[1])
    keep.start()

    def send_in(q, c):
        src = wv.at[pl.ds(q * step, step), half(c)]
        dst = raw.at[0, far_slot, pl.ds(pl.multiple_of(my_rows + q * step, step), step)]
        copy = pltpu.make_async_remote_copy(
            src_ref=src, dst_ref=dst, send_sem=ssem.at[SEM["in"] + q * 2 + c],
            recv_sem=rsem.at[SEM["in"] + q * 2 + far_slot],
            device_id=(core(rep, c), far), device_id_type=MESH)
        copy.start()
        sent.append(copy)

    for q in range(8):
        for c in range(2):
            send_in(q, c)
    for c in range(2):
        copy = pltpu.make_async_remote_copy(
            src_ref=wv.at[:, half(c)],
            dst_ref=raw.at[1, slot, pl.ds(pl.multiple_of(my_rows, H), H)],
            send_sem=ssem.at[SEM["z_raw"] + c], recv_sem=rsem.at[SEM["z_raw"] + slot],
            device_id=(core(chip[Z0], c), h), device_id_type=MESH)
        copy.start()
        sent.append(copy)
    send(wv.at[:, pl.ds(pl.multiple_of((1 - g) * F, F), F)],
         raw.at[0, slot, pl.ds(pl.multiple_of(my_rows, H), H)], SEM["near_raw"], near)

    perms[0, slot] = p_ref[0]
    perm_to = [(0, near, 0)]
    for at, b in ((1, Z0), (2, Z2), (3, X1), (4, Y1)):
        for c in range(2):
            perm_to.append((at, (core(chip[b], c), h), c))
    for at, device, c in perm_to:
        copy = pltpu.make_async_remote_copy(
            src_ref=p_ref.at[0], dst_ref=perms.at[at, slot],
            send_sem=ssem.at[SEM["perm"] + at * 2 + c], recv_sem=rsem.at[SEM["perm"] + at * 2 + slot],
            device_id=device, device_id_type=MESH)
        copy.start()
        sent.append(copy)

    for q in range(8):
        for s in range(2):
            rows = pl.ds(pl.multiple_of(far_rows + q * step, step), step)
            arrived(raw.at[0, s, rows], SEM["in"] + q * 2 + s)
            send(raw.at[0, s, rows], raw.at[1, s, rows], SEM["z_fwd"] + q * 2 + s, same[Z0])

    keep.wait()
    arrived(raw.at[0, 1 - slot, pl.ds(pl.multiple_of(my_rows, H), H)], SEM["near_raw"])
    arrived(perms.at[0, 1 - slot], SEM["perm"] + (1 - slot))
    for at in range(1, 5):
        for s in range(2):
            arrived(perms.at[at, s], SEM["perm"] + at * 2 + s)

    Q = N // 4

    def rows4(q):
        return pl.ds(q * Q, Q)

    pieces = {}

    def cost_part(level, q, part, own, parts=4):
        pieces[level] = parts
        rows = pl.ds(q * (N // parts), N // parts)
        mine_g[level, rows] = lax.dot_general(
            part[rows], own[...], (((1,), (1,)), ((), ())), preferred_element_type=jnp.float32)
        send(mine_g.at[level, rows], near_g.at[level, rows], SEM["cost"] + level * 4 + q, near)

    def fourth_of(level):
        parts = pieces[level]
        for q in range(parts):
            arrived(near_g.at[level, pl.ds(q * (N // parts), N // parts)], SEM["cost"] + level * 4 + q)
        cost = (mine_g[level] + near_g[level]) * (1.0 / math.sqrt(D))
        squared = cost * cost
        return squared * squared

    def onehot_of(perm_row):
        neuron = lax.broadcasted_iota(jnp.int32, (N, N), 0)
        return jnp.where(neuron == perm_row, 0.5, 0.0)

    def mixing_of(fourth, perm_row):
        scale = 0.5 / (1.0 + jnp.sum(fourth, axis=0, keepdims=True))
        mix[...] = (onehot_of(perm_row) + fourth * scale).T.astype(jnp.bfloat16)

    def mix_in(part, own, out, then):
        for t in range(F // N):
            tile = pl.ds(t * N, N)
            aligned = jnp.dot(mix[...], part[:, tile], preferred_element_type=jnp.float32)
            out[:, tile] = (
                (own[:, tile].astype(jnp.float32) + aligned) * (1.0 / math.sqrt(2.0))).astype(jnp.bfloat16)
        for q in range(4):
            then(q)

    def merge(level, perm_row, part, own, out, then=lambda q: None):
        mixing_of(fourth_of(level), perm_row)
        mix_in(part, own, out, then)

    def perm_of(at, r):
        return perms[at, 0, r:r + 1]

    cost_part(0, 0, raw.at[0, 1], raw.at[0, 0], 1)
    merge(0, perm_of(0, 0), raw.at[0, 1], raw.at[0, 0], first.at[0])
    for s in range(2):
        arrived(raw.at[1, s, pl.ds(pl.multiple_of(my_rows, H), H)], SEM["z_raw"] + s)
    for q in range(8):
        for s in range(2):
            rows = pl.ds(pl.multiple_of(far_rows + q * step, step), step)
            arrived(raw.at[1, s, rows], SEM["z_fwd"] + q * 2 + s)
    cost_part(1, 0, raw.at[1, 1], raw.at[1, 0], 1)
    merge(1, perm_of(1, 0), raw.at[1, 1], raw.at[1, 0], first.at[1])
    cost_part(2, 0, first.at[1], first.at[0], 1)

    def quad(level, at, r, own, slots, wait_rings, wait_last, tmp):
        for q in range(4):
            wait_rings(q)
            cost_part(level, q, slots.at[0], own)
        merge(level, perm_of(0, r), slots.at[0], own, tmp.at[0])
        wait_last()
        cost_part(level + 1, 0, slots.at[2], slots.at[1], 1)
        merge(level + 1, perm_of(at, r), slots.at[2], slots.at[1], tmp.at[1])
        cost_part(level + 2, 0, tmp.at[1], tmp.at[0], 1)

    zq = got.at[pl.ds(0, 3)]

    def bit1(v):
        return (v // 2) % 2

    def send_z1(q):
        send(cur.at[0, rows4(q)], relay.at[0, rows4(q)], SEM["z1"] + q, z_next)
        send(cur.at[0, rows4(q)], relay.at[1, rows4(q)], SEM["z1"] + 4 + q, z_last)

    to_next, to_last = 2 * (1 - bit1((z + 1) % 8)), 2 * bit1((z + 7) % 8)
    from_last, from_next = 2 * (1 - bit1(z)), 2 * bit1(z)

    merge(2, perm_of(0, 1), first.at[1], first.at[0], cur.at[0], send_z1)
    for q in range(4):
        arrived(relay.at[0, rows4(q)], SEM["z1"] + q)
        send(relay.at[0, rows4(q)], zq.at[to_next, rows4(q)], SEM["z2"] + q, z_next)
        arrived(relay.at[1, rows4(q)], SEM["z1"] + 4 + q)
        send(relay.at[1, rows4(q)], zq.at[to_last, rows4(q)], SEM["z2"] + 4 + q, z_last)

    def rings_z(q):
        arrived(zq.at[from_last, rows4(q)], SEM["z2"] + q)
        if q < 2:
            send(zq.at[from_last, rows4(q)], relay_half.at[0, rows4(q)], SEM["z3"] + q, z_next)
        arrived(zq.at[from_next, rows4(q)], SEM["z2"] + 4 + q)
        if q >= 2:
            send(zq.at[from_next, rows4(q)], relay_half.at[1, rows4(q - 2)], SEM["z3"] + q, z_last)

    def last_z():
        for q in range(2):
            arrived(relay_half.at[0, rows4(q)], SEM["z3"] + q)
            send(relay_half.at[0, rows4(q)], zq.at[1, rows4(q)], SEM["z4"] + q, z_next)
            arrived(relay_half.at[1, rows4(q)], SEM["z3"] + 2 + q)
            send(relay_half.at[1, rows4(q)], zq.at[1, rows4(q + 2)], SEM["z4"] + 2 + q, z_last)
        for q in range(4):
            arrived(zq.at[1, rows4(q)], SEM["z4"] + q)

    def send_x1(q):
        send(cur.at[1, rows4(q)], xq.at[2 * (x % 2), rows4(q)], SEM["x1"] + q, x_next)
        send(cur.at[1, rows4(q)], xq.at[2 * (1 - x % 2), rows4(q)], SEM["x1"] + 4 + q, x_last)

    xq = got.at[pl.ds(3, 3)]
    quad(3, 2, 2, cur.at[0], zq, rings_z, last_z, first.at[pl.ds(2, 2)])
    merge(5, perm_of(0, 3), first.at[3], first.at[2], cur.at[1], send_x1)

    def rings_x(q):
        arrived(xq.at[2 * (1 - x % 2), rows4(q)], SEM["x1"] + q)
        if q < 2:
            send(xq.at[2 * (1 - x % 2), rows4(q)], xq.at[1, rows4(q)], SEM["x2"] + q, x_next)
        arrived(xq.at[2 * (x % 2), rows4(q)], SEM["x1"] + 4 + q)
        if q >= 2:
            send(xq.at[2 * (x % 2), rows4(q)], xq.at[1, rows4(q)], SEM["x2"] + q, x_last)

    def last_x():
        for q in range(4):
            arrived(xq.at[1, rows4(q)], SEM["x2"] + q)

    quad(6, 3, 4, cur.at[1], xq, rings_x, last_x, first.at[pl.ds(4, 2)])

    yq = got.at[pl.ds(6, 3)]
    o_cols = pl.ds(pl.multiple_of(g * F, F), F)

    @pl.when(inner == 0)
    def _():
        outer_sends = []
        merge(8, perm_of(0, 5), first.at[5], first.at[4], cur.at[2])
        for q in range(4):
            copy = pltpu.make_async_remote_copy(
                src_ref=cur.at[2, rows4(q)], dst_ref=yq.at[0, rows4(q)], send_sem=ssem.at[SEM["y1"] + q],
                recv_sem=rsem.at[SEM["y1"] + q], device_id=same[Y0], device_id_type=MESH)
            copy.start()
            outer_sends.append(copy)
        for c in range(2):
            arrived(o_ref.at[0, :, half(c)], SEM["out"] + c)
        for copy in outer_sends:
            copy.wait_send()

    @pl.when(inner == 1)
    def _():
        before = len(sent)

        def send_y2(q):
            send(cur.at[2, rows4(q)], yq.at[2, rows4(q)], SEM["y2"] + q, y_cross)

        merge(8, perm_of(0, 5), first.at[5], first.at[4], cur.at[2], send_y2)

        def rings_y(q):
            arrived(yq.at[0, rows4(q)], SEM["y1"] + q)
            send(yq.at[0, rows4(q)], yq.at[1, rows4(q)], SEM["y3"] + q, y_cross)

        def last_y():
            for q in range(4):
                arrived(yq.at[2, rows4(q)], SEM["y2"] + q)
            for q in range(4):
                arrived(yq.at[1, rows4(q)], SEM["y3"] + q)

        quad(9, 4, 6, cur.at[2], yq, rings_y, last_y, first.at[pl.ds(6, 2)])
        ours, theirs = first.at[6], first.at[7]

        def away(src, rows, at, device):
            copy = pltpu.make_async_remote_copy(
                src_ref=src.at[pl.ds(pl.multiple_of(rows, H), H)], dst_ref=o_ref.at[0, :, o_cols],
                send_sem=ssem.at[SEM["away"] + at], recv_sem=rsem.at[SEM["out"] + g],
                device_id=device, device_id_type=MESH)
            copy.start()
            return copy

        fourth = fourth_of(11)
        mixing_of(fourth, perm_of(0, 7))
        mix_in(theirs, ours, cur.at[3], lambda q: None)
        leaving = [away(cur.at[3], far_rows, 0, (core(rep, h), far))]
        scale = 0.5 / (1.0 + jnp.sum(fourth, axis=1, keepdims=True))
        mix[...] = (onehot_of(perm_of(4, 7)).T + fourth * scale).astype(jnp.bfloat16)
        mix_in(ours, theirs, cur.at[4], lambda q: None)
        leaving.append(away(cur.at[4], my_rows, 1, (core(chip[Y1], h), h)))
        leaving.append(away(cur.at[4], far_rows, 2, (core(chip[Y1], h), far)))

        @pl.when(slot == 0)
        def _():
            home = pltpu.make_async_copy(
                cur.at[3, pl.ds(pl.multiple_of(my_rows, H), H)], o_ref.at[0, :, o_cols], lsem.at[2])
            home.start()
            home.wait()
            arrived(o_ref.at[0, :, pl.ds(pl.multiple_of((1 - g) * F, F), F)], SEM["out"] + 1 - g)

        @pl.when(slot == 1)
        def _():
            home = away(cur.at[3], my_rows, 3, near)
            for c in range(2):
                arrived(o_ref.at[0, :, half(c)], SEM["out"] + c)
            home.wait_send()

        for copy in leaving + sent[before:]:
            copy.wait_send()
        del sent[before:]

    for copy in sent:
        copy.wait_send()


def local(weights, perms):
    rows = (N, F)
    return pl.pallas_call(
        kernel,
        out_shape=jax.ShapeDtypeStruct((1, H, D), jnp.bfloat16),
        in_specs=[pl.BlockSpec(memory_space=pl.ANY), pl.BlockSpec(memory_space=pltpu.VMEM)],
        out_specs=pl.BlockSpec(memory_space=pl.ANY),
        scratch_shapes=[
            pltpu.VMEM((H, D), jnp.bfloat16),
            pltpu.VMEM((5, 2, 8, N), jnp.int32),
            pltpu.VMEM((2, 2, *rows), jnp.bfloat16),
            pltpu.VMEM((8, *rows), jnp.bfloat16),
            pltpu.VMEM((5, *rows), jnp.bfloat16),
            pltpu.VMEM((9, *rows), jnp.bfloat16),
            pltpu.VMEM((2, *rows), jnp.bfloat16),
            pltpu.VMEM((2, H, F), jnp.bfloat16),
            pltpu.VMEM((12, N, N), jnp.float32),
            pltpu.VMEM((12, N, N), jnp.float32),
            pltpu.VMEM((N, N), jnp.bfloat16),
            pltpu.SemaphoreType.DMA((N_SEM,)),
            pltpu.SemaphoreType.DMA((N_SEM,)),
            pltpu.SemaphoreType.DMA((3,)),
        ],
        compiler_params=pltpu.CompilerParams(
            collective_id=0, has_side_effects=True, vmem_limit_bytes=60 * 1024 * 1024),
    )(weights, perms)


def solution(mesh):
    placed = (P("rep", "slab", None), P("rep", None, None))
    return jax.shard_map(
        local, mesh=mesh, in_specs=placed, out_specs=P("rep", "slab", None), check_vma=False
    )
```

```python
import functools
import math

import jax
import jax.numpy as jnp
from jax import lax
from jax.experimental import pallas as pl
from jax.experimental.pallas import tpu as pltpu
from jax.sharding import PartitionSpec as P

D = 3072
N = 256
H = N // 2
F = D // 2
MESH = pl.DeviceIdType.MESH
NEAR, Z0, Z1, Z2, X0, X1, Y0, Y1 = range(8)


def layout(counts):
    at, out = 0, {}
    for name, count in counts:
        out[name] = at
        at += count
    return out, at


T = 256
TILES = F // T

SEM, N_SEM = layout([
    ("near_raw", 1), ("in", 16), ("z_raw", 2), ("z_fwd", 16), ("perm", 10),
    ("z1", 12), ("z2", 12), ("z3", 6), ("z4", 6), ("x1", 12), ("x2", 6), ("y1", 6), ("y2", 6), ("y3", 6), ("out", 4), ("away", 8),
    ("cost", 12 * 2),
])


def kernel(w_hbm, p_ref, o_ref, perms, raw, first, cur, got, relay, relay_half, mine_g, near_g, mix, ssem, rsem, lsem):
    rep, h = lax.axis_index("rep"), lax.axis_index("slab")
    g = rep % 2
    far = 1 - h

    def flip(bit):
        return rep + (1 << bit) * (1 - 2 * ((rep // (1 << bit)) % 2))

    def core(base, c):
        return base - g + c

    def xor(a, b):
        return a + b - 2 * a * b

    near = (flip(0), h)
    chip = [flip(b) for b in range(8)]
    same = [(chip[b], h) for b in range(8)]

    wv = w_hbm.at[0]

    z, x = (rep // 2) % 8, (rep // 16) % 4
    z_next, z_last = (rep + 2 * ((z + 1) % 8 - z), h), (rep + 2 * ((z + 7) % 8 - z), h)
    x_next, x_last = (rep + 16 * ((x + 1) % 4 - x), h), (rep + 16 * ((x + 3) % 4 - x), h)

    y = (rep // 64) % 4
    inner = ((y + 1) // 2) % 2
    y_cross = (rep + 64 * (3 - 2 * y), h)
    peers = [near, z_next, z_last, x_next, x_last, same[Y0], y_cross]
    for c in range(2):
        peers.append((core(rep, c), far))
        peers.append((core(chip[Y1], c), far))
        for b in (Z0, Z2, X1, Y1):
            peers.append((core(chip[b], c), h))
    barrier = pltpu.get_barrier_semaphore()
    for peer in peers:
        pl.semaphore_signal(barrier, inc=1, device_id=peer, device_id_type=MESH)
    pl.semaphore_wait(barrier, len(peers))

    sent = []

    def send(src, dst, sem, device):
        copy = pltpu.make_async_remote_copy(
            src_ref=src, dst_ref=dst, send_sem=ssem.at[sem], recv_sem=rsem.at[sem],
            device_id=device, device_id_type=MESH,
        )
        copy.start()
        sent.append(copy)

    def arrived(dst, sem):
        pltpu.make_async_remote_copy(
            src_ref=dst, dst_ref=dst, send_sem=ssem.at[0], recv_sem=rsem.at[sem],
            device_id=near, device_id_type=MESH,
        ).wait_recv()

    def half(c):
        return pl.ds(c * F, F)

    slot, far_slot = xor(g, h), xor(g, far)
    my_rows, far_rows = h * H, far * H
    step = H // 8

    keep = pltpu.make_async_copy(
        wv.at[:, pl.ds(pl.multiple_of(g * F, F), F)],
        raw.at[0, slot, pl.ds(pl.multiple_of(my_rows, H), H)], lsem.at[1])
    keep.start()

    def send_in(q, c):
        src = wv.at[pl.ds(q * step, step), half(c)]
        dst = raw.at[0, far_slot, pl.ds(pl.multiple_of(my_rows + q * step, step), step)]
        copy = pltpu.make_async_remote_copy(
            src_ref=src, dst_ref=dst, send_sem=ssem.at[SEM["in"] + q * 2 + c],
            recv_sem=rsem.at[SEM["in"] + q * 2 + far_slot],
            device_id=(core(rep, c), far), device_id_type=MESH)
        copy.start()
        sent.append(copy)

    for q in range(8):
        for c in range(2):
            send_in(q, c)
    for c in range(2):
        copy = pltpu.make_async_remote_copy(
            src_ref=wv.at[:, half(c)],
            dst_ref=raw.at[1, slot, pl.ds(pl.multiple_of(my_rows, H), H)],
            send_sem=ssem.at[SEM["z_raw"] + c], recv_sem=rsem.at[SEM["z_raw"] + slot],
            device_id=(core(chip[Z0], c), h), device_id_type=MESH)
        copy.start()
        sent.append(copy)
    send(wv.at[:, pl.ds(pl.multiple_of((1 - g) * F, F), F)],
         raw.at[0, slot, pl.ds(pl.multiple_of(my_rows, H), H)], SEM["near_raw"], near)

    perms[0, slot] = p_ref[0]
    perm_to = [(0, near, 0)]
    for at, b in ((1, Z0), (2, Z2), (3, X1), (4, Y1)):
        for c in range(2):
            perm_to.append((at, (core(chip[b], c), h), c))
    for at, device, c in perm_to:
        copy = pltpu.make_async_remote_copy(
            src_ref=p_ref.at[0], dst_ref=perms.at[at, slot],
            send_sem=ssem.at[SEM["perm"] + at * 2 + c], recv_sem=rsem.at[SEM["perm"] + at * 2 + slot],
            device_id=device, device_id_type=MESH)
        copy.start()
        sent.append(copy)

    for q in range(8):
        for s in range(2):
            rows = pl.ds(pl.multiple_of(far_rows + q * step, step), step)
            arrived(raw.at[0, s, rows], SEM["in"] + q * 2 + s)
            send(raw.at[0, s, rows], raw.at[1, s, rows], SEM["z_fwd"] + q * 2 + s, same[Z0])

    keep.wait()
    arrived(raw.at[0, 1 - slot, pl.ds(pl.multiple_of(my_rows, H), H)], SEM["near_raw"])
    arrived(perms.at[0, 1 - slot], SEM["perm"] + (1 - slot))
    for at in range(1, 5):
        for s in range(2):
            arrived(perms.at[at, s], SEM["perm"] + at * 2 + s)

    def tile(t):
        return pl.ds(t * T, T)

    def cost_of(level, part, own, early=(), late=tuple(range(TILES)), wait=lambda t: None):
        def over(tiles, rows):
            return sum(lax.dot_general(
                part[rows, tile(t)], own[:, tile(t)], (((1,), (1,)), ((), ())), preferred_element_type=jnp.float32)
                for t in tiles)

        if early:
            for t in early:
                wait(t)
            mine_g[level] = over(early, slice(None))
        for t in late:
            wait(t)
        for q in range(2):
            rows = pl.ds(q * H, H)
            value = over(late, rows)
            mine_g[level, rows] = mine_g[level, rows] + value if early else value
            send(mine_g.at[level, rows], near_g.at[level, rows], SEM["cost"] + level * 2 + q, near)

    def fourth_of(level):
        for q in range(2):
            arrived(near_g.at[level, pl.ds(q * H, H)], SEM["cost"] + level * 2 + q)
        cost = (mine_g[level] + near_g[level]) * (1.0 / math.sqrt(D))
        squared = cost * cost
        return squared * squared

    def onehot_of(perm_row):
        neuron = lax.broadcasted_iota(jnp.int32, (N, N), 0)
        return jnp.where(neuron == perm_row, 0.5, 0.0)

    def mixing_of(fourth, perm_row):
        scale = 0.5 / (1.0 + jnp.sum(fourth, axis=0, keepdims=True))
        mix[0] = (onehot_of(perm_row) + fourth * scale).T.astype(jnp.bfloat16)

    def mix_tile(at, t, part, own, out):
        aligned = jnp.dot(mix[at], part[:, tile(t)], preferred_element_type=jnp.float32)
        out[:, tile(t)] = (
            (own[:, tile(t)].astype(jnp.float32) + aligned) * (1.0 / math.sqrt(2.0))).astype(jnp.bfloat16)

    def merge(level, perm_row, part, own, out, then=lambda t: None):
        mixing_of(fourth_of(level), perm_row)
        for t in range(TILES):
            mix_tile(0, t, part, own, out)
            then(t)

    def perm_of(at, r):
        return perms[at, 0, r:r + 1]

    cost_of(0, raw.at[0, 1], raw.at[0, 0])
    merge(0, perm_of(0, 0), raw.at[0, 1], raw.at[0, 0], first.at[0])
    for s in range(2):
        arrived(raw.at[1, s, pl.ds(pl.multiple_of(my_rows, H), H)], SEM["z_raw"] + s)
    for q in range(8):
        for s in range(2):
            rows = pl.ds(pl.multiple_of(far_rows + q * step, step), step)
            arrived(raw.at[1, s, rows], SEM["z_fwd"] + q * 2 + s)
    cost_of(1, raw.at[1, 1], raw.at[1, 0])
    merge(1, perm_of(1, 0), raw.at[1, 1], raw.at[1, 0], first.at[1])
    cost_of(2, first.at[1], first.at[0])

    L = TILES // 2
    EARLY = tuple(t for e in range(L - 1) for t in (e, e + L))
    LATE = (L - 1, 2 * L - 1)

    def quad(level, at, r, own, slots, wait_rings, wait_opposite, tmp, early, late):
        for t in range(TILES):
            wait_rings(t)
        cost_of(level, slots.at[0], own)
        merge(level, perm_of(0, r), slots.at[0], own, tmp.at[0])
        cost_of(level + 1, slots.at[2], slots.at[1], early, late, wait_opposite)
        merge(level + 1, perm_of(at, r), slots.at[2], slots.at[1], tmp.at[1])
        cost_of(level + 2, tmp.at[1], tmp.at[0])

    zq = got.at[pl.ds(0, 3)]

    def bit1(v):
        return (v // 2) % 2

    to_next, to_last = 2 * (1 - bit1((z + 1) % 8)), 2 * bit1((z + 7) % 8)
    from_last, from_next = 2 * (1 - bit1(z)), 2 * bit1(z)

    def send_z1(t):
        send(cur.at[0, :, tile(t)], relay.at[0, :, tile(t)], SEM["z1"] + t, z_next)
        send(cur.at[0, :, tile(t)], relay.at[1, :, tile(t)], SEM["z1"] + TILES + t, z_last)

    merge(2, perm_of(0, 1), first.at[1], first.at[0], cur.at[0], send_z1)
    for t in range(TILES):
        arrived(relay.at[0, :, tile(t)], SEM["z1"] + t)
        send(relay.at[0, :, tile(t)], zq.at[to_next, :, tile(t)], SEM["z2"] + t, z_next)
        arrived(relay.at[1, :, tile(t)], SEM["z1"] + TILES + t)
        send(relay.at[1, :, tile(t)], zq.at[to_last, :, tile(t)], SEM["z2"] + TILES + t, z_last)

    def rings_z(t):
        arrived(zq.at[from_last, :, tile(t)], SEM["z2"] + t)
        if t < L:
            send(zq.at[from_last, :, tile(t)], relay_half.at[0, :, tile(t)], SEM["z3"] + t, z_next)
        arrived(zq.at[from_next, :, tile(t)], SEM["z2"] + TILES + t)
        if t >= L:
            send(zq.at[from_next, :, tile(t)], relay_half.at[1, :, tile(t - L)], SEM["z3"] + t, z_last)

    def pass_on_z(t):
        side, there = (0, z_next) if t < L else (1, z_last)
        arrived(relay_half.at[side, :, tile(t % L)], SEM["z3"] + t)
        send(relay_half.at[side, :, tile(t % L)], zq.at[1, :, tile(t)], SEM["z4"] + t, there)

    def opposite_z(t):
        if t == 0:
            for e in EARLY + LATE:
                pass_on_z(e)
        arrived(zq.at[1, :, tile(t)], SEM["z4"] + t)

    def send_x1(t):
        send(cur.at[1, :, tile(t)], xq.at[2 * (x % 2), :, tile(t)], SEM["x1"] + t, x_next)
        send(cur.at[1, :, tile(t)], xq.at[2 * (1 - x % 2), :, tile(t)], SEM["x1"] + TILES + t, x_last)

    quad(3, 2, 2, cur.at[0], zq, rings_z, opposite_z, first.at[pl.ds(2, 2)], EARLY, LATE)

    xq = got.at[pl.ds(3, 3)]
    merge(5, perm_of(0, 3), first.at[3], first.at[2], cur.at[1], send_x1)

    def rings_x(t):
        arrived(xq.at[2 * (1 - x % 2), :, tile(t)], SEM["x1"] + t)
        if t < L:
            send(xq.at[2 * (1 - x % 2), :, tile(t)], xq.at[1, :, tile(t)], SEM["x2"] + t, x_next)
        arrived(xq.at[2 * (x % 2), :, tile(t)], SEM["x1"] + TILES + t)
        if t >= L:
            send(xq.at[2 * (x % 2), :, tile(t)], xq.at[1, :, tile(t)], SEM["x2"] + t, x_last)

    def opposite_x(t):
        arrived(xq.at[1, :, tile(t)], SEM["x2"] + t)

    quad(6, 3, 4, cur.at[1], xq, rings_x, opposite_x, first.at[pl.ds(4, 2)], EARLY, LATE)

    yq = got.at[pl.ds(6, 3)]

    def out_cols(c, s):
        return pl.ds(pl.multiple_of(c * F + s * (F // 2), F // 2), F // 2)

    @pl.when(inner == 0)
    def _():
        before = len(sent)

        def send_y1(t):
            send(cur.at[2, :, tile(t)], yq.at[0, :, tile(t)], SEM["y1"] + t, same[Y0])

        merge(8, perm_of(0, 5), first.at[5], first.at[4], cur.at[2], send_y1)
        for c in range(2):
            for s in range(2):
                arrived(o_ref.at[0, :, out_cols(c, s)], SEM["out"] + 2 * c + s)
        for copy in sent[before:]:
            copy.wait_send()
        del sent[before:]

    @pl.when(inner == 1)
    def _():
        before = len(sent)

        def send_y2(t):
            send(cur.at[2, :, tile(t)], yq.at[2, :, tile(t)], SEM["y2"] + t, y_cross)

        merge(8, perm_of(0, 5), first.at[5], first.at[4], cur.at[2], send_y2)

        def rings_y(t):
            arrived(yq.at[0, :, tile(t)], SEM["y1"] + t)
            send(yq.at[0, :, tile(t)], yq.at[1, :, tile(t)], SEM["y3"] + t, y_cross)

        def opposite_y(t):
            if t == 0:
                for e in range(TILES):
                    arrived(yq.at[2, :, tile(e)], SEM["y2"] + e)
            arrived(yq.at[1, :, tile(t)], SEM["y3"] + t)

        quad(9, 4, 6, cur.at[2], yq, rings_y, opposite_y, first.at[pl.ds(6, 2)],
             tuple(range(TILES - 1)), (TILES - 1,))
        ours, theirs = first.at[6], first.at[7]

        def away(src, rows, s, at, device):
            copy = pltpu.make_async_remote_copy(
                src_ref=src.at[pl.ds(pl.multiple_of(rows, H), H), pl.ds(s * (F // 2), F // 2)],
                dst_ref=o_ref.at[0, :, out_cols(g, s)],
                send_sem=ssem.at[SEM["away"] + 2 * at + s], recv_sem=rsem.at[SEM["out"] + 2 * g + s],
                device_id=device, device_id_type=MESH)
            copy.start()
            return copy

        fourth = fourth_of(11)
        mixing_of(fourth, perm_of(0, 7))
        scale = 0.5 / (1.0 + jnp.sum(fourth, axis=1, keepdims=True))
        mix[1] = (onehot_of(perm_of(4, 7)).T + fourth * scale).astype(jnp.bfloat16)
        leaving = []
        for s in range(2):
            for t in range(s * L, (s + 1) * L):
                mix_tile(1, t, ours, theirs, cur.at[4])
            leaving.append(away(cur.at[4], my_rows, s, 1, (core(chip[Y1], h), h)))
            leaving.append(away(cur.at[4], far_rows, s, 2, (core(chip[Y1], h), far)))
            for t in range(s * L, (s + 1) * L):
                mix_tile(0, t, theirs, ours, cur.at[3])
            leaving.append(away(cur.at[3], far_rows, s, 0, (core(rep, h), far)))

        @pl.when(slot == 0)
        def _():
            home = pltpu.make_async_copy(
                cur.at[3, pl.ds(pl.multiple_of(my_rows, H), H)],
                o_ref.at[0, :, pl.ds(pl.multiple_of(g * F, F), F)], lsem.at[2])
            home.start()
            home.wait()
            for s in range(2):
                arrived(o_ref.at[0, :, out_cols(1 - g, s)], SEM["out"] + 2 * (1 - g) + s)

        @pl.when(slot == 1)
        def _():
            home = [away(cur.at[3], my_rows, s, 3, near) for s in range(2)]
            for c in range(2):
                for s in range(2):
                    arrived(o_ref.at[0, :, out_cols(c, s)], SEM["out"] + 2 * c + s)
            for copy in home:
                copy.wait_send()

        for copy in leaving + sent[before:]:
            copy.wait_send()
        del sent[before:]

    for copy in sent:
        copy.wait_send()


def local(weights, perms):
    rows = (N, F)
    return pl.pallas_call(
        kernel,
        out_shape=jax.ShapeDtypeStruct((1, H, D), jnp.bfloat16),
        in_specs=[pl.BlockSpec(memory_space=pltpu.HBM), pl.BlockSpec(memory_space=pltpu.VMEM)],
        out_specs=pl.BlockSpec(memory_space=pl.ANY),
        scratch_shapes=[
            pltpu.VMEM((5, 2, 8, N), jnp.int32),
            pltpu.VMEM((2, 2, *rows), jnp.bfloat16),
            pltpu.VMEM((8, *rows), jnp.bfloat16),
            pltpu.VMEM((5, *rows), jnp.bfloat16),
            pltpu.VMEM((9, *rows), jnp.bfloat16),
            pltpu.VMEM((2, *rows), jnp.bfloat16),
            pltpu.VMEM((2, N, F // 2), jnp.bfloat16),
            pltpu.VMEM((12, N, N), jnp.float32),
            pltpu.VMEM((12, N, N), jnp.float32),
            pltpu.VMEM((2, N, N), jnp.bfloat16),
            pltpu.SemaphoreType.DMA((N_SEM,)),
            pltpu.SemaphoreType.DMA((N_SEM,)),
            pltpu.SemaphoreType.DMA((3,)),
        ],
        compiler_params=pltpu.CompilerParams(
            collective_id=0, has_side_effects=True, vmem_limit_bytes=40 * 1024 * 1024),
    )(weights, perms)


def solution(mesh):
    placed = (P("rep", "slab", None), P("rep", None, None))
    return jax.shard_map(
        local, mesh=mesh, in_specs=placed, out_specs=P("rep", "slab", None), check_vma=False
    )
```

```python
import functools
import math

import jax
import jax.numpy as jnp
from jax import lax
from jax.experimental import pallas as pl
from jax.experimental.pallas import tpu as pltpu
from jax.sharding import PartitionSpec as P

D = 3072
N = 256
H = N // 2
F = D // 2
MESH = pl.DeviceIdType.MESH
NEAR, Z0, Z1, Z2, X0, X1, Y0, Y1 = range(8)


def layout(counts):
    at, out = 0, {}
    for name, count in counts:
        out[name] = at
        at += count
    return out, at


SEM, N_SEM = layout([
    ("near_raw", 1), ("in", 16), ("z_raw", 2), ("z_fwd", 16), ("perm", 10),
    ("z1", 8), ("z2", 8), ("z3", 4), ("z4", 4), ("x1", 8), ("x2", 4), ("y1", 4), ("y2", 4), ("y3", 4), ("out", 2), ("away", 4),
    ("cost", 6 * 4), ("pair", 3 * 4), ("seen", 3),
])


def kernel(w_hbm, p_ref, o_ref, wv, perms, raw, first, cur, got, relay, relay_half, mine_g, near_g, mine_p, near_p, mine_e, near_e, seen, next_fourth, onehot, mix, ssem, rsem, lsem):
    rep, h = lax.axis_index("rep"), lax.axis_index("slab")
    g = rep % 2
    far = 1 - h

    def flip(bit):
        return rep + (1 << bit) * (1 - 2 * ((rep // (1 << bit)) % 2))

    def core(base, c):
        return base - g + c

    def xor(a, b):
        return a + b - 2 * a * b

    near = (flip(0), h)
    chip = [flip(b) for b in range(8)]
    same = [(chip[b], h) for b in range(8)]

    load = pltpu.make_async_copy(w_hbm.at[0], wv, lsem.at[0])
    load.start()

    z, x = (rep // 2) % 8, (rep // 16) % 4
    z_next, z_last = (rep + 2 * ((z + 1) % 8 - z), h), (rep + 2 * ((z + 7) % 8 - z), h)
    x_next, x_last = (rep + 16 * ((x + 1) % 4 - x), h), (rep + 16 * ((x + 3) % 4 - x), h)

    y = (rep // 64) % 4
    inner = ((y + 1) // 2) % 2
    y_cross = (rep + 64 * (3 - 2 * y), h)
    peers = [near, z_next, z_last, x_next, x_last, same[Y0], y_cross]
    for c in range(2):
        peers.append((core(rep, c), far))
        peers.append((core(chip[Y1], c), far))
        for b in (Z0, Z2, X1, Y1):
            peers.append((core(chip[b], c), h))
    barrier = pltpu.get_barrier_semaphore()
    for peer in peers:
        pl.semaphore_signal(barrier, inc=1, device_id=peer, device_id_type=MESH)
    pl.semaphore_wait(barrier, len(peers))

    sent = []

    def send(src, dst, sem, device):
        copy = pltpu.make_async_remote_copy(
            src_ref=src, dst_ref=dst, send_sem=ssem.at[sem], recv_sem=rsem.at[sem],
            device_id=device, device_id_type=MESH,
        )
        copy.start()
        sent.append(copy)

    def arrived(dst, sem):
        pltpu.make_async_remote_copy(
            src_ref=dst, dst_ref=dst, send_sem=ssem.at[0], recv_sem=rsem.at[sem],
            device_id=near, device_id_type=MESH,
        ).wait_recv()

    def half(c):
        return pl.ds(c * F, F)

    slot, far_slot = xor(g, h), xor(g, far)
    my_rows, far_rows = h * H, far * H
    step = H // 8

    load.wait()
    keep = pltpu.make_async_copy(
        wv.at[:, pl.ds(pl.multiple_of(g * F, F), F)],
        raw.at[0, slot, pl.ds(pl.multiple_of(my_rows, H), H)], lsem.at[1])
    keep.start()

    def send_in(q, c):
        src = wv.at[pl.ds(q * step, step), half(c)]
        dst = raw.at[0, far_slot, pl.ds(pl.multiple_of(my_rows + q * step, step), step)]
        copy = pltpu.make_async_remote_copy(
            src_ref=src, dst_ref=dst, send_sem=ssem.at[SEM["in"] + q * 2 + c],
            recv_sem=rsem.at[SEM["in"] + q * 2 + far_slot],
            device_id=(core(rep, c), far), device_id_type=MESH)
        copy.start()
        sent.append(copy)

    for q in range(8):
        for c in range(2):
            send_in(q, c)
    for c in range(2):
        copy = pltpu.make_async_remote_copy(
            src_ref=wv.at[:, half(c)],
            dst_ref=raw.at[1, slot, pl.ds(pl.multiple_of(my_rows, H), H)],
            send_sem=ssem.at[SEM["z_raw"] + c], recv_sem=rsem.at[SEM["z_raw"] + slot],
            device_id=(core(chip[Z0], c), h), device_id_type=MESH)
        copy.start()
        sent.append(copy)
    send(wv.at[:, pl.ds(pl.multiple_of((1 - g) * F, F), F)],
         raw.at[0, slot, pl.ds(pl.multiple_of(my_rows, H), H)], SEM["near_raw"], near)

    perms[0, slot] = p_ref[0]
    perm_to = [(0, near, 0)]
    for at, b in ((1, Z0), (2, Z2), (3, X1), (4, Y1)):
        for c in range(2):
            perm_to.append((at, (core(chip[b], c), h), c))
    for at, device, c in perm_to:
        copy = pltpu.make_async_remote_copy(
            src_ref=p_ref.at[0], dst_ref=perms.at[at, slot],
            send_sem=ssem.at[SEM["perm"] + at * 2 + c], recv_sem=rsem.at[SEM["perm"] + at * 2 + slot],
            device_id=device, device_id_type=MESH)
        copy.start()
        sent.append(copy)

    for q in range(8):
        for s in range(2):
            rows = pl.ds(pl.multiple_of(far_rows + q * step, step), step)
            arrived(raw.at[0, s, rows], SEM["in"] + q * 2 + s)
            send(raw.at[0, s, rows], raw.at[1, s, rows], SEM["z_fwd"] + q * 2 + s, same[Z0])

    keep.wait()
    arrived(raw.at[0, 1 - slot, pl.ds(pl.multiple_of(my_rows, H), H)], SEM["near_raw"])
    arrived(perms.at[0, 1 - slot], SEM["perm"] + (1 - slot))
    for at in range(1, 5):
        for s in range(2):
            arrived(perms.at[at, s], SEM["perm"] + at * 2 + s)

    Q = N // 4

    def rows4(q):
        return pl.ds(q * Q, Q)

    pieces = {}

    def cost_part(level, q, part, own, parts=4):
        pieces[level] = parts
        rows = pl.ds(q * (N // parts), N // parts)
        mine_g[level, rows] = lax.dot_general(
            part[rows], own[...], (((1,), (1,)), ((), ())), preferred_element_type=jnp.float32)
        send(mine_g.at[level, rows], near_g.at[level, rows], SEM["cost"] + level * 4 + q, near)

    def fourth_of(level):
        parts = pieces[level]
        for q in range(parts):
            arrived(near_g.at[level, pl.ds(q * (N // parts), N // parts)], SEM["cost"] + level * 4 + q)
        cost = (mine_g[level] + near_g[level]) * (1.0 / math.sqrt(D))
        squared = cost * cost
        return squared * squared

    def onehot_of(perm_row):
        neuron = lax.broadcasted_iota(jnp.int32, (N, N), 0)
        return jnp.where(neuron == perm_row, 0.5, 0.0)

    def mixing_of(fourth, perm_row):
        scale = 0.5 / (1.0 + jnp.sum(fourth, axis=0, keepdims=True))
        mix[0] = (onehot_of(perm_row) + fourth * scale).T.astype(jnp.bfloat16)

    def rows2(q):
        return pl.ds(q * H, H)

    def mix_rows(at, rows, part, own, out):
        for t in range(F // N):
            tile = pl.ds(t * N, N)
            aligned = jnp.dot(mix[at, rows], part[:, tile], preferred_element_type=jnp.float32)
            out[rows, tile] = (
                (own[rows, tile].astype(jnp.float32) + aligned) * (1.0 / math.sqrt(2.0))).astype(jnp.bfloat16)

    def merge_with(fourth, perm_row, part, own, out, then=lambda q: None):
        mixing_of(fourth, perm_row)
        for q in range(2):
            mix_rows(0, rows2(q), part, own, out)
            then(2 * q)
            then(2 * q + 1)

    def merge(level, perm_row, part, own, out, then=lambda q: None):
        merge_with(fourth_of(level), perm_row, part, own, out, then)

    def perm_of(at, r):
        return perms[at, 0, r:r + 1]

    cost_part(0, 0, raw.at[0, 1], raw.at[0, 0], 1)
    merge(0, perm_of(0, 0), raw.at[0, 1], raw.at[0, 0], first.at[0])
    for s in range(2):
        arrived(raw.at[1, s, pl.ds(pl.multiple_of(my_rows, H), H)], SEM["z_raw"] + s)
    for q in range(8):
        for s in range(2):
            rows = pl.ds(pl.multiple_of(far_rows + q * step, step), step)
            arrived(raw.at[1, s, rows], SEM["z_fwd"] + q * 2 + s)
    cost_part(1, 0, raw.at[1, 1], raw.at[1, 0], 1)
    merge(1, perm_of(1, 0), raw.at[1, 1], raw.at[1, 0], first.at[1])
    cost_part(2, 0, first.at[1], first.at[0], 1)

    def quad(k, at, r, own, slots, wait_rings, order, wait_opposite, tmp):
        level = 3 + k
        for q in range(4):
            wait_rings(q)
            cost_part(level, q, slots.at[0], own)
        onehot[...] = onehot_of(perm_of(at, r)).T
        merge(level, perm_of(0, r), slots.at[0], own, tmp.at[0])
        mine_e[k] = lax.dot_general(
            slots[2], tmp[0], (((1,), (1,)), ((), ())), preferred_element_type=jnp.float32)
        send(mine_e.at[k], near_e.at[k], SEM["seen"] + k, near)

        def sums(q):
            mine_p[k, rows4(q), pl.ds(0, N)] = lax.dot_general(
                slots[1, rows4(q)], slots[2], (((1,), (1,)), ((), ())), preferred_element_type=jnp.float32)
            mine_p[k, rows4(q), pl.ds(N, N)] = lax.dot_general(
                slots[1, rows4(q)], tmp[0], (((1,), (1,)), ((), ())), preferred_element_type=jnp.float32)
            send(mine_p.at[k, rows4(q)], near_p.at[k, rows4(q)], SEM["pair"] + 4 * k + q, near)

        def level_of(q):
            rows = rows4(q)
            arrived(near_p.at[k, rows], SEM["pair"] + 4 * k + q)
            cost = (mine_p[k, rows, pl.ds(0, N)] + near_p[k, rows, pl.ds(0, N)]) * (1.0 / math.sqrt(D))
            squared = cost * cost
            fourth = squared * squared
            mixing = (onehot[rows] + fourth * (0.5 / (1.0 + jnp.sum(fourth, axis=1, keepdims=True)))).astype(jnp.bfloat16)
            mix[1, rows] = mixing
            through = (jnp.dot(mixing, seen[0], preferred_element_type=jnp.float32)
                       + jnp.dot(mixing, seen[1], preferred_element_type=jnp.float32))
            direct = mine_p[k, rows, pl.ds(N, N)] + near_p[k, rows, pl.ds(N, N)]
            cost = (direct + through) * (1.0 / math.sqrt(2.0 * D))
            squared = cost * cost
            next_fourth[rows] = squared * squared
            mix_rows(1, rows, slots.at[2], slots.at[1], tmp.at[1])

        for e, q in enumerate(order):
            wait_opposite(q)
            sums(q)
            if e == 0:
                arrived(near_e.at[k], SEM["seen"] + k)
                both = mine_e[k] + near_e[k]
                seen[0] = both.astype(jnp.bfloat16)
                seen[1] = (both - seen[0].astype(jnp.float32)).astype(jnp.bfloat16)
            else:
                level_of(order[e - 1])
        level_of(order[-1])

    zq = got.at[pl.ds(0, 3)]

    def bit1(v):
        return (v // 2) % 2

    def send_z1(q):
        send(cur.at[0, rows4(q)], relay.at[0, rows4(q)], SEM["z1"] + q, z_next)
        send(cur.at[0, rows4(q)], relay.at[1, rows4(q)], SEM["z1"] + 4 + q, z_last)

    to_next, to_last = 2 * (1 - bit1((z + 1) % 8)), 2 * bit1((z + 7) % 8)
    from_last, from_next = 2 * (1 - bit1(z)), 2 * bit1(z)

    merge(2, perm_of(0, 1), first.at[1], first.at[0], cur.at[0], send_z1)
    for q in range(4):
        arrived(relay.at[0, rows4(q)], SEM["z1"] + q)
        send(relay.at[0, rows4(q)], zq.at[to_next, rows4(q)], SEM["z2"] + q, z_next)
        arrived(relay.at[1, rows4(q)], SEM["z1"] + 4 + q)
        send(relay.at[1, rows4(q)], zq.at[to_last, rows4(q)], SEM["z2"] + 4 + q, z_last)

    def rings_z(q):
        arrived(zq.at[from_last, rows4(q)], SEM["z2"] + q)
        if q < 2:
            send(zq.at[from_last, rows4(q)], relay_half.at[0, rows4(q)], SEM["z3"] + q, z_next)
        arrived(zq.at[from_next, rows4(q)], SEM["z2"] + 4 + q)
        if q >= 2:
            send(zq.at[from_next, rows4(q)], relay_half.at[1, rows4(q - 2)], SEM["z3"] + q, z_last)

    def opposite_z(q):
        if q == 0:
            for e in (0, 2, 1, 3):
                side, there = (0, z_next) if e < 2 else (1, z_last)
                arrived(relay_half.at[side, rows4(e % 2)], SEM["z3"] + e)
                send(relay_half.at[side, rows4(e % 2)], zq.at[1, rows4(e)], SEM["z4"] + e, there)
        arrived(zq.at[1, rows4(q)], SEM["z4"] + q)

    def send_x1(q):
        send(cur.at[1, rows4(q)], xq.at[2 * (x % 2), rows4(q)], SEM["x1"] + q, x_next)
        send(cur.at[1, rows4(q)], xq.at[2 * (1 - x % 2), rows4(q)], SEM["x1"] + 4 + q, x_last)

    xq = got.at[pl.ds(3, 3)]
    quad(0, 2, 2, cur.at[0], zq, rings_z, (0, 2, 1, 3), opposite_z, first.at[pl.ds(2, 2)])
    merge_with(next_fourth[...], perm_of(0, 3), first.at[3], first.at[2], cur.at[1], send_x1)

    def rings_x(q):
        arrived(xq.at[2 * (1 - x % 2), rows4(q)], SEM["x1"] + q)
        if q < 2:
            send(xq.at[2 * (1 - x % 2), rows4(q)], xq.at[1, rows4(q)], SEM["x2"] + q, x_next)
        arrived(xq.at[2 * (x % 2), rows4(q)], SEM["x1"] + 4 + q)
        if q >= 2:
            send(xq.at[2 * (x % 2), rows4(q)], xq.at[1, rows4(q)], SEM["x2"] + q, x_last)

    def opposite_x(q):
        arrived(xq.at[1, rows4(q)], SEM["x2"] + q)

    quad(1, 3, 4, cur.at[1], xq, rings_x, (0, 2, 1, 3), opposite_x, first.at[pl.ds(4, 2)])

    yq = got.at[pl.ds(6, 3)]
    o_cols = pl.ds(pl.multiple_of(g * F, F), F)

    @pl.when(inner == 0)
    def _():
        outer_sends = []
        def send_y1(q):
            copy = pltpu.make_async_remote_copy(
                src_ref=cur.at[2, rows4(q)], dst_ref=yq.at[0, rows4(q)], send_sem=ssem.at[SEM["y1"] + q],
                recv_sem=rsem.at[SEM["y1"] + q], device_id=same[Y0], device_id_type=MESH)
            copy.start()
            outer_sends.append(copy)

        merge_with(next_fourth[...], perm_of(0, 5), first.at[5], first.at[4], cur.at[2], send_y1)
        for c in range(2):
            arrived(o_ref.at[0, :, half(c)], SEM["out"] + c)
        for copy in outer_sends:
            copy.wait_send()

    @pl.when(inner == 1)
    def _():
        before = len(sent)

        def send_y2(q):
            send(cur.at[2, rows4(q)], yq.at[2, rows4(q)], SEM["y2"] + q, y_cross)

        merge_with(next_fourth[...], perm_of(0, 5), first.at[5], first.at[4], cur.at[2], send_y2)

        def rings_y(q):
            arrived(yq.at[0, rows4(q)], SEM["y1"] + q)
            send(yq.at[0, rows4(q)], yq.at[1, rows4(q)], SEM["y3"] + q, y_cross)
            arrived(yq.at[2, rows4(q)], SEM["y2"] + q)

        def opposite_y(q):
            arrived(yq.at[1, rows4(q)], SEM["y3"] + q)

        quad(2, 4, 6, cur.at[2], yq, rings_y, (0, 1, 2, 3), opposite_y, first.at[pl.ds(6, 2)])
        ours, theirs = first.at[6], first.at[7]

        def away(src, rows, at, device):
            copy = pltpu.make_async_remote_copy(
                src_ref=src.at[pl.ds(pl.multiple_of(rows, H), H)], dst_ref=o_ref.at[0, :, o_cols],
                send_sem=ssem.at[SEM["away"] + at], recv_sem=rsem.at[SEM["out"] + g],
                device_id=device, device_id_type=MESH)
            copy.start()
            return copy

        fourth = next_fourth[...]
        mixing_of(fourth, perm_of(0, 7))
        scale = 0.5 / (1.0 + jnp.sum(fourth, axis=1, keepdims=True))
        mix[1] = (onehot_of(perm_of(4, 7)).T + fourth * scale).astype(jnp.bfloat16)
        leaving = []
        far_half, my_half = pl.ds(pl.multiple_of(far_rows, H), H), pl.ds(pl.multiple_of(my_rows, H), H)
        mix_rows(1, far_half, ours, theirs, cur.at[4])
        leaving.append(away(cur.at[4], far_rows, 2, (core(chip[Y1], h), far)))
        mix_rows(0, far_half, theirs, ours, cur.at[3])
        leaving.append(away(cur.at[3], far_rows, 0, (core(rep, h), far)))
        mix_rows(1, my_half, ours, theirs, cur.at[4])
        leaving.append(away(cur.at[4], my_rows, 1, (core(chip[Y1], h), h)))
        mix_rows(0, my_half, theirs, ours, cur.at[3])

        @pl.when(slot == 0)
        def _():
            home = pltpu.make_async_copy(
                cur.at[3, pl.ds(pl.multiple_of(my_rows, H), H)], o_ref.at[0, :, o_cols], lsem.at[2])
            home.start()
            home.wait()
            arrived(o_ref.at[0, :, pl.ds(pl.multiple_of((1 - g) * F, F), F)], SEM["out"] + 1 - g)

        @pl.when(slot == 1)
        def _():
            home = away(cur.at[3], my_rows, 3, near)
            for c in range(2):
                arrived(o_ref.at[0, :, half(c)], SEM["out"] + c)
            home.wait_send()

        for copy in leaving + sent[before:]:
            copy.wait_send()
        del sent[before:]

    for copy in sent:
        copy.wait_send()


def local(weights, perms):
    rows = (N, F)
    return pl.pallas_call(
        kernel,
        out_shape=jax.ShapeDtypeStruct((1, H, D), jnp.bfloat16),
        in_specs=[pl.BlockSpec(memory_space=pl.ANY), pl.BlockSpec(memory_space=pltpu.VMEM)],
        out_specs=pl.BlockSpec(memory_space=pl.ANY),
        scratch_shapes=[
            pltpu.VMEM((H, D), jnp.bfloat16),
            pltpu.VMEM((5, 2, 8, N), jnp.int32),
            pltpu.VMEM((2, 2, *rows), jnp.bfloat16),
            pltpu.VMEM((8, *rows), jnp.bfloat16),
            pltpu.VMEM((5, *rows), jnp.bfloat16),
            pltpu.VMEM((9, *rows), jnp.bfloat16),
            pltpu.VMEM((2, *rows), jnp.bfloat16),
            pltpu.VMEM((2, H, F), jnp.bfloat16),
            pltpu.VMEM((6, N, N), jnp.float32),
            pltpu.VMEM((6, N, N), jnp.float32),
            pltpu.VMEM((3, N, 2 * N), jnp.float32),
            pltpu.VMEM((3, N, 2 * N), jnp.float32),
            pltpu.VMEM((3, N, N), jnp.float32),
            pltpu.VMEM((3, N, N), jnp.float32),
            pltpu.VMEM((2, N, N), jnp.bfloat16),
            pltpu.VMEM((N, N), jnp.float32),
            pltpu.VMEM((N, N), jnp.float32),
            pltpu.VMEM((2, N, N), jnp.bfloat16),
            pltpu.SemaphoreType.DMA((N_SEM,)),
            pltpu.SemaphoreType.DMA((N_SEM,)),
            pltpu.SemaphoreType.DMA((3,)),
        ],
        compiler_params=pltpu.CompilerParams(
            collective_id=0, has_side_effects=True, vmem_limit_bytes=60 * 1024 * 1024),
    )(weights, perms)


def solution(mesh):
    placed = (P("rep", "slab", None), P("rep", None, None))
    return jax.shard_map(
        local, mesh=mesh, in_specs=placed, out_specs=P("rep", "slab", None), check_vma=False
    )
```

```python
import functools
import math

import jax
import jax.numpy as jnp
from jax import lax
from jax.experimental import pallas as pl
from jax.experimental.pallas import tpu as pltpu
from jax.sharding import PartitionSpec as P

D = 3072
N = 256
H = N // 2
F = D // 2
MESH = pl.DeviceIdType.MESH
NEAR, Z0, Z1, Z2, X0, X1, Y0, Y1 = range(8)


def layout(counts):
    at, out = 0, {}
    for name, count in counts:
        out[name] = at
        at += count
    return out, at


SEM, N_SEM = layout([
    ("near_raw", 1), ("in", 32), ("z_raw", 2), ("z_fwd", 32), ("perm", 10),
    ("z1", 8), ("z2", 8), ("z3", 4), ("z4", 4), ("x1", 8), ("x2", 4), ("y1", 4), ("y2", 4), ("y3", 4), ("out", 2), ("away", 4),
    ("cost", 6 * 4), ("pair", 3 * 4), ("seen", 3),
])


def kernel(w_hbm, p_hbm, o_ref, wv, perms, raw, first, cur, got, relay, relay_half, mine_g, near_g, mine_p, near_p, mine_e, near_e, seen, next_fourth, onehot, mix, ssem, rsem, lsem):
    rep, h = lax.axis_index("rep"), lax.axis_index("slab")
    g = rep % 2
    far = 1 - h

    def flip(bit):
        return rep + (1 << bit) * (1 - 2 * ((rep // (1 << bit)) % 2))

    def core(base, c):
        return base - g + c

    def xor(a, b):
        return a + b - 2 * a * b

    near = (flip(0), h)
    chip = [flip(b) for b in range(8)]
    same = [(chip[b], h) for b in range(8)]

    load = pltpu.make_async_copy(w_hbm.at[0], wv, lsem.at[0])
    load.start()
    slot = g + h - 2 * g * h
    load_perms = pltpu.make_async_copy(p_hbm.at[0], perms.at[0, slot], lsem.at[3])
    load_perms.start()

    z, x = (rep // 2) % 8, (rep // 16) % 4
    z_next, z_last = (rep + 2 * ((z + 1) % 8 - z), h), (rep + 2 * ((z + 7) % 8 - z), h)
    x_next, x_last = (rep + 16 * ((x + 1) % 4 - x), h), (rep + 16 * ((x + 3) % 4 - x), h)

    y = (rep // 64) % 4
    inner = ((y + 1) // 2) % 2
    y_cross = (rep + 64 * (3 - 2 * y), h)
    peers = [near, z_next, z_last, x_next, x_last, same[Y0], y_cross]
    for c in range(2):
        peers.append((core(rep, c), far))
        peers.append((core(chip[Y1], c), far))
        for b in (Z0, Z2, X1, Y1):
            peers.append((core(chip[b], c), h))
    barrier = pltpu.get_barrier_semaphore()
    for peer in peers:
        pl.semaphore_signal(barrier, inc=1, device_id=peer, device_id_type=MESH)
    pl.semaphore_wait(barrier, len(peers))

    sent = []

    def send(src, dst, sem, device):
        copy = pltpu.make_async_remote_copy(
            src_ref=src, dst_ref=dst, send_sem=ssem.at[sem], recv_sem=rsem.at[sem],
            device_id=device, device_id_type=MESH,
        )
        copy.start()
        sent.append(copy)

    def arrived(dst, sem):
        pltpu.make_async_remote_copy(
            src_ref=dst, dst_ref=dst, send_sem=ssem.at[0], recv_sem=rsem.at[sem],
            device_id=near, device_id_type=MESH,
        ).wait_recv()

    def half(c):
        return pl.ds(c * F, F)

    far_slot = xor(g, far)
    my_rows, far_rows = h * H, far * H
    step = H // 8

    load.wait()
    keep = pltpu.make_async_copy(
        wv.at[:, pl.ds(pl.multiple_of(g * F, F), F)],
        raw.at[0, slot, pl.ds(pl.multiple_of(my_rows, H), H)], lsem.at[1])
    keep.start()

    def piece(e):
        return pl.ds(e * (F // 2), F // 2)

    def send_in(q, e, c):
        src = wv.at[pl.ds(q * step, step), pl.ds(c * F + e * (F // 2), F // 2)]
        dst = raw.at[0, far_slot, pl.ds(pl.multiple_of(my_rows + q * step, step), step), piece(e)]
        copy = pltpu.make_async_remote_copy(
            src_ref=src, dst_ref=dst, send_sem=ssem.at[SEM["in"] + q * 4 + e * 2 + c],
            recv_sem=rsem.at[SEM["in"] + q * 4 + e * 2 + far_slot],
            device_id=(core(rep, c), far), device_id_type=MESH)
        copy.start()
        sent.append(copy)

    for q in range(8):
        for e in range(2):
            for c in range(2):
                send_in(q, e, c)
    for c in range(2):
        copy = pltpu.make_async_remote_copy(
            src_ref=wv.at[:, half(c)],
            dst_ref=raw.at[1, slot, pl.ds(pl.multiple_of(my_rows, H), H)],
            send_sem=ssem.at[SEM["z_raw"] + c], recv_sem=rsem.at[SEM["z_raw"] + slot],
            device_id=(core(chip[Z0], c), h), device_id_type=MESH)
        copy.start()
        sent.append(copy)
    send(wv.at[:, pl.ds(pl.multiple_of((1 - g) * F, F), F)],
         raw.at[0, slot, pl.ds(pl.multiple_of(my_rows, H), H)], SEM["near_raw"], near)

    load_perms.wait()
    perm_to = [(0, near, 0)]
    for at, b in ((1, Z0), (2, Z2), (3, X1), (4, Y1)):
        for c in range(2):
            perm_to.append((at, (core(chip[b], c), h), c))
    for at, device, c in perm_to:
        copy = pltpu.make_async_remote_copy(
            src_ref=perms.at[0, slot], dst_ref=perms.at[at, slot],
            send_sem=ssem.at[SEM["perm"] + at * 2 + c], recv_sem=rsem.at[SEM["perm"] + at * 2 + slot],
            device_id=device, device_id_type=MESH)
        copy.start()
        sent.append(copy)

    for q in range(8):
        rows = pl.ds(pl.multiple_of(far_rows + q * step, step), step)
        for e in range(2):
            for s in range(2):
                at = q * 4 + e * 2 + s
                arrived(raw.at[0, s, rows, piece(e)], SEM["in"] + at)
                send(raw.at[0, s, rows, piece(e)], raw.at[1, s, rows, piece(e)], SEM["z_fwd"] + at, same[Z0])

    keep.wait()
    arrived(raw.at[0, 1 - slot, pl.ds(pl.multiple_of(my_rows, H), H)], SEM["near_raw"])
    arrived(perms.at[0, 1 - slot], SEM["perm"] + (1 - slot))
    for at in range(1, 5):
        for s in range(2):
            arrived(perms.at[at, s], SEM["perm"] + at * 2 + s)

    Q = N // 4

    def rows4(q):
        return pl.ds(q * Q, Q)

    pieces = {}

    def cost_part(level, q, part, own, parts=4):
        pieces[level] = parts
        rows = pl.ds(q * (N // parts), N // parts)
        mine_g[level, rows] = lax.dot_general(
            part[rows], own[...], (((1,), (1,)), ((), ())), preferred_element_type=jnp.float32)
        send(mine_g.at[level, rows], near_g.at[level, rows], SEM["cost"] + level * 4 + q, near)

    def fourth_of(level):
        parts = pieces[level]
        for q in range(parts):
            arrived(near_g.at[level, pl.ds(q * (N // parts), N // parts)], SEM["cost"] + level * 4 + q)
        cost = (mine_g[level] + near_g[level]) * (1.0 / math.sqrt(D))
        squared = cost * cost
        return squared * squared

    def onehot_of(perm_row):
        neuron = lax.broadcasted_iota(jnp.int32, (N, N), 0)
        return jnp.where(neuron == perm_row, 0.5, 0.0)

    def mixing_of(fourth, perm_row):
        scale = 0.5 / (1.0 + jnp.sum(fourth, axis=0, keepdims=True))
        mix[0] = (onehot_of(perm_row) + fourth * scale).T.astype(jnp.bfloat16)

    def rows2(q):
        return pl.ds(q * H, H)

    def mix_rows(at, rows, part, own, out):
        for t in range(F // N):
            tile = pl.ds(t * N, N)
            aligned = jnp.dot(mix[at, rows], part[:, tile], preferred_element_type=jnp.float32)
            out[rows, tile] = (
                (own[rows, tile].astype(jnp.float32) + aligned) * (1.0 / math.sqrt(2.0))).astype(jnp.bfloat16)

    def merge_with(fourth, perm_row, part, own, out, then=lambda q: None):
        mixing_of(fourth, perm_row)
        for first_piece, count in ((0, 1), (1, 1), (2, 2)):
            mix_rows(0, pl.ds(first_piece * Q, count * Q), part, own, out)
            for q in range(first_piece, first_piece + count):
                then(q)

    def merge(level, perm_row, part, own, out, then=lambda q: None):
        merge_with(fourth_of(level), perm_row, part, own, out, then)

    def perm_of(at, r):
        return perms[at, 0, r:r + 1]

    cost_part(0, 0, raw.at[0, 1], raw.at[0, 0], 1)
    merge(0, perm_of(0, 0), raw.at[0, 1], raw.at[0, 0], first.at[0])
    for s in range(2):
        arrived(raw.at[1, s, pl.ds(pl.multiple_of(my_rows, H), H)], SEM["z_raw"] + s)
    for q in range(8):
        rows = pl.ds(pl.multiple_of(far_rows + q * step, step), step)
        for e in range(2):
            for s in range(2):
                arrived(raw.at[1, s, rows, piece(e)], SEM["z_fwd"] + q * 4 + e * 2 + s)
    cost_part(1, 0, raw.at[1, 1], raw.at[1, 0], 1)
    merge(1, perm_of(1, 0), raw.at[1, 1], raw.at[1, 0], first.at[1])
    cost_part(2, 0, first.at[1], first.at[0], 1)

    def quad(k, at, r, own, slots, wait_rings, order, wait_opposite, tmp):
        level = 3 + k
        for q in range(4):
            wait_rings(q)
            cost_part(level, q, slots.at[0], own)
        onehot[...] = onehot_of(perm_of(at, r)).T
        merge(level, perm_of(0, r), slots.at[0], own, tmp.at[0])
        mine_e[k] = lax.dot_general(
            slots[2], tmp[0], (((1,), (1,)), ((), ())), preferred_element_type=jnp.float32)
        send(mine_e.at[k], near_e.at[k], SEM["seen"] + k, near)

        def sums(q):
            mine_p[k, rows4(q), pl.ds(0, N)] = lax.dot_general(
                slots[1, rows4(q)], slots[2], (((1,), (1,)), ((), ())), preferred_element_type=jnp.float32)
            mine_p[k, rows4(q), pl.ds(N, N)] = lax.dot_general(
                slots[1, rows4(q)], tmp[0], (((1,), (1,)), ((), ())), preferred_element_type=jnp.float32)
            send(mine_p.at[k, rows4(q)], near_p.at[k, rows4(q)], SEM["pair"] + 4 * k + q, near)

        def level_of(q):
            rows = rows4(q)
            arrived(near_p.at[k, rows], SEM["pair"] + 4 * k + q)
            cost = (mine_p[k, rows, pl.ds(0, N)] + near_p[k, rows, pl.ds(0, N)]) * (1.0 / math.sqrt(D))
            squared = cost * cost
            fourth = squared * squared
            mixing = (onehot[rows] + fourth * (0.5 / (1.0 + jnp.sum(fourth, axis=1, keepdims=True)))).astype(jnp.bfloat16)
            mix[1, rows] = mixing
            through = (jnp.dot(mixing, seen[0], preferred_element_type=jnp.float32)
                       + jnp.dot(mixing, seen[1], preferred_element_type=jnp.float32))
            direct = mine_p[k, rows, pl.ds(N, N)] + near_p[k, rows, pl.ds(N, N)]
            cost = (direct + through) * (1.0 / math.sqrt(2.0 * D))
            squared = cost * cost
            next_fourth[rows] = squared * squared
            mix_rows(1, rows, slots.at[2], slots.at[1], tmp.at[1])

        for e, q in enumerate(order):
            wait_opposite(q)
            sums(q)
            if e == 0:
                arrived(near_e.at[k], SEM["seen"] + k)
                both = mine_e[k] + near_e[k]
                seen[0] = both.astype(jnp.bfloat16)
                seen[1] = (both - seen[0].astype(jnp.float32)).astype(jnp.bfloat16)
            else:
                level_of(order[e - 1])
        level_of(order[-1])

    zq = got.at[pl.ds(0, 3)]

    def bit1(v):
        return (v // 2) % 2

    def send_z1(q):
        send(cur.at[0, rows4(q)], relay.at[0, rows4(q)], SEM["z1"] + q, z_next)
        send(cur.at[0, rows4(q)], relay.at[1, rows4(q)], SEM["z1"] + 4 + q, z_last)

    to_next, to_last = 2 * (1 - bit1((z + 1) % 8)), 2 * bit1((z + 7) % 8)
    from_last, from_next = 2 * (1 - bit1(z)), 2 * bit1(z)

    merge(2, perm_of(0, 1), first.at[1], first.at[0], cur.at[0], send_z1)
    for q in range(4):
        arrived(relay.at[0, rows4(q)], SEM["z1"] + q)
        send(relay.at[0, rows4(q)], zq.at[to_next, rows4(q)], SEM["z2"] + q, z_next)
        arrived(relay.at[1, rows4(q)], SEM["z1"] + 4 + q)
        send(relay.at[1, rows4(q)], zq.at[to_last, rows4(q)], SEM["z2"] + 4 + q, z_last)

    def rings_z(q):
        arrived(zq.at[from_last, rows4(q)], SEM["z2"] + q)
        if q < 2:
            send(zq.at[from_last, rows4(q)], relay_half.at[0, rows4(q)], SEM["z3"] + q, z_next)
        arrived(zq.at[from_next, rows4(q)], SEM["z2"] + 4 + q)
        if q >= 2:
            send(zq.at[from_next, rows4(q)], relay_half.at[1, rows4(q - 2)], SEM["z3"] + q, z_last)

    def opposite_z(q):
        if q == 0:
            for e in (0, 2, 1, 3):
                side, there = (0, z_next) if e < 2 else (1, z_last)
                arrived(relay_half.at[side, rows4(e % 2)], SEM["z3"] + e)
                send(relay_half.at[side, rows4(e % 2)], zq.at[1, rows4(e)], SEM["z4"] + e, there)
        arrived(zq.at[1, rows4(q)], SEM["z4"] + q)

    def send_x1(q):
        send(cur.at[1, rows4(q)], xq.at[2 * (x % 2), rows4(q)], SEM["x1"] + q, x_next)
        send(cur.at[1, rows4(q)], xq.at[2 * (1 - x % 2), rows4(q)], SEM["x1"] + 4 + q, x_last)

    xq = got.at[pl.ds(3, 3)]
    quad(0, 2, 2, cur.at[0], zq, rings_z, (0, 2, 1, 3), opposite_z, first.at[pl.ds(2, 2)])
    merge_with(next_fourth[...], perm_of(0, 3), first.at[3], first.at[2], cur.at[1], send_x1)

    def rings_x(q):
        arrived(xq.at[2 * (1 - x % 2), rows4(q)], SEM["x1"] + q)
        if q < 2:
            send(xq.at[2 * (1 - x % 2), rows4(q)], xq.at[1, rows4(q)], SEM["x2"] + q, x_next)
        arrived(xq.at[2 * (x % 2), rows4(q)], SEM["x1"] + 4 + q)
        if q >= 2:
            send(xq.at[2 * (x % 2), rows4(q)], xq.at[1, rows4(q)], SEM["x2"] + q, x_last)

    def opposite_x(q):
        arrived(xq.at[1, rows4(q)], SEM["x2"] + q)

    quad(1, 3, 4, cur.at[1], xq, rings_x, (0, 2, 1, 3), opposite_x, first.at[pl.ds(4, 2)])

    yq = got.at[pl.ds(6, 3)]
    o_cols = pl.ds(pl.multiple_of(g * F, F), F)

    @pl.when(inner == 0)
    def _():
        outer_sends = []
        def send_y1(q):
            copy = pltpu.make_async_remote_copy(
                src_ref=cur.at[2, rows4(q)], dst_ref=yq.at[0, rows4(q)], send_sem=ssem.at[SEM["y1"] + q],
                recv_sem=rsem.at[SEM["y1"] + q], device_id=same[Y0], device_id_type=MESH)
            copy.start()
            outer_sends.append(copy)

        merge_with(next_fourth[...], perm_of(0, 5), first.at[5], first.at[4], cur.at[2], send_y1)
        for c in range(2):
            arrived(o_ref.at[0, :, half(c)], SEM["out"] + c)
        for copy in outer_sends:
            copy.wait_send()

    @pl.when(inner == 1)
    def _():
        before = len(sent)

        def send_y2(q):
            send(cur.at[2, rows4(q)], yq.at[2, rows4(q)], SEM["y2"] + q, y_cross)

        merge_with(next_fourth[...], perm_of(0, 5), first.at[5], first.at[4], cur.at[2], send_y2)

        def rings_y(q):
            arrived(yq.at[0, rows4(q)], SEM["y1"] + q)
            send(yq.at[0, rows4(q)], yq.at[1, rows4(q)], SEM["y3"] + q, y_cross)
            arrived(yq.at[2, rows4(q)], SEM["y2"] + q)

        def opposite_y(q):
            arrived(yq.at[1, rows4(q)], SEM["y3"] + q)

        quad(2, 4, 6, cur.at[2], yq, rings_y, (0, 1, 2, 3), opposite_y, first.at[pl.ds(6, 2)])
        ours, theirs = first.at[6], first.at[7]

        def away(src, rows, at, device):
            copy = pltpu.make_async_remote_copy(
                src_ref=src.at[pl.ds(pl.multiple_of(rows, H), H)], dst_ref=o_ref.at[0, :, o_cols],
                send_sem=ssem.at[SEM["away"] + at], recv_sem=rsem.at[SEM["out"] + g],
                device_id=device, device_id_type=MESH)
            copy.start()
            return copy

        fourth = next_fourth[...]
        mixing_of(fourth, perm_of(0, 7))
        leaving = []
        far_half, my_half = pl.ds(pl.multiple_of(far_rows, H), H), pl.ds(pl.multiple_of(my_rows, H), H)
        mix_rows(0, far_half, theirs, ours, cur.at[3])
        leaving.append(away(cur.at[3], far_rows, 0, (core(rep, h), far)))
        scale = 0.5 / (1.0 + jnp.sum(fourth, axis=1, keepdims=True))
        mix[1] = (onehot_of(perm_of(4, 7)).T + fourth * scale).astype(jnp.bfloat16)
        mix_rows(1, far_half, ours, theirs, cur.at[4])
        leaving.append(away(cur.at[4], far_rows, 2, (core(chip[Y1], h), far)))
        mix_rows(1, my_half, ours, theirs, cur.at[4])
        leaving.append(away(cur.at[4], my_rows, 1, (core(chip[Y1], h), h)))
        mix_rows(0, my_half, theirs, ours, cur.at[3])

        @pl.when(slot == 0)
        def _():
            home = pltpu.make_async_copy(
                cur.at[3, pl.ds(pl.multiple_of(my_rows, H), H)], o_ref.at[0, :, o_cols], lsem.at[2])
            home.start()
            home.wait()
            arrived(o_ref.at[0, :, pl.ds(pl.multiple_of((1 - g) * F, F), F)], SEM["out"] + 1 - g)

        @pl.when(slot == 1)
        def _():
            home = away(cur.at[3], my_rows, 3, near)
            for c in range(2):
                arrived(o_ref.at[0, :, half(c)], SEM["out"] + c)
            home.wait_send()

        for copy in leaving + sent[before:]:
            copy.wait_send()
        del sent[before:]

    for copy in sent:
        copy.wait_send()


def local(weights, perms):
    rows = (N, F)
    return pl.pallas_call(
        kernel,
        out_shape=jax.ShapeDtypeStruct((1, H, D), jnp.bfloat16),
        in_specs=[pl.BlockSpec(memory_space=pl.ANY), pl.BlockSpec(memory_space=pl.ANY)],
        out_specs=pl.BlockSpec(memory_space=pl.ANY),
        scratch_shapes=[
            pltpu.VMEM((H, D), jnp.bfloat16),
            pltpu.VMEM((5, 2, 8, N), jnp.int32),
            pltpu.VMEM((2, 2, *rows), jnp.bfloat16),
            pltpu.VMEM((8, *rows), jnp.bfloat16),
            pltpu.VMEM((5, *rows), jnp.bfloat16),
            pltpu.VMEM((9, *rows), jnp.bfloat16),
            pltpu.VMEM((2, *rows), jnp.bfloat16),
            pltpu.VMEM((2, H, F), jnp.bfloat16),
            pltpu.VMEM((6, N, N), jnp.float32),
            pltpu.VMEM((6, N, N), jnp.float32),
            pltpu.VMEM((3, N, 2 * N), jnp.float32),
            pltpu.VMEM((3, N, 2 * N), jnp.float32),
            pltpu.VMEM((3, N, N), jnp.float32),
            pltpu.VMEM((3, N, N), jnp.float32),
            pltpu.VMEM((2, N, N), jnp.bfloat16),
            pltpu.VMEM((N, N), jnp.float32),
            pltpu.VMEM((N, N), jnp.float32),
            pltpu.VMEM((2, N, N), jnp.bfloat16),
            pltpu.SemaphoreType.DMA((N_SEM,)),
            pltpu.SemaphoreType.DMA((N_SEM,)),
            pltpu.SemaphoreType.DMA((4,)),
        ],
        compiler_params=pltpu.CompilerParams(
            collective_id=0, has_side_effects=True, vmem_limit_bytes=60 * 1024 * 1024),
    )(weights, perms)


def solution(mesh):
    placed = (P("rep", "slab", None), P("rep", None, None))
    return jax.shard_map(
        local, mesh=mesh, in_specs=placed, out_specs=P("rep", "slab", None), check_vma=False
    )
```

```python
import functools
import math

import jax
import jax.numpy as jnp
from jax import lax
from jax.experimental import pallas as pl
from jax.experimental.pallas import tpu as pltpu
from jax.sharding import PartitionSpec as P

D = 3072
N = 256
H = N // 2
F = D // 2
MESH = pl.DeviceIdType.MESH
NEAR, Z0, Z1, Z2, X0, X1, Y0, Y1 = range(8)


def layout(counts):
    at, out = 0, {}
    for name, count in counts:
        out[name] = at
        at += count
    return out, at


SEM, N_SEM = layout([
    ("near_raw", 1), ("in", 32), ("z_raw", 2), ("z_fwd", 32), ("perm", 10),
    ("z1", 8), ("z2", 8), ("z3", 4), ("z4", 4), ("x1", 8), ("x2", 4), ("y1", 4), ("y2", 4), ("y3", 4), ("out", 2), ("away", 4),
    ("cost", 6 * 4), ("pair", 3 * 4), ("seen", 3),
])


def kernel(w_hbm, p_hbm, o_ref, wv, perms, raw, first, cur, got, relay, relay_half, mine_g, near_g, mine_p, near_p, mine_e, near_e, seen, next_fourth, onehot, mix, ssem, rsem, lsem):
    rep, h = lax.axis_index("rep"), lax.axis_index("slab")
    g = rep % 2
    far = 1 - h

    def flip(bit):
        return rep + (1 << bit) * (1 - 2 * ((rep // (1 << bit)) % 2))

    def core(base, c):
        return base - g + c

    def xor(a, b):
        return a + b - 2 * a * b

    near = (flip(0), h)
    chip = [flip(b) for b in range(8)]
    same = [(chip[b], h) for b in range(8)]

    load = pltpu.make_async_copy(w_hbm.at[0], wv, lsem.at[0])
    load.start()
    slot = g + h - 2 * g * h
    load_perms = pltpu.make_async_copy(p_hbm.at[0], perms.at[0, slot], lsem.at[3])
    load_perms.start()

    z, x = (rep // 2) % 8, (rep // 16) % 4
    z_next, z_last = (rep + 2 * ((z + 1) % 8 - z), h), (rep + 2 * ((z + 7) % 8 - z), h)
    x_next, x_last = (rep + 16 * ((x + 1) % 4 - x), h), (rep + 16 * ((x + 3) % 4 - x), h)

    y = (rep // 64) % 4
    inner = ((y + 1) // 2) % 2
    y_cross = (rep + 64 * (3 - 2 * y), h)
    peers = [near, z_next, z_last, x_next, x_last, same[Y0], y_cross]
    for c in range(2):
        peers.append((core(rep, c), far))
        peers.append((core(chip[Y1], c), far))
        for b in (Z0, Z2, X1, Y1):
            peers.append((core(chip[b], c), h))
    barrier = pltpu.get_barrier_semaphore()
    for peer in peers:
        pl.semaphore_signal(barrier, inc=1, device_id=peer, device_id_type=MESH)
    pl.semaphore_wait(barrier, len(peers))

    sent = []

    def send(src, dst, sem, device):
        copy = pltpu.make_async_remote_copy(
            src_ref=src, dst_ref=dst, send_sem=ssem.at[sem], recv_sem=rsem.at[sem],
            device_id=device, device_id_type=MESH,
        )
        copy.start()
        sent.append(copy)

    def arrived(dst, sem):
        pltpu.make_async_remote_copy(
            src_ref=dst, dst_ref=dst, send_sem=ssem.at[0], recv_sem=rsem.at[sem],
            device_id=near, device_id_type=MESH,
        ).wait_recv()

    def half(c):
        return pl.ds(c * F, F)

    far_slot = xor(g, far)
    my_rows, far_rows = h * H, far * H
    step = H // 8

    load.wait()
    keep = pltpu.make_async_copy(
        wv.at[:, pl.ds(pl.multiple_of(g * F, F), F)],
        raw.at[0, slot, pl.ds(pl.multiple_of(my_rows, H), H)], lsem.at[1])
    keep.start()

    def piece(e):
        return pl.ds(e * (F // 2), F // 2)

    def send_in(q, e, c):
        src = wv.at[pl.ds(q * step, step), pl.ds(c * F + e * (F // 2), F // 2)]
        dst = raw.at[0, far_slot, pl.ds(pl.multiple_of(my_rows + q * step, step), step), piece(e)]
        copy = pltpu.make_async_remote_copy(
            src_ref=src, dst_ref=dst, send_sem=ssem.at[SEM["in"] + q * 4 + e * 2 + c],
            recv_sem=rsem.at[SEM["in"] + q * 4 + e * 2 + far_slot],
            device_id=(core(rep, c), far), device_id_type=MESH)
        copy.start()
        sent.append(copy)

    for q in range(8):
        for e in range(2):
            for c in range(2):
                send_in(q, e, c)
    for c in range(2):
        copy = pltpu.make_async_remote_copy(
            src_ref=wv.at[:, half(c)],
            dst_ref=raw.at[1, slot, pl.ds(pl.multiple_of(my_rows, H), H)],
            send_sem=ssem.at[SEM["z_raw"] + c], recv_sem=rsem.at[SEM["z_raw"] + slot],
            device_id=(core(chip[Z0], c), h), device_id_type=MESH)
        copy.start()
        sent.append(copy)
    send(wv.at[:, pl.ds(pl.multiple_of((1 - g) * F, F), F)],
         raw.at[0, slot, pl.ds(pl.multiple_of(my_rows, H), H)], SEM["near_raw"], near)

    load_perms.wait()
    perm_to = [(0, near, 0)]
    for at, b in ((1, Z0), (2, Z2), (3, X1), (4, Y1)):
        for c in range(2):
            perm_to.append((at, (core(chip[b], c), h), c))
    for at, device, c in perm_to:
        copy = pltpu.make_async_remote_copy(
            src_ref=perms.at[0, slot], dst_ref=perms.at[at, slot],
            send_sem=ssem.at[SEM["perm"] + at * 2 + c], recv_sem=rsem.at[SEM["perm"] + at * 2 + slot],
            device_id=device, device_id_type=MESH)
        copy.start()
        sent.append(copy)

    for q in range(8):
        rows = pl.ds(pl.multiple_of(far_rows + q * step, step), step)
        for e in range(2):
            for s in range(2):
                at = q * 4 + e * 2 + s
                arrived(raw.at[0, s, rows, piece(e)], SEM["in"] + at)
                send(raw.at[0, s, rows, piece(e)], raw.at[1, s, rows, piece(e)], SEM["z_fwd"] + at, same[Z0])

    keep.wait()
    arrived(raw.at[0, 1 - slot, pl.ds(pl.multiple_of(my_rows, H), H)], SEM["near_raw"])
    arrived(perms.at[0, 1 - slot], SEM["perm"] + (1 - slot))
    for at in range(1, 5):
        for s in range(2):
            arrived(perms.at[at, s], SEM["perm"] + at * 2 + s)

    Q = N // 4

    def rows4(q):
        return pl.ds(q * Q, Q)

    pieces = {}

    def cost_part(level, q, part, own, parts=4):
        pieces[level] = parts
        rows = pl.ds(q * (N // parts), N // parts)
        mine_g[level, rows] = lax.dot_general(
            part[rows], own[...], (((1,), (1,)), ((), ())), preferred_element_type=jnp.float32)
        send(mine_g.at[level, rows], near_g.at[level, rows], SEM["cost"] + level * 4 + q, near)

    def fourth_of(level):
        parts = pieces[level]
        for q in range(parts):
            arrived(near_g.at[level, pl.ds(q * (N // parts), N // parts)], SEM["cost"] + level * 4 + q)
        cost = (mine_g[level] + near_g[level]) * (1.0 / math.sqrt(D))
        squared = cost * cost
        return squared * squared

    def onehot_of(perm_row):
        neuron = lax.broadcasted_iota(jnp.int32, (N, N), 0)
        return jnp.where(neuron == perm_row, 0.5, 0.0)

    def mixing_of(fourth, perm_row):
        scale = 0.5 / (1.0 + jnp.sum(fourth, axis=0, keepdims=True))
        mix[0] = (onehot_of(perm_row) + fourth * scale).T.astype(jnp.bfloat16)

    def rows2(q):
        return pl.ds(q * H, H)

    def mix_rows(at, rows, part, own, out):
        for t in range(F // N):
            tile = pl.ds(t * N, N)
            aligned = jnp.dot(mix[at, rows], part[:, tile], preferred_element_type=jnp.float32)
            out[rows, tile] = (
                (own[rows, tile].astype(jnp.float32) + aligned) * (1.0 / math.sqrt(2.0))).astype(jnp.bfloat16)

    def merge_with(fourth, perm_row, part, own, out, then=lambda q: None):
        mixing_of(fourth, perm_row)
        for first_piece, count in ((0, 1), (1, 1), (2, 2)):
            mix_rows(0, pl.ds(first_piece * Q, count * Q), part, own, out)
            for q in range(first_piece, first_piece + count):
                then(q)

    def merge(level, perm_row, part, own, out, then=lambda q: None):
        merge_with(fourth_of(level), perm_row, part, own, out, then)

    def perm_of(at, r):
        return perms[at, 0, r:r + 1]

    cost_part(0, 0, raw.at[0, 1], raw.at[0, 0], 1)
    merge(0, perm_of(0, 0), raw.at[0, 1], raw.at[0, 0], first.at[0])
    for s in range(2):
        arrived(raw.at[1, s, pl.ds(pl.multiple_of(my_rows, H), H)], SEM["z_raw"] + s)
    for q in range(8):
        rows = pl.ds(pl.multiple_of(far_rows + q * step, step), step)
        for e in range(2):
            for s in range(2):
                arrived(raw.at[1, s, rows, piece(e)], SEM["z_fwd"] + q * 4 + e * 2 + s)
    cost_part(1, 0, raw.at[1, 1], raw.at[1, 0], 1)
    merge(1, perm_of(1, 0), raw.at[1, 1], raw.at[1, 0], first.at[1])
    cost_part(2, 0, first.at[1], first.at[0], 1)

    def quad(k, at, r, own, slots, wait_rings, order, wait_opposite, tmp):
        level = 3 + k
        for q in range(4):
            wait_rings(q)
            cost_part(level, q, slots.at[0], own)
        onehot[...] = onehot_of(perm_of(at, r)).T
        merge(level, perm_of(0, r), slots.at[0], own, tmp.at[0])
        mine_e[k] = lax.dot_general(
            slots[2], tmp[0], (((1,), (1,)), ((), ())), preferred_element_type=jnp.float32)
        send(mine_e.at[k], near_e.at[k], SEM["seen"] + k, near)

        def sums(q):
            mine_p[k, rows4(q), pl.ds(0, N)] = lax.dot_general(
                slots[1, rows4(q)], slots[2], (((1,), (1,)), ((), ())), preferred_element_type=jnp.float32)
            mine_p[k, rows4(q), pl.ds(N, N)] = lax.dot_general(
                slots[1, rows4(q)], tmp[0], (((1,), (1,)), ((), ())), preferred_element_type=jnp.float32)
            send(mine_p.at[k, rows4(q)], near_p.at[k, rows4(q)], SEM["pair"] + 4 * k + q, near)

        def level_of(q):
            rows = rows4(q)
            arrived(near_p.at[k, rows], SEM["pair"] + 4 * k + q)
            cost = (mine_p[k, rows, pl.ds(0, N)] + near_p[k, rows, pl.ds(0, N)]) * (1.0 / math.sqrt(D))
            squared = cost * cost
            fourth = squared * squared
            mixing = (onehot[rows] + fourth * (0.5 / (1.0 + jnp.sum(fourth, axis=1, keepdims=True)))).astype(jnp.bfloat16)
            mix[1, rows] = mixing
            through = (jnp.dot(mixing, seen[0], preferred_element_type=jnp.float32)
                       + jnp.dot(mixing, seen[1], preferred_element_type=jnp.float32))
            direct = mine_p[k, rows, pl.ds(N, N)] + near_p[k, rows, pl.ds(N, N)]
            cost = (direct + through) * (1.0 / math.sqrt(2.0 * D))
            squared = cost * cost
            next_fourth[rows] = squared * squared
            mix_rows(1, rows, slots.at[2], slots.at[1], tmp.at[1])

        for e, q in enumerate(order):
            wait_opposite(q)
            sums(q)
            if e == 0:
                arrived(near_e.at[k], SEM["seen"] + k)
                both = mine_e[k] + near_e[k]
                seen[0] = both.astype(jnp.bfloat16)
                seen[1] = (both - seen[0].astype(jnp.float32)).astype(jnp.bfloat16)
            else:
                level_of(order[e - 1])
        level_of(order[-1])

    zq = got.at[pl.ds(0, 3)]

    def bit1(v):
        return (v // 2) % 2

    def send_z1(q):
        send(cur.at[0, rows4(q)], relay.at[0, rows4(q)], SEM["z1"] + q, z_next)
        send(cur.at[0, rows4(q)], relay.at[1, rows4(q)], SEM["z1"] + 4 + q, z_last)

    to_next, to_last = 2 * (1 - bit1((z + 1) % 8)), 2 * bit1((z + 7) % 8)
    from_last, from_next = 2 * (1 - bit1(z)), 2 * bit1(z)

    merge(2, perm_of(0, 1), first.at[1], first.at[0], cur.at[0], send_z1)
    for q in range(4):
        arrived(relay.at[0, rows4(q)], SEM["z1"] + q)
        send(relay.at[0, rows4(q)], zq.at[to_next, rows4(q)], SEM["z2"] + q, z_next)
        arrived(relay.at[1, rows4(q)], SEM["z1"] + 4 + q)
        send(relay.at[1, rows4(q)], zq.at[to_last, rows4(q)], SEM["z2"] + 4 + q, z_last)

    def rings_z(q):
        arrived(zq.at[from_last, rows4(q)], SEM["z2"] + q)
        if q < 2:
            send(zq.at[from_last, rows4(q)], relay_half.at[0, rows4(q)], SEM["z3"] + q, z_next)
        arrived(zq.at[from_next, rows4(q)], SEM["z2"] + 4 + q)
        if q >= 2:
            send(zq.at[from_next, rows4(q)], relay_half.at[1, rows4(q - 2)], SEM["z3"] + q, z_last)

    def opposite_z(q):
        if q == 0:
            for e in (0, 2, 1, 3):
                side, there = (0, z_next) if e < 2 else (1, z_last)
                arrived(relay_half.at[side, rows4(e % 2)], SEM["z3"] + e)
                send(relay_half.at[side, rows4(e % 2)], zq.at[1, rows4(e)], SEM["z4"] + e, there)
        arrived(zq.at[1, rows4(q)], SEM["z4"] + q)

    def send_x1(q):
        send(cur.at[1, rows4(q)], xq.at[2 * (x % 2), rows4(q)], SEM["x1"] + q, x_next)
        send(cur.at[1, rows4(q)], xq.at[2 * (1 - x % 2), rows4(q)], SEM["x1"] + 4 + q, x_last)

    xq = got.at[pl.ds(3, 3)]
    quad(0, 2, 2, cur.at[0], zq, rings_z, (0, 2, 1, 3), opposite_z, first.at[pl.ds(2, 2)])
    merge_with(next_fourth[...], perm_of(0, 3), first.at[3], first.at[2], cur.at[1], send_x1)

    def rings_x(q):
        arrived(xq.at[2 * (1 - x % 2), rows4(q)], SEM["x1"] + q)
        if q < 2:
            send(xq.at[2 * (1 - x % 2), rows4(q)], xq.at[1, rows4(q)], SEM["x2"] + q, x_next)
        arrived(xq.at[2 * (x % 2), rows4(q)], SEM["x1"] + 4 + q)
        if q >= 2:
            send(xq.at[2 * (x % 2), rows4(q)], xq.at[1, rows4(q)], SEM["x2"] + q, x_last)

    def opposite_x(q):
        arrived(xq.at[1, rows4(q)], SEM["x2"] + q)

    quad(1, 3, 4, cur.at[1], xq, rings_x, (0, 2, 1, 3), opposite_x, first.at[pl.ds(4, 2)])

    yq = got.at[pl.ds(6, 3)]
    o_cols = pl.ds(pl.multiple_of(g * F, F), F)

    @pl.when(inner == 0)
    def _():
        outer_sends = []
        def send_y1(q):
            copy = pltpu.make_async_remote_copy(
                src_ref=cur.at[2, rows4(q)], dst_ref=yq.at[0, rows4(q)], send_sem=ssem.at[SEM["y1"] + q],
                recv_sem=rsem.at[SEM["y1"] + q], device_id=same[Y0], device_id_type=MESH)
            copy.start()
            outer_sends.append(copy)

        merge_with(next_fourth[...], perm_of(0, 5), first.at[5], first.at[4], cur.at[2], send_y1)
        for c in range(2):
            arrived(o_ref.at[0, :, half(c)], SEM["out"] + c)
        for copy in outer_sends:
            copy.wait_send()

    @pl.when(inner == 1)
    def _():
        before = len(sent)

        def send_y2(q):
            send(cur.at[2, rows4(q)], yq.at[2, rows4(q)], SEM["y2"] + q, y_cross)

        merge_with(next_fourth[...], perm_of(0, 5), first.at[5], first.at[4], cur.at[2], send_y2)

        def rings_y(q):
            arrived(yq.at[0, rows4(q)], SEM["y1"] + q)
            send(yq.at[0, rows4(q)], yq.at[1, rows4(q)], SEM["y3"] + q, y_cross)
            arrived(yq.at[2, rows4(q)], SEM["y2"] + q)

        def opposite_y(q):
            arrived(yq.at[1, rows4(q)], SEM["y3"] + q)

        quad(2, 4, 6, cur.at[2], yq, rings_y, (0, 1, 2, 3), opposite_y, first.at[pl.ds(6, 2)])
        ours, theirs = first.at[6], first.at[7]

        def away(src, rows, at, device):
            copy = pltpu.make_async_remote_copy(
                src_ref=src.at[pl.ds(pl.multiple_of(rows, H), H)], dst_ref=o_ref.at[0, :, o_cols],
                send_sem=ssem.at[SEM["away"] + at], recv_sem=rsem.at[SEM["out"] + g],
                device_id=device, device_id_type=MESH)
            return copy

        fourth = next_fourth[...]
        mixing_of(fourth, perm_of(0, 7))
        far_half, my_half = pl.ds(pl.multiple_of(far_rows, H), H), pl.ds(pl.multiple_of(my_rows, H), H)
        ours_far = away(cur.at[3], far_rows, 0, (core(rep, h), far))
        theirs_far = away(cur.at[4], far_rows, 2, (core(chip[Y1], h), far))
        theirs_near = away(cur.at[4], my_rows, 1, (core(chip[Y1], h), h))
        ours_near = away(cur.at[3], my_rows, 3, near)
        mix_rows(0, far_half, theirs, ours, cur.at[3])
        ours_far.start()
        scale = 0.5 / (1.0 + jnp.sum(fourth, axis=1, keepdims=True))
        mix[1] = (onehot_of(perm_of(4, 7)).T + fourth * scale).astype(jnp.bfloat16)
        mix_rows(1, far_half, ours, theirs, cur.at[4])
        theirs_far.start()
        mix_rows(0, my_half, theirs, ours, cur.at[3])

        @pl.when(slot == 0)
        def _():
            home = pltpu.make_async_copy(cur.at[3, my_half], o_ref.at[0, :, o_cols], lsem.at[2])
            home.start()
            home.wait()

        @pl.when(slot == 1)
        def _():
            ours_near.start()

        mix_rows(1, my_half, ours, theirs, cur.at[4])
        ours_far.wait_send()
        theirs_far.wait_send()
        theirs_near.start()

        @pl.when(slot == 0)
        def _():
            arrived(o_ref.at[0, :, pl.ds(pl.multiple_of((1 - g) * F, F), F)], SEM["out"] + 1 - g)

        @pl.when(slot == 1)
        def _():
            for c in range(2):
                arrived(o_ref.at[0, :, half(c)], SEM["out"] + c)
            ours_near.wait_send()

        leaving = [theirs_near]
        for copy in leaving + sent[before:]:
            copy.wait_send()
        del sent[before:]

    for copy in sent:
        copy.wait_send()


def local(weights, perms):
    rows = (N, F)
    return pl.pallas_call(
        kernel,
        out_shape=jax.ShapeDtypeStruct((1, H, D), jnp.bfloat16),
        in_specs=[pl.BlockSpec(memory_space=pl.ANY), pl.BlockSpec(memory_space=pl.ANY)],
        out_specs=pl.BlockSpec(memory_space=pl.ANY),
        scratch_shapes=[
            pltpu.VMEM((H, D), jnp.bfloat16),
            pltpu.VMEM((5, 2, 8, N), jnp.int32),
            pltpu.VMEM((2, 2, *rows), jnp.bfloat16),
            pltpu.VMEM((8, *rows), jnp.bfloat16),
            pltpu.VMEM((5, *rows), jnp.bfloat16),
            pltpu.VMEM((9, *rows), jnp.bfloat16),
            pltpu.VMEM((2, *rows), jnp.bfloat16),
            pltpu.VMEM((2, H, F), jnp.bfloat16),
            pltpu.VMEM((6, N, N), jnp.float32),
            pltpu.VMEM((6, N, N), jnp.float32),
            pltpu.VMEM((3, N, 2 * N), jnp.float32),
            pltpu.VMEM((3, N, 2 * N), jnp.float32),
            pltpu.VMEM((3, N, N), jnp.float32),
            pltpu.VMEM((3, N, N), jnp.float32),
            pltpu.VMEM((2, N, N), jnp.bfloat16),
            pltpu.VMEM((N, N), jnp.float32),
            pltpu.VMEM((N, N), jnp.float32),
            pltpu.VMEM((2, N, N), jnp.bfloat16),
            pltpu.SemaphoreType.DMA((N_SEM,)),
            pltpu.SemaphoreType.DMA((N_SEM,)),
            pltpu.SemaphoreType.DMA((4,)),
        ],
        compiler_params=pltpu.CompilerParams(
            collective_id=0, has_side_effects=True, vmem_limit_bytes=60 * 1024 * 1024),
    )(weights, perms)


def solution(mesh):
    placed = (P("rep", "slab", None), P("rep", None, None))
    return jax.shard_map(
        local, mesh=mesh, in_specs=placed, out_specs=P("rep", "slab", None), check_vma=False
    )
```

```python
import functools
import math

import jax
import jax.numpy as jnp
from jax import lax
from jax.experimental import pallas as pl
from jax.experimental.pallas import tpu as pltpu
from jax.sharding import PartitionSpec as P

D = 3072
N = 256
H = N // 2
F = D // 2
MESH = pl.DeviceIdType.MESH
NEAR, Z0, Z1, Z2, X0, X1, Y0, Y1 = range(8)


def layout(counts):
    at, out = 0, {}
    for name, count in counts:
        out[name] = at
        at += count
    return out, at


SEM, N_SEM = layout([
    ("near_raw", 1), ("in", 32), ("z_raw", 2), ("z_fwd", 32), ("perm", 10),
    ("z1", 8), ("z2", 8), ("z3", 4), ("z4", 4), ("x1", 8), ("x2", 4), ("y1", 4), ("y2", 4), ("y3", 4), ("out", 2), ("away", 4),
    ("cost", 6 * 4), ("pair", 3 * 4), ("seen", 3),
])


def kernel(w_hbm, p_hbm, o_ref, wv, perms, raw, first, cur, got, relay, relay_half, mine_g, near_g, mine_p, near_p, mine_e, near_e, seen, next_fourth, onehot, mix, ssem, rsem, lsem):
    rep, h = lax.axis_index("rep"), lax.axis_index("slab")
    g = rep % 2
    far = 1 - h

    def flip(bit):
        return rep + (1 << bit) * (1 - 2 * ((rep // (1 << bit)) % 2))

    def core(base, c):
        return base - g + c

    def xor(a, b):
        return a + b - 2 * a * b

    near = (flip(0), h)
    chip = [flip(b) for b in range(8)]
    same = [(chip[b], h) for b in range(8)]

    load = pltpu.make_async_copy(w_hbm.at[0], wv, lsem.at[0])
    load.start()
    slot = g + h - 2 * g * h
    load_perms = pltpu.make_async_copy(p_hbm.at[0], perms.at[0, slot], lsem.at[3])
    load_perms.start()

    z, x = (rep // 2) % 8, (rep // 16) % 4
    z_next, z_last = (rep + 2 * ((z + 1) % 8 - z), h), (rep + 2 * ((z + 7) % 8 - z), h)
    x_next, x_last = (rep + 16 * ((x + 1) % 4 - x), h), (rep + 16 * ((x + 3) % 4 - x), h)

    y = (rep // 64) % 4
    inner = ((y + 1) // 2) % 2
    y_cross = (rep + 64 * (3 - 2 * y), h)
    peers = [near, z_next, z_last, x_next, x_last, same[Y0], y_cross]
    for c in range(2):
        peers.append((core(rep, c), far))
        peers.append((core(chip[Y1], c), far))
        for b in (Z0, Z2, X1, Y1):
            peers.append((core(chip[b], c), h))
    barrier = pltpu.get_barrier_semaphore()
    for peer in peers:
        pl.semaphore_signal(barrier, inc=1, device_id=peer, device_id_type=MESH)
    pl.semaphore_wait(barrier, len(peers))

    sent = []

    def send(src, dst, sem, device):
        copy = pltpu.make_async_remote_copy(
            src_ref=src, dst_ref=dst, send_sem=ssem.at[sem], recv_sem=rsem.at[sem],
            device_id=device, device_id_type=MESH,
        )
        copy.start()
        sent.append(copy)

    def arrived(dst, sem):
        pltpu.make_async_remote_copy(
            src_ref=dst, dst_ref=dst, send_sem=ssem.at[0], recv_sem=rsem.at[sem],
            device_id=near, device_id_type=MESH,
        ).wait_recv()

    def half(c):
        return pl.ds(c * F, F)

    far_slot = xor(g, far)
    my_rows, far_rows = h * H, far * H
    step = H // 8

    load.wait()
    keep = pltpu.make_async_copy(
        wv.at[:, pl.ds(pl.multiple_of(g * F, F), F)],
        raw.at[0, slot, pl.ds(pl.multiple_of(my_rows, H), H)], lsem.at[1])
    keep.start()

    def piece(e):
        return pl.ds(e * (F // 2), F // 2)

    def send_in(q, e, c):
        src = wv.at[pl.ds(q * step, step), pl.ds(c * F + e * (F // 2), F // 2)]
        dst = raw.at[0, far_slot, pl.ds(pl.multiple_of(my_rows + q * step, step), step), piece(e)]
        copy = pltpu.make_async_remote_copy(
            src_ref=src, dst_ref=dst, send_sem=ssem.at[SEM["in"] + q * 4 + e * 2 + c],
            recv_sem=rsem.at[SEM["in"] + q * 4 + e * 2 + far_slot],
            device_id=(core(rep, c), far), device_id_type=MESH)
        copy.start()
        sent.append(copy)

    for q in range(8):
        for e in range(2):
            for c in range(2):
                send_in(q, e, c)
    for c in range(2):
        copy = pltpu.make_async_remote_copy(
            src_ref=wv.at[:, half(c)],
            dst_ref=raw.at[1, slot, pl.ds(pl.multiple_of(my_rows, H), H)],
            send_sem=ssem.at[SEM["z_raw"] + c], recv_sem=rsem.at[SEM["z_raw"] + slot],
            device_id=(core(chip[Z0], c), h), device_id_type=MESH)
        copy.start()
        sent.append(copy)
    send(wv.at[:, pl.ds(pl.multiple_of((1 - g) * F, F), F)],
         raw.at[0, slot, pl.ds(pl.multiple_of(my_rows, H), H)], SEM["near_raw"], near)

    load_perms.wait()
    perm_to = [(0, near, 0)]
    for at, b in ((1, Z0), (2, Z2), (3, X1), (4, Y1)):
        for c in range(2):
            perm_to.append((at, (core(chip[b], c), h), c))
    for at, device, c in perm_to:
        copy = pltpu.make_async_remote_copy(
            src_ref=perms.at[0, slot], dst_ref=perms.at[at, slot],
            send_sem=ssem.at[SEM["perm"] + at * 2 + c], recv_sem=rsem.at[SEM["perm"] + at * 2 + slot],
            device_id=device, device_id_type=MESH)
        copy.start()
        sent.append(copy)

    for q in range(8):
        rows = pl.ds(pl.multiple_of(far_rows + q * step, step), step)
        for e in range(2):
            for s in range(2):
                at = q * 4 + e * 2 + s
                arrived(raw.at[0, s, rows, piece(e)], SEM["in"] + at)
                send(raw.at[0, s, rows, piece(e)], raw.at[1, s, rows, piece(e)], SEM["z_fwd"] + at, same[Z0])

    keep.wait()
    arrived(raw.at[0, 1 - slot, pl.ds(pl.multiple_of(my_rows, H), H)], SEM["near_raw"])
    arrived(perms.at[0, 1 - slot], SEM["perm"] + (1 - slot))
    for at in range(1, 5):
        for s in range(2):
            arrived(perms.at[at, s], SEM["perm"] + at * 2 + s)

    Q = N // 4

    def rows4(q):
        return pl.ds(q * Q, Q)

    pieces = {}

    def cost_part(level, q, part, own, parts=4):
        pieces[level] = parts
        rows = pl.ds(q * (N // parts), N // parts)
        mine_g[level, rows] = lax.dot_general(
            part[rows], own[...], (((1,), (1,)), ((), ())), preferred_element_type=jnp.float32)
        send(mine_g.at[level, rows], near_g.at[level, rows], SEM["cost"] + level * 4 + q, near)

    def fourth_of(level):
        parts = pieces[level]
        for q in range(parts):
            arrived(near_g.at[level, pl.ds(q * (N // parts), N // parts)], SEM["cost"] + level * 4 + q)
        cost = (mine_g[level] + near_g[level]) * (1.0 / math.sqrt(D))
        squared = cost * cost
        return squared * squared

    def onehot_of(perm_row):
        neuron = lax.broadcasted_iota(jnp.int32, (N, N), 0)
        return jnp.where(neuron == perm_row, 0.5, 0.0)

    def mixing_of(fourth, perm_row):
        scale = 0.5 / (1.0 + jnp.sum(fourth, axis=0, keepdims=True))
        mix[0] = (onehot_of(perm_row) + fourth * scale).T.astype(jnp.bfloat16)

    def rows2(q):
        return pl.ds(q * H, H)

    def mix_rows(at, rows, part, own, out):
        for t in range(F // N):
            tile = pl.ds(t * N, N)
            aligned = jnp.dot(mix[at, rows], part[:, tile], preferred_element_type=jnp.float32)
            out[rows, tile] = (
                (own[rows, tile].astype(jnp.float32) + aligned) * (1.0 / math.sqrt(2.0))).astype(jnp.bfloat16)

    def merge_with(fourth, perm_row, part, own, out, then=lambda q: None):
        mixing_of(fourth, perm_row)
        for first_piece, count in ((0, 1), (1, 1), (2, 2)):
            mix_rows(0, pl.ds(first_piece * Q, count * Q), part, own, out)
            for q in range(first_piece, first_piece + count):
                then(q)

    def merge(level, perm_row, part, own, out, then=lambda q: None):
        merge_with(fourth_of(level), perm_row, part, own, out, then)

    def perm_of(at, r):
        return perms[at, 0, r:r + 1]

    cost_part(0, 0, raw.at[0, 1], raw.at[0, 0], 1)
    merge(0, perm_of(0, 0), raw.at[0, 1], raw.at[0, 0], first.at[0])
    for s in range(2):
        arrived(raw.at[1, s, pl.ds(pl.multiple_of(my_rows, H), H)], SEM["z_raw"] + s)
    for q in range(8):
        rows = pl.ds(pl.multiple_of(far_rows + q * step, step), step)
        for e in range(2):
            for s in range(2):
                arrived(raw.at[1, s, rows, piece(e)], SEM["z_fwd"] + q * 4 + e * 2 + s)
    cost_part(1, 0, raw.at[1, 1], raw.at[1, 0], 1)
    merge(1, perm_of(1, 0), raw.at[1, 1], raw.at[1, 0], first.at[1])
    cost_part(2, 0, first.at[1], first.at[0], 1)

    def quad(k, at, r, own, slots, wait_rings, order, wait_opposite, tmp):
        level = 3 + k
        for q in range(4):
            wait_rings(q)
            cost_part(level, q, slots.at[0], own)
        onehot[...] = onehot_of(perm_of(at, r)).T
        merge(level, perm_of(0, r), slots.at[0], own, tmp.at[0])
        mine_e[k] = lax.dot_general(
            slots[2], tmp[0], (((1,), (1,)), ((), ())), preferred_element_type=jnp.float32)
        send(mine_e.at[k], near_e.at[k], SEM["seen"] + k, near)

        def sums(q):
            mine_p[k, rows4(q), pl.ds(0, N)] = lax.dot_general(
                slots[1, rows4(q)], slots[2], (((1,), (1,)), ((), ())), preferred_element_type=jnp.float32)
            mine_p[k, rows4(q), pl.ds(N, N)] = lax.dot_general(
                slots[1, rows4(q)], tmp[0], (((1,), (1,)), ((), ())), preferred_element_type=jnp.float32)
            send(mine_p.at[k, rows4(q)], near_p.at[k, rows4(q)], SEM["pair"] + 4 * k + q, near)

        def level_of(q):
            rows = rows4(q)
            arrived(near_p.at[k, rows], SEM["pair"] + 4 * k + q)
            cost = (mine_p[k, rows, pl.ds(0, N)] + near_p[k, rows, pl.ds(0, N)]) * (1.0 / math.sqrt(D))
            squared = cost * cost
            fourth = squared * squared
            mixing = (onehot[rows] + fourth * (0.5 / (1.0 + jnp.sum(fourth, axis=1, keepdims=True)))).astype(jnp.bfloat16)
            mix[1, rows] = mixing
            through = (jnp.dot(mixing, seen[0], preferred_element_type=jnp.float32)
                       + jnp.dot(mixing, seen[1], preferred_element_type=jnp.float32))
            direct = mine_p[k, rows, pl.ds(N, N)] + near_p[k, rows, pl.ds(N, N)]
            cost = (direct + through) * (1.0 / math.sqrt(2.0 * D))
            squared = cost * cost
            next_fourth[rows] = squared * squared
            mix_rows(1, rows, slots.at[2], slots.at[1], tmp.at[1])

        for e, q in enumerate(order):
            wait_opposite(q)
            sums(q)
            if e == 0:
                arrived(near_e.at[k], SEM["seen"] + k)
                both = mine_e[k] + near_e[k]
                seen[0] = both.astype(jnp.bfloat16)
                seen[1] = (both - seen[0].astype(jnp.float32)).astype(jnp.bfloat16)
            else:
                level_of(order[e - 1])
        level_of(order[-1])

    zq = got.at[pl.ds(0, 3)]

    def bit1(v):
        return (v // 2) % 2

    def send_z1(q):
        send(cur.at[0, rows4(q)], relay.at[0, rows4(q)], SEM["z1"] + q, z_next)
        send(cur.at[0, rows4(q)], relay.at[1, rows4(q)], SEM["z1"] + 4 + q, z_last)

    to_next, to_last = 2 * (1 - bit1((z + 1) % 8)), 2 * bit1((z + 7) % 8)
    from_last, from_next = 2 * (1 - bit1(z)), 2 * bit1(z)

    merge(2, perm_of(0, 1), first.at[1], first.at[0], cur.at[0], send_z1)
    for q in range(4):
        arrived(relay.at[0, rows4(q)], SEM["z1"] + q)
        send(relay.at[0, rows4(q)], zq.at[to_next, rows4(q)], SEM["z2"] + q, z_next)
        arrived(relay.at[1, rows4(q)], SEM["z1"] + 4 + q)
        send(relay.at[1, rows4(q)], zq.at[to_last, rows4(q)], SEM["z2"] + 4 + q, z_last)

    def rings_z(q):
        arrived(zq.at[from_last, rows4(q)], SEM["z2"] + q)
        if q < 2:
            send(zq.at[from_last, rows4(q)], relay_half.at[0, rows4(q)], SEM["z3"] + q, z_next)
        arrived(zq.at[from_next, rows4(q)], SEM["z2"] + 4 + q)
        if q >= 2:
            send(zq.at[from_next, rows4(q)], relay_half.at[1, rows4(q - 2)], SEM["z3"] + q, z_last)

    def opposite_z(q):
        if q == 0:
            for e in (0, 2, 1, 3):
                side, there = (0, z_next) if e < 2 else (1, z_last)
                arrived(relay_half.at[side, rows4(e % 2)], SEM["z3"] + e)
                send(relay_half.at[side, rows4(e % 2)], zq.at[1, rows4(e)], SEM["z4"] + e, there)
        arrived(zq.at[1, rows4(q)], SEM["z4"] + q)

    def send_x1(q):
        send(cur.at[1, rows4(q)], xq.at[2 * (x % 2), rows4(q)], SEM["x1"] + q, x_next)
        send(cur.at[1, rows4(q)], xq.at[2 * (1 - x % 2), rows4(q)], SEM["x1"] + 4 + q, x_last)

    xq = got.at[pl.ds(3, 3)]
    quad(0, 2, 2, cur.at[0], zq, rings_z, (0, 2, 1, 3), opposite_z, first.at[pl.ds(2, 2)])
    merge_with(next_fourth[...], perm_of(0, 3), first.at[3], first.at[2], cur.at[1], send_x1)

    def rings_x(q):
        arrived(xq.at[2 * (1 - x % 2), rows4(q)], SEM["x1"] + q)
        if q < 2:
            send(xq.at[2 * (1 - x % 2), rows4(q)], xq.at[1, rows4(q)], SEM["x2"] + q, x_next)
        arrived(xq.at[2 * (x % 2), rows4(q)], SEM["x1"] + 4 + q)
        if q >= 2:
            send(xq.at[2 * (x % 2), rows4(q)], xq.at[1, rows4(q)], SEM["x2"] + q, x_last)

    def opposite_x(q):
        arrived(xq.at[1, rows4(q)], SEM["x2"] + q)

    quad(1, 3, 4, cur.at[1], xq, rings_x, (0, 2, 1, 3), opposite_x, first.at[pl.ds(4, 2)])

    yq = got.at[pl.ds(6, 3)]
    o_cols = pl.ds(pl.multiple_of(g * F, F), F)

    @pl.when(inner == 0)
    def _():
        outer_sends = []
        def send_y1(q):
            copy = pltpu.make_async_remote_copy(
                src_ref=cur.at[2, rows4(q)], dst_ref=yq.at[0, rows4(q)], send_sem=ssem.at[SEM["y1"] + q],
                recv_sem=rsem.at[SEM["y1"] + q], device_id=same[Y0], device_id_type=MESH)
            copy.start()
            outer_sends.append(copy)

        merge_with(next_fourth[...], perm_of(0, 5), first.at[5], first.at[4], cur.at[2], send_y1)
        for c in range(2):
            arrived(o_ref.at[0, :, half(c)], SEM["out"] + c)
        for copy in outer_sends:
            copy.wait_send()

    @pl.when(inner == 1)
    def _():
        before = len(sent)

        def send_y2(q):
            send(cur.at[2, rows4(q)], yq.at[2, rows4(q)], SEM["y2"] + q, y_cross)

        merge_with(next_fourth[...], perm_of(0, 5), first.at[5], first.at[4], cur.at[2], send_y2)

        def rings_y(q):
            arrived(yq.at[0, rows4(q)], SEM["y1"] + q)
            send(yq.at[0, rows4(q)], yq.at[1, rows4(q)], SEM["y3"] + q, y_cross)
            arrived(yq.at[2, rows4(q)], SEM["y2"] + q)

        def opposite_y(q):
            arrived(yq.at[1, rows4(q)], SEM["y3"] + q)

        quad(2, 4, 6, cur.at[2], yq, rings_y, (0, 1, 2, 3), opposite_y, first.at[pl.ds(6, 2)])
        ours, theirs = first.at[6], first.at[7]

        def away(src, rows, at, device):
            copy = pltpu.make_async_remote_copy(
                src_ref=src.at[pl.ds(pl.multiple_of(rows, H), H)], dst_ref=o_ref.at[0, :, o_cols],
                send_sem=ssem.at[SEM["away"] + at], recv_sem=rsem.at[SEM["out"] + g],
                device_id=device, device_id_type=MESH)
            return copy

        fourth = next_fourth[...]
        mixing_of(fourth, perm_of(0, 7))
        far_half, my_half = pl.ds(pl.multiple_of(far_rows, H), H), pl.ds(pl.multiple_of(my_rows, H), H)
        ours_far = away(cur.at[3], far_rows, 0, (core(rep, h), far))
        theirs_far = away(cur.at[4], far_rows, 2, (core(chip[Y1], h), far))
        theirs_near = away(cur.at[4], my_rows, 1, (core(chip[Y1], h), h))
        ours_near = away(cur.at[3], my_rows, 3, near)
        mix_rows(0, far_half, theirs, ours, cur.at[3])
        ours_far.start()
        scale = 0.5 / (1.0 + jnp.sum(fourth, axis=1, keepdims=True))
        mix[1] = (onehot_of(perm_of(4, 7)).T + fourth * scale).astype(jnp.bfloat16)
        mix_rows(1, far_half, ours, theirs, cur.at[4])
        theirs_far.start()
        mix_rows(0, my_half, theirs, ours, cur.at[3])

        @pl.when(slot == 0)
        def _():
            home = pltpu.make_async_copy(cur.at[3, my_half], o_ref.at[0, :, o_cols], lsem.at[2])
            home.start()
            home.wait()

        @pl.when(slot == 1)
        def _():
            ours_near.start()

        mix_rows(1, my_half, ours, theirs, cur.at[4])
        ours_far.wait_send()
        theirs_far.wait_send()
        theirs_near.start()

        @pl.when(slot == 0)
        def _():
            arrived(o_ref.at[0, :, pl.ds(pl.multiple_of((1 - g) * F, F), F)], SEM["out"] + 1 - g)

        @pl.when(slot == 1)
        def _():
            for c in range(2):
                arrived(o_ref.at[0, :, half(c)], SEM["out"] + c)
            ours_near.wait_send()

        leaving = [theirs_near]
        for copy in leaving + sent[before:]:
            copy.wait_send()
        del sent[before:]

    for copy in sent:
        copy.wait_send()


def local(weights, perms):
    rows = (N, F)
    return pl.pallas_call(
        kernel,
        out_shape=pltpu.VMEM((1, H, D), jnp.bfloat16),
        in_specs=[pl.BlockSpec(memory_space=pl.ANY), pl.BlockSpec(memory_space=pl.ANY)],
        out_specs=pl.BlockSpec(memory_space=pl.ANY),
        scratch_shapes=[
            pltpu.VMEM((H, D), jnp.bfloat16),
            pltpu.VMEM((5, 2, 8, N), jnp.int32),
            pltpu.VMEM((2, 2, *rows), jnp.bfloat16),
            pltpu.VMEM((8, *rows), jnp.bfloat16),
            pltpu.VMEM((5, *rows), jnp.bfloat16),
            pltpu.VMEM((9, *rows), jnp.bfloat16),
            pltpu.VMEM((2, *rows), jnp.bfloat16),
            pltpu.VMEM((2, H, F), jnp.bfloat16),
            pltpu.VMEM((6, N, N), jnp.float32),
            pltpu.VMEM((6, N, N), jnp.float32),
            pltpu.VMEM((3, N, 2 * N), jnp.float32),
            pltpu.VMEM((3, N, 2 * N), jnp.float32),
            pltpu.VMEM((3, N, N), jnp.float32),
            pltpu.VMEM((3, N, N), jnp.float32),
            pltpu.VMEM((2, N, N), jnp.bfloat16),
            pltpu.VMEM((N, N), jnp.float32),
            pltpu.VMEM((N, N), jnp.float32),
            pltpu.VMEM((2, N, N), jnp.bfloat16),
            pltpu.SemaphoreType.DMA((N_SEM,)),
            pltpu.SemaphoreType.DMA((N_SEM,)),
            pltpu.SemaphoreType.DMA((4,)),
        ],
        compiler_params=pltpu.CompilerParams(
            collective_id=0, has_side_effects=True, vmem_limit_bytes=60 * 1024 * 1024),
    )(weights, perms)


def solution(mesh):
    placed = (P("rep", "slab", None), P("rep", None, None))
    return jax.shard_map(
        local, mesh=mesh, in_specs=placed, out_specs=P("rep", "slab", None), check_vma=False
    )
```

```python
import functools
import math

import jax
import jax.numpy as jnp
from jax import lax
from jax.experimental import pallas as pl
from jax.experimental.pallas import tpu as pltpu
from jax.sharding import PartitionSpec as P

D = 3072
N = 256
H = N // 2
F = D // 2
MESH = pl.DeviceIdType.MESH
NEAR, Z0, Z1, Z2, X0, X1, Y0, Y1 = range(8)


def layout(counts):
    at, out = 0, {}
    for name, count in counts:
        out[name] = at
        at += count
    return out, at


SEM, N_SEM = layout([
    ("near_raw", 1), ("in", 32), ("z_raw", 2), ("z_fwd", 32), ("perm", 10),
    ("z1", 8), ("z2", 8), ("z3", 4), ("z4", 4), ("x1", 8), ("x2", 4), ("y1", 4), ("y2", 4), ("y3", 4), ("out", 2), ("away", 4),
    ("cost", 6 * 4), ("pair", 3 * 4 + 2), ("seen", 3 + 2),
])


def kernel(w_hbm, p_hbm, o_ref, wv, perms, raw, first, cur, got, relay, relay_half, mine_g, near_g, mine_p, near_p, mine_e, near_e, seen, next_fourth, onehot, mix, ssem, rsem, lsem):
    rep, h = lax.axis_index("rep"), lax.axis_index("slab")
    g = rep % 2
    far = 1 - h

    def flip(bit):
        return rep + (1 << bit) * (1 - 2 * ((rep // (1 << bit)) % 2))

    def core(base, c):
        return base - g + c

    def xor(a, b):
        return a + b - 2 * a * b

    near = (flip(0), h)
    chip = [flip(b) for b in range(8)]
    same = [(chip[b], h) for b in range(8)]

    load = pltpu.make_async_copy(w_hbm.at[0], wv, lsem.at[0])
    load.start()
    slot = g + h - 2 * g * h
    load_perms = pltpu.make_async_copy(p_hbm.at[0], perms.at[0, slot], lsem.at[3])
    load_perms.start()

    z, x = (rep // 2) % 8, (rep // 16) % 4
    z_next, z_last = (rep + 2 * ((z + 1) % 8 - z), h), (rep + 2 * ((z + 7) % 8 - z), h)
    x_next, x_last = (rep + 16 * ((x + 1) % 4 - x), h), (rep + 16 * ((x + 3) % 4 - x), h)

    y = (rep // 64) % 4
    inner = ((y + 1) // 2) % 2
    y_cross = (rep + 64 * (3 - 2 * y), h)
    peers = [near, z_next, z_last, x_next, x_last, same[Y0], y_cross]
    for c in range(2):
        peers.append((core(rep, c), far))
        peers.append((core(chip[Y1], c), far))
        for b in (Z0, Z2, X1, Y1):
            peers.append((core(chip[b], c), h))
    barrier = pltpu.get_barrier_semaphore()
    for peer in peers:
        pl.semaphore_signal(barrier, inc=1, device_id=peer, device_id_type=MESH)
    pl.semaphore_wait(barrier, len(peers))

    sent = []

    def send(src, dst, sem, device):
        copy = pltpu.make_async_remote_copy(
            src_ref=src, dst_ref=dst, send_sem=ssem.at[sem], recv_sem=rsem.at[sem],
            device_id=device, device_id_type=MESH,
        )
        copy.start()
        sent.append(copy)

    def arrived(dst, sem):
        pltpu.make_async_remote_copy(
            src_ref=dst, dst_ref=dst, send_sem=ssem.at[0], recv_sem=rsem.at[sem],
            device_id=near, device_id_type=MESH,
        ).wait_recv()

    def half(c):
        return pl.ds(c * F, F)

    far_slot = xor(g, far)
    my_rows, far_rows = h * H, far * H
    step = H // 8

    load.wait()
    keep = pltpu.make_async_copy(
        wv.at[:, pl.ds(pl.multiple_of(g * F, F), F)],
        raw.at[0, slot, pl.ds(pl.multiple_of(my_rows, H), H)], lsem.at[1])
    keep.start()

    def piece(e):
        return pl.ds(e * (F // 2), F // 2)

    def send_in(q, e, c):
        src = wv.at[pl.ds(q * step, step), pl.ds(c * F + e * (F // 2), F // 2)]
        dst = raw.at[0, far_slot, pl.ds(pl.multiple_of(my_rows + q * step, step), step), piece(e)]
        copy = pltpu.make_async_remote_copy(
            src_ref=src, dst_ref=dst, send_sem=ssem.at[SEM["in"] + q * 4 + e * 2 + c],
            recv_sem=rsem.at[SEM["in"] + q * 4 + e * 2 + far_slot],
            device_id=(core(rep, c), far), device_id_type=MESH)
        copy.start()
        sent.append(copy)

    for q in range(8):
        for e in range(2):
            for c in range(2):
                send_in(q, e, c)
    for c in range(2):
        copy = pltpu.make_async_remote_copy(
            src_ref=wv.at[:, half(c)],
            dst_ref=raw.at[1, slot, pl.ds(pl.multiple_of(my_rows, H), H)],
            send_sem=ssem.at[SEM["z_raw"] + c], recv_sem=rsem.at[SEM["z_raw"] + slot],
            device_id=(core(chip[Z0], c), h), device_id_type=MESH)
        copy.start()
        sent.append(copy)
    send(wv.at[:, pl.ds(pl.multiple_of((1 - g) * F, F), F)],
         raw.at[0, slot, pl.ds(pl.multiple_of(my_rows, H), H)], SEM["near_raw"], near)

    load_perms.wait()
    perm_to = [(0, near, 0)]
    for at, b in ((1, Z0), (2, Z2), (3, X1), (4, Y1)):
        for c in range(2):
            perm_to.append((at, (core(chip[b], c), h), c))
    for at, device, c in perm_to:
        copy = pltpu.make_async_remote_copy(
            src_ref=perms.at[0, slot], dst_ref=perms.at[at, slot],
            send_sem=ssem.at[SEM["perm"] + at * 2 + c], recv_sem=rsem.at[SEM["perm"] + at * 2 + slot],
            device_id=device, device_id_type=MESH)
        copy.start()
        sent.append(copy)

    for q in range(8):
        rows = pl.ds(pl.multiple_of(far_rows + q * step, step), step)
        for e in range(2):
            for s in range(2):
                at = q * 4 + e * 2 + s
                arrived(raw.at[0, s, rows, piece(e)], SEM["in"] + at)
                send(raw.at[0, s, rows, piece(e)], raw.at[1, s, rows, piece(e)], SEM["z_fwd"] + at, same[Z0])

    keep.wait()
    arrived(raw.at[0, 1 - slot, pl.ds(pl.multiple_of(my_rows, H), H)], SEM["near_raw"])
    arrived(perms.at[0, 1 - slot], SEM["perm"] + (1 - slot))
    for at in range(1, 5):
        for s in range(2):
            arrived(perms.at[at, s], SEM["perm"] + at * 2 + s)

    Q = N // 4

    def rows4(q):
        return pl.ds(q * Q, Q)

    pieces = {}

    def cost_part(level, q, part, own, parts=4):
        pieces[level] = parts
        rows = pl.ds(q * (N // parts), N // parts)
        mine_g[level, rows] = lax.dot_general(
            part[rows], own[...], (((1,), (1,)), ((), ())), preferred_element_type=jnp.float32)
        send(mine_g.at[level, rows], near_g.at[level, rows], SEM["cost"] + level * 4 + q, near)

    def fourth_of(level):
        parts = pieces[level]
        for q in range(parts):
            arrived(near_g.at[level, pl.ds(q * (N // parts), N // parts)], SEM["cost"] + level * 4 + q)
        cost = (mine_g[level] + near_g[level]) * (1.0 / math.sqrt(D))
        squared = cost * cost
        return squared * squared

    def onehot_of(perm_row):
        neuron = lax.broadcasted_iota(jnp.int32, (N, N), 0)
        return jnp.where(neuron == perm_row, 0.5, 0.0)

    def mixing_of(fourth, perm_row):
        scale = 0.5 / (1.0 + jnp.sum(fourth, axis=0, keepdims=True))
        mix[0] = (onehot_of(perm_row) + fourth * scale).T.astype(jnp.bfloat16)

    def rows2(q):
        return pl.ds(q * H, H)

    def mix_rows(at, rows, part, own, out):
        for t in range(F // N):
            tile = pl.ds(t * N, N)
            aligned = jnp.dot(mix[at, rows], part[:, tile], preferred_element_type=jnp.float32)
            out[rows, tile] = (
                (own[rows, tile].astype(jnp.float32) + aligned) * (1.0 / math.sqrt(2.0))).astype(jnp.bfloat16)

    def merge_with(fourth, perm_row, part, own, out, then=None):
        mixing_of(fourth, perm_row)
        for first_piece, count in ((0, 1), (1, 1), (2, 2)) if then else ((0, 4),):
            mix_rows(0, pl.ds(first_piece * Q, count * Q), part, own, out)
            for q in range(first_piece, first_piece + count) if then else ():
                then(q)

    def merge(level, perm_row, part, own, out, then=None):
        merge_with(fourth_of(level), perm_row, part, own, out, then)

    def perm_of(at, r):
        return perms[at, 0, r:r + 1]

    def split_seen(k):
        both = mine_e[k] + near_e[k]
        seen[0] = both.astype(jnp.bfloat16)
        seen[1] = (both - seen[0].astype(jnp.float32)).astype(jnp.bfloat16)

    def level_rows(k, rows, sem, part, own, out):
        arrived(near_p.at[k, rows], sem)
        cost = (mine_p[k, rows, pl.ds(0, N)] + near_p[k, rows, pl.ds(0, N)]) * (1.0 / math.sqrt(D))
        squared = cost * cost
        fourth = squared * squared
        mixing = (onehot[rows] + fourth * (0.5 / (1.0 + jnp.sum(fourth, axis=1, keepdims=True)))).astype(jnp.bfloat16)
        mix[1, rows] = mixing
        through = (jnp.dot(mixing, seen[0], preferred_element_type=jnp.float32)
                   + jnp.dot(mixing, seen[1], preferred_element_type=jnp.float32))
        direct = mine_p[k, rows, pl.ds(N, N)] + near_p[k, rows, pl.ds(N, N)]
        cost = (direct + through) * (1.0 / math.sqrt(2.0 * D))
        squared = cost * cost
        next_fourth[rows] = squared * squared
        mix_rows(1, rows, part, own, out)

    def product(rows_of, columns_of):
        return lax.dot_general(
            rows_of, columns_of, (((1,), (1,)), ((), ())), preferred_element_type=jnp.float32)

    cost_part(0, 0, raw.at[0, 1], raw.at[0, 0], 1)
    merge(0, perm_of(0, 0), raw.at[0, 1], raw.at[0, 0], first.at[0])
    onehot[...] = onehot_of(perm_of(1, 0)).T
    halves = [pl.ds(pl.multiple_of(my_rows, H), H), pl.ds(pl.multiple_of(far_rows, H), H)]
    for e, rows in enumerate(halves):
        if e == 0:
            for s in range(2):
                arrived(raw.at[1, s, rows], SEM["z_raw"] + s)
        else:
            for q in range(8):
                at_rows = pl.ds(pl.multiple_of(far_rows + q * step, step), step)
                for c in range(2):
                    for s in range(2):
                        arrived(raw.at[1, s, at_rows, piece(c)], SEM["z_fwd"] + q * 4 + c * 2 + s)
        mine_e[3, rows] = product(raw[1, 1, rows], first[0])
        send(mine_e.at[3, rows], near_e.at[3, rows], SEM["seen"] + 3 + e, near)
        mine_p[3, rows, pl.ds(N, N)] = product(raw[1, 0, rows], first[0])
    for e, rows in enumerate(halves):
        mine_p[3, rows, pl.ds(0, N)] = product(raw[1, 0, rows], raw[1, 1])
        send(mine_p.at[3, rows], near_p.at[3, rows], SEM["pair"] + 12 + e, near)
    for e, rows in enumerate(halves):
        arrived(near_e.at[3, rows], SEM["seen"] + 3 + e)
    split_seen(3)
    for e, rows in enumerate(halves):
        level_rows(3, rows, SEM["pair"] + 12 + e, raw.at[1, 1], raw.at[1, 0], first.at[1])

    def quad(k, at, r, own, slots, wait_rings, order, wait_opposite, tmp):
        level = 3 + k
        for q in range(4):
            wait_rings(q)
            cost_part(level, q, slots.at[0], own)
        onehot[...] = onehot_of(perm_of(at, r)).T
        merge(level, perm_of(0, r), slots.at[0], own, tmp.at[0])
        mine_e[k] = lax.dot_general(
            slots[2], tmp[0], (((1,), (1,)), ((), ())), preferred_element_type=jnp.float32)
        send(mine_e.at[k], near_e.at[k], SEM["seen"] + k, near)

        def sums(q):
            mine_p[k, rows4(q), pl.ds(0, N)] = lax.dot_general(
                slots[1, rows4(q)], slots[2], (((1,), (1,)), ((), ())), preferred_element_type=jnp.float32)
            mine_p[k, rows4(q), pl.ds(N, N)] = lax.dot_general(
                slots[1, rows4(q)], tmp[0], (((1,), (1,)), ((), ())), preferred_element_type=jnp.float32)
            send(mine_p.at[k, rows4(q)], near_p.at[k, rows4(q)], SEM["pair"] + 4 * k + q, near)

        def level_of(q):
            level_rows(k, rows4(q), SEM["pair"] + 4 * k + q, slots.at[2], slots.at[1], tmp.at[1])

        for e, q in enumerate(order):
            wait_opposite(q)
            sums(q)
            if e == 0:
                arrived(near_e.at[k], SEM["seen"] + k)
                split_seen(k)
            else:
                level_of(order[e - 1])
        level_of(order[-1])

    zq = got.at[pl.ds(0, 3)]

    def bit1(v):
        return (v // 2) % 2

    def send_z1(q):
        send(cur.at[0, rows4(q)], relay.at[0, rows4(q)], SEM["z1"] + q, z_next)
        send(cur.at[0, rows4(q)], relay.at[1, rows4(q)], SEM["z1"] + 4 + q, z_last)

    to_next, to_last = 2 * (1 - bit1((z + 1) % 8)), 2 * bit1((z + 7) % 8)
    from_last, from_next = 2 * (1 - bit1(z)), 2 * bit1(z)

    merge_with(next_fourth[...], perm_of(0, 1), first.at[1], first.at[0], cur.at[0], send_z1)
    for q in range(4):
        arrived(relay.at[0, rows4(q)], SEM["z1"] + q)
        send(relay.at[0, rows4(q)], zq.at[to_next, rows4(q)], SEM["z2"] + q, z_next)
        arrived(relay.at[1, rows4(q)], SEM["z1"] + 4 + q)
        send(relay.at[1, rows4(q)], zq.at[to_last, rows4(q)], SEM["z2"] + 4 + q, z_last)

    def rings_z(q):
        arrived(zq.at[from_last, rows4(q)], SEM["z2"] + q)
        if q < 2:
            send(zq.at[from_last, rows4(q)], relay_half.at[0, rows4(q)], SEM["z3"] + q, z_next)
        arrived(zq.at[from_next, rows4(q)], SEM["z2"] + 4 + q)
        if q >= 2:
            send(zq.at[from_next, rows4(q)], relay_half.at[1, rows4(q - 2)], SEM["z3"] + q, z_last)

    def opposite_z(q):
        if q == 0:
            for e in (0, 2, 1, 3):
                side, there = (0, z_next) if e < 2 else (1, z_last)
                arrived(relay_half.at[side, rows4(e % 2)], SEM["z3"] + e)
                send(relay_half.at[side, rows4(e % 2)], zq.at[1, rows4(e)], SEM["z4"] + e, there)
        arrived(zq.at[1, rows4(q)], SEM["z4"] + q)

    def send_x1(q):
        send(cur.at[1, rows4(q)], xq.at[2 * (x % 2), rows4(q)], SEM["x1"] + q, x_next)
        send(cur.at[1, rows4(q)], xq.at[2 * (1 - x % 2), rows4(q)], SEM["x1"] + 4 + q, x_last)

    xq = got.at[pl.ds(3, 3)]
    quad(0, 2, 2, cur.at[0], zq, rings_z, (0, 2, 1, 3), opposite_z, first.at[pl.ds(2, 2)])
    merge_with(next_fourth[...], perm_of(0, 3), first.at[3], first.at[2], cur.at[1], send_x1)

    def rings_x(q):
        arrived(xq.at[2 * (1 - x % 2), rows4(q)], SEM["x1"] + q)
        if q < 2:
            send(xq.at[2 * (1 - x % 2), rows4(q)], xq.at[1, rows4(q)], SEM["x2"] + q, x_next)
        arrived(xq.at[2 * (x % 2), rows4(q)], SEM["x1"] + 4 + q)
        if q >= 2:
            send(xq.at[2 * (x % 2), rows4(q)], xq.at[1, rows4(q)], SEM["x2"] + q, x_last)

    def opposite_x(q):
        arrived(xq.at[1, rows4(q)], SEM["x2"] + q)

    quad(1, 3, 4, cur.at[1], xq, rings_x, (0, 2, 1, 3), opposite_x, first.at[pl.ds(4, 2)])

    yq = got.at[pl.ds(6, 3)]
    o_cols = pl.ds(pl.multiple_of(g * F, F), F)

    @pl.when(inner == 0)
    def _():
        outer_sends = []
        def send_y1(q):
            copy = pltpu.make_async_remote_copy(
                src_ref=cur.at[2, rows4(q)], dst_ref=yq.at[0, rows4(q)], send_sem=ssem.at[SEM["y1"] + q],
                recv_sem=rsem.at[SEM["y1"] + q], device_id=same[Y0], device_id_type=MESH)
            copy.start()
            outer_sends.append(copy)

        merge_with(next_fourth[...], perm_of(0, 5), first.at[5], first.at[4], cur.at[2], send_y1)
        for c in range(2):
            arrived(o_ref.at[0, :, half(c)], SEM["out"] + c)
        for copy in outer_sends:
            copy.wait_send()

    @pl.when(inner == 1)
    def _():
        before = len(sent)

        def send_y2(q):
            send(cur.at[2, rows4(q)], yq.at[2, rows4(q)], SEM["y2"] + q, y_cross)

        merge_with(next_fourth[...], perm_of(0, 5), first.at[5], first.at[4], cur.at[2], send_y2)

        def rings_y(q):
            arrived(yq.at[0, rows4(q)], SEM["y1"] + q)
            send(yq.at[0, rows4(q)], yq.at[1, rows4(q)], SEM["y3"] + q, y_cross)
            arrived(yq.at[2, rows4(q)], SEM["y2"] + q)

        def opposite_y(q):
            arrived(yq.at[1, rows4(q)], SEM["y3"] + q)

        quad(2, 4, 6, cur.at[2], yq, rings_y, (0, 1, 2, 3), opposite_y, first.at[pl.ds(6, 2)])
        ours, theirs = first.at[6], first.at[7]

        def away(src, rows, at, device):
            copy = pltpu.make_async_remote_copy(
                src_ref=src.at[pl.ds(pl.multiple_of(rows, H), H)], dst_ref=o_ref.at[0, :, o_cols],
                send_sem=ssem.at[SEM["away"] + at], recv_sem=rsem.at[SEM["out"] + g],
                device_id=device, device_id_type=MESH)
            return copy

        fourth = next_fourth[...]
        mixing_of(fourth, perm_of(0, 7))
        far_half, my_half = pl.ds(pl.multiple_of(far_rows, H), H), pl.ds(pl.multiple_of(my_rows, H), H)
        ours_far = away(cur.at[3], far_rows, 0, (core(rep, h), far))
        theirs_far = away(cur.at[4], far_rows, 2, (core(chip[Y1], h), far))
        theirs_near = away(cur.at[4], my_rows, 1, (core(chip[Y1], h), h))
        ours_near = away(cur.at[3], my_rows, 3, near)
        mix_rows(0, far_half, theirs, ours, cur.at[3])
        ours_far.start()
        scale = 0.5 / (1.0 + jnp.sum(fourth, axis=1, keepdims=True))
        mix[1] = (onehot_of(perm_of(4, 7)).T + fourth * scale).astype(jnp.bfloat16)
        mix_rows(1, far_half, ours, theirs, cur.at[4])
        theirs_far.start()
        mix_rows(0, my_half, theirs, ours, cur.at[3])

        @pl.when(slot == 0)
        def _():
            home = pltpu.make_async_copy(cur.at[3, my_half], o_ref.at[0, :, o_cols], lsem.at[2])
            home.start()
            home.wait()

        @pl.when(slot == 1)
        def _():
            ours_near.start()

        mix_rows(1, my_half, ours, theirs, cur.at[4])
        ours_far.wait_send()
        theirs_far.wait_send()
        theirs_near.start()

        @pl.when(slot == 0)
        def _():
            arrived(o_ref.at[0, :, pl.ds(pl.multiple_of((1 - g) * F, F), F)], SEM["out"] + 1 - g)

        @pl.when(slot == 1)
        def _():
            for c in range(2):
                arrived(o_ref.at[0, :, half(c)], SEM["out"] + c)
            ours_near.wait_send()

        leaving = [theirs_near]
        for copy in leaving + sent[before:]:
            copy.wait_send()
        del sent[before:]

    for copy in sent:
        copy.wait_send()


def local(weights, perms):
    rows = (N, F)
    return pl.pallas_call(
        kernel,
        out_shape=pltpu.VMEM((1, H, D), jnp.bfloat16),
        in_specs=[pl.BlockSpec(memory_space=pl.ANY), pl.BlockSpec(memory_space=pl.ANY)],
        out_specs=pl.BlockSpec(memory_space=pl.ANY),
        scratch_shapes=[
            pltpu.VMEM((H, D), jnp.bfloat16),
            pltpu.VMEM((5, 2, 8, N), jnp.int32),
            pltpu.VMEM((2, 2, *rows), jnp.bfloat16),
            pltpu.VMEM((8, *rows), jnp.bfloat16),
            pltpu.VMEM((5, *rows), jnp.bfloat16),
            pltpu.VMEM((9, *rows), jnp.bfloat16),
            pltpu.VMEM((2, *rows), jnp.bfloat16),
            pltpu.VMEM((2, H, F), jnp.bfloat16),
            pltpu.VMEM((6, N, N), jnp.float32),
            pltpu.VMEM((6, N, N), jnp.float32),
            pltpu.VMEM((4, N, 2 * N), jnp.float32),
            pltpu.VMEM((4, N, 2 * N), jnp.float32),
            pltpu.VMEM((4, N, N), jnp.float32),
            pltpu.VMEM((4, N, N), jnp.float32),
            pltpu.VMEM((2, N, N), jnp.bfloat16),
            pltpu.VMEM((N, N), jnp.float32),
            pltpu.VMEM((N, N), jnp.float32),
            pltpu.VMEM((2, N, N), jnp.bfloat16),
            pltpu.SemaphoreType.DMA((N_SEM,)),
            pltpu.SemaphoreType.DMA((N_SEM,)),
            pltpu.SemaphoreType.DMA((4,)),
        ],
        compiler_params=pltpu.CompilerParams(
            collective_id=0, has_side_effects=True, vmem_limit_bytes=60 * 1024 * 1024),
    )(weights, perms)


def solution(mesh):
    placed = (P("rep", "slab", None), P("rep", None, None))
    return jax.shard_map(
        local, mesh=mesh, in_specs=placed, out_specs=P("rep", "slab", None), check_vma=False
    )
```

```python
import functools
import math

import jax
import jax.numpy as jnp
from jax import lax
from jax.experimental import pallas as pl
from jax.experimental.pallas import tpu as pltpu
from jax.sharding import PartitionSpec as P

D = 3072
N = 256
H = N // 2
F = D // 2
MESH = pl.DeviceIdType.MESH
NEAR, Z0, Z1, Z2, X0, X1, Y0, Y1 = range(8)


def layout(counts):
    at, out = 0, {}
    for name, count in counts:
        out[name] = at
        at += count
    return out, at


SEM, N_SEM = layout([
    ("near_raw", 1), ("in", 32), ("z_raw", 2), ("z_fwd", 32), ("perm", 10),
    ("z1", 8), ("z2", 8), ("z3", 4), ("z4", 4), ("x1", 8), ("x2", 4), ("y1", 4), ("y2", 4), ("y3", 4), ("out", 2), ("away", 4),
    ("cost", 6 * 4), ("pair", 3 * 4), ("seen", 3),
])


def kernel(w_hbm, p_hbm, o_ref, wv, perms, raw, first, cur, got, relay, relay_half, mine_g, near_g, mine_p, near_p, mine_e, near_e, seen, next_fourth, onehot, mix, ssem, rsem, lsem):
    rep, h = lax.axis_index("rep"), lax.axis_index("slab")
    g = rep % 2
    far = 1 - h

    def flip(bit):
        return rep + (1 << bit) * (1 - 2 * ((rep // (1 << bit)) % 2))

    def core(base, c):
        return base - g + c

    def xor(a, b):
        return a + b - 2 * a * b

    near = (flip(0), h)
    chip = [flip(b) for b in range(8)]
    same = [(chip[b], h) for b in range(8)]

    load = pltpu.make_async_copy(w_hbm.at[0], wv, lsem.at[0])
    load.start()
    slot = g + h - 2 * g * h
    load_perms = pltpu.make_async_copy(p_hbm.at[0], perms.at[0, slot], lsem.at[3])
    load_perms.start()

    z, x = (rep // 2) % 8, (rep // 16) % 4
    z_next, z_last = (rep + 2 * ((z + 1) % 8 - z), h), (rep + 2 * ((z + 7) % 8 - z), h)
    x_next, x_last = (rep + 16 * ((x + 1) % 4 - x), h), (rep + 16 * ((x + 3) % 4 - x), h)

    y = (rep // 64) % 4
    inner = ((y + 1) // 2) % 2
    y_cross = (rep + 64 * (3 - 2 * y), h)
    peers = [(core(rep, c), far) for c in range(2)]
    for b in (Z2, X1, Y1, Z0):
        for c in range(2):
            peers.append((core(chip[b], c), h))
    peers += [(core(chip[Y1], c), far) for c in range(2)]
    peers += [z_next, z_last, x_next, x_last, same[Y0], y_cross, near]
    barrier = pltpu.get_barrier_semaphore()
    for peer in peers:
        pl.semaphore_signal(barrier, inc=1, device_id=peer, device_id_type=MESH)
    pl.semaphore_wait(barrier, len(peers))

    sent = []

    def send(src, dst, sem, device):
        copy = pltpu.make_async_remote_copy(
            src_ref=src, dst_ref=dst, send_sem=ssem.at[sem], recv_sem=rsem.at[sem],
            device_id=device, device_id_type=MESH,
        )
        copy.start()
        sent.append(copy)

    def arrived(dst, sem):
        pltpu.make_async_remote_copy(
            src_ref=dst, dst_ref=dst, send_sem=ssem.at[0], recv_sem=rsem.at[sem],
            device_id=near, device_id_type=MESH,
        ).wait_recv()

    def half(c):
        return pl.ds(c * F, F)

    far_slot = xor(g, far)
    my_rows, far_rows = h * H, far * H
    step = H // 8

    load.wait()
    keep = pltpu.make_async_copy(
        wv.at[:, pl.ds(pl.multiple_of(g * F, F), F)],
        raw.at[0, slot, pl.ds(pl.multiple_of(my_rows, H), H)], lsem.at[1])
    keep.start()

    def piece(e):
        return pl.ds(e * (F // 2), F // 2)

    def send_in(q, e, c):
        src = wv.at[pl.ds(q * step, step), pl.ds(c * F + e * (F // 2), F // 2)]
        dst = raw.at[0, far_slot, pl.ds(pl.multiple_of(my_rows + q * step, step), step), piece(e)]
        copy = pltpu.make_async_remote_copy(
            src_ref=src, dst_ref=dst, send_sem=ssem.at[SEM["in"] + q * 4 + e * 2 + c],
            recv_sem=rsem.at[SEM["in"] + q * 4 + e * 2 + far_slot],
            device_id=(core(rep, c), far), device_id_type=MESH)
        copy.start()
        sent.append(copy)

    for q in range(8):
        for e in range(2):
            for c in range(2):
                send_in(q, e, c)
    for c in range(2):
        copy = pltpu.make_async_remote_copy(
            src_ref=wv.at[:, half(c)],
            dst_ref=raw.at[1, slot, pl.ds(pl.multiple_of(my_rows, H), H)],
            send_sem=ssem.at[SEM["z_raw"] + c], recv_sem=rsem.at[SEM["z_raw"] + slot],
            device_id=(core(chip[Z0], c), h), device_id_type=MESH)
        copy.start()
        sent.append(copy)
    send(wv.at[:, pl.ds(pl.multiple_of((1 - g) * F, F), F)],
         raw.at[0, slot, pl.ds(pl.multiple_of(my_rows, H), H)], SEM["near_raw"], near)

    load_perms.wait()
    perm_to = [(0, near, 0)]
    for at, b in ((1, Z0), (2, Z2), (3, X1), (4, Y1)):
        for c in range(2):
            perm_to.append((at, (core(chip[b], c), h), c))
    for at, device, c in perm_to:
        copy = pltpu.make_async_remote_copy(
            src_ref=perms.at[0, slot], dst_ref=perms.at[at, slot],
            send_sem=ssem.at[SEM["perm"] + at * 2 + c], recv_sem=rsem.at[SEM["perm"] + at * 2 + slot],
            device_id=device, device_id_type=MESH)
        copy.start()
        sent.append(copy)

    for q in range(8):
        rows = pl.ds(pl.multiple_of(far_rows + q * step, step), step)
        for e in range(2):
            for s in range(2):
                at = q * 4 + e * 2 + s
                arrived(raw.at[0, s, rows, piece(e)], SEM["in"] + at)
                send(raw.at[0, s, rows, piece(e)], raw.at[1, s, rows, piece(e)], SEM["z_fwd"] + at, same[Z0])

    keep.wait()
    arrived(raw.at[0, 1 - slot, pl.ds(pl.multiple_of(my_rows, H), H)], SEM["near_raw"])
    arrived(perms.at[0, 1 - slot], SEM["perm"] + (1 - slot))
    for at in range(1, 5):
        for s in range(2):
            arrived(perms.at[at, s], SEM["perm"] + at * 2 + s)

    Q = N // 4

    def rows4(q):
        return pl.ds(q * Q, Q)

    pieces = {}

    def cost_part(level, q, part, own, parts=4):
        pieces[level] = parts
        rows = pl.ds(q * (N // parts), N // parts)
        mine_g[level, rows] = lax.dot_general(
            part[rows], own[...], (((1,), (1,)), ((), ())), preferred_element_type=jnp.float32)
        send(mine_g.at[level, rows], near_g.at[level, rows], SEM["cost"] + level * 4 + q, near)

    def fourth_of(level):
        parts = pieces[level]
        for q in range(parts):
            arrived(near_g.at[level, pl.ds(q * (N // parts), N // parts)], SEM["cost"] + level * 4 + q)
        cost = (mine_g[level] + near_g[level]) * (1.0 / math.sqrt(D))
        squared = cost * cost
        return squared * squared

    def onehot_of(perm_row):
        neuron = lax.broadcasted_iota(jnp.int32, (N, N), 0)
        return jnp.where(neuron == perm_row, 0.5, 0.0)

    def mixing_of(fourth, perm_row):
        scale = 0.5 / (1.0 + jnp.sum(fourth, axis=0, keepdims=True))
        mix[0] = (onehot_of(perm_row) + fourth * scale).T.astype(jnp.bfloat16)

    def rows2(q):
        return pl.ds(q * H, H)

    def mix_rows(at, rows, part, own, out):
        for t in range(F // N):
            tile = pl.ds(t * N, N)
            aligned = jnp.dot(mix[at, rows], part[:, tile], preferred_element_type=jnp.float32)
            out[rows, tile] = (
                (own[rows, tile].astype(jnp.float32) + aligned) * (1.0 / math.sqrt(2.0))).astype(jnp.bfloat16)

    def merge_with(fourth, perm_row, part, own, out, then=None):
        mixing_of(fourth, perm_row)
        for first_piece, count in ((0, 1), (1, 1), (2, 2)) if then else ((0, 4),):
            mix_rows(0, pl.ds(first_piece * Q, count * Q), part, own, out)
            for q in range(first_piece, first_piece + count) if then else ():
                then(q)

    def merge(level, perm_row, part, own, out, then=None):
        merge_with(fourth_of(level), perm_row, part, own, out, then)

    def perm_of(at, r):
        return perms[at, 0, r:r + 1]

    cost_part(0, 0, raw.at[0, 1], raw.at[0, 0], 1)
    merge(0, perm_of(0, 0), raw.at[0, 1], raw.at[0, 0], first.at[0])
    for s in range(2):
        arrived(raw.at[1, s, pl.ds(pl.multiple_of(my_rows, H), H)], SEM["z_raw"] + s)
    for q in range(8):
        rows = pl.ds(pl.multiple_of(far_rows + q * step, step), step)
        for e in range(2):
            for s in range(2):
                arrived(raw.at[1, s, rows, piece(e)], SEM["z_fwd"] + q * 4 + e * 2 + s)
    cost_part(1, 0, raw.at[1, 1], raw.at[1, 0], 1)
    merge(1, perm_of(1, 0), raw.at[1, 1], raw.at[1, 0], first.at[1])
    cost_part(2, 0, first.at[1], first.at[0], 1)

    def quad(k, at, r, own, slots, wait_rings, order, wait_opposite, tmp):
        level = 3 + k
        for q in range(4):
            wait_rings(q)
            cost_part(level, q, slots.at[0], own)
        onehot[...] = onehot_of(perm_of(at, r)).T
        merge(level, perm_of(0, r), slots.at[0], own, tmp.at[0])
        mine_e[k] = lax.dot_general(
            slots[2], tmp[0], (((1,), (1,)), ((), ())), preferred_element_type=jnp.float32)
        send(mine_e.at[k], near_e.at[k], SEM["seen"] + k, near)

        def sums(q):
            mine_p[k, rows4(q), pl.ds(0, N)] = lax.dot_general(
                slots[1, rows4(q)], slots[2], (((1,), (1,)), ((), ())), preferred_element_type=jnp.float32)
            mine_p[k, rows4(q), pl.ds(N, N)] = lax.dot_general(
                slots[1, rows4(q)], tmp[0], (((1,), (1,)), ((), ())), preferred_element_type=jnp.float32)
            send(mine_p.at[k, rows4(q)], near_p.at[k, rows4(q)], SEM["pair"] + 4 * k + q, near)

        def level_of(q):
            rows = rows4(q)
            arrived(near_p.at[k, rows], SEM["pair"] + 4 * k + q)
            cost = (mine_p[k, rows, pl.ds(0, N)] + near_p[k, rows, pl.ds(0, N)]) * (1.0 / math.sqrt(D))
            squared = cost * cost
            fourth = squared * squared
            mixing = (onehot[rows] + fourth * (0.5 / (1.0 + jnp.sum(fourth, axis=1, keepdims=True)))).astype(jnp.bfloat16)
            mix[1, rows] = mixing
            through = (jnp.dot(mixing, seen[0], preferred_element_type=jnp.float32)
                       + jnp.dot(mixing, seen[1], preferred_element_type=jnp.float32))
            direct = mine_p[k, rows, pl.ds(N, N)] + near_p[k, rows, pl.ds(N, N)]
            cost = (direct + through) * (1.0 / math.sqrt(2.0 * D))
            squared = cost * cost
            next_fourth[rows] = squared * squared
            mix_rows(1, rows, slots.at[2], slots.at[1], tmp.at[1])

        for e, q in enumerate(order):
            wait_opposite(q)
            sums(q)
            if e == 0:
                arrived(near_e.at[k], SEM["seen"] + k)
                both = mine_e[k] + near_e[k]
                seen[0] = both.astype(jnp.bfloat16)
                seen[1] = (both - seen[0].astype(jnp.float32)).astype(jnp.bfloat16)
            else:
                level_of(order[e - 1])
        level_of(order[-1])

    zq = got.at[pl.ds(0, 3)]

    def bit1(v):
        return (v // 2) % 2

    def send_z1(q):
        send(cur.at[0, rows4(q)], relay.at[0, rows4(q)], SEM["z1"] + q, z_next)
        send(cur.at[0, rows4(q)], relay.at[1, rows4(q)], SEM["z1"] + 4 + q, z_last)

    to_next, to_last = 2 * (1 - bit1((z + 1) % 8)), 2 * bit1((z + 7) % 8)
    from_last, from_next = 2 * (1 - bit1(z)), 2 * bit1(z)

    merge(2, perm_of(0, 1), first.at[1], first.at[0], cur.at[0], send_z1)
    for q in range(4):
        arrived(relay.at[0, rows4(q)], SEM["z1"] + q)
        send(relay.at[0, rows4(q)], zq.at[to_next, rows4(q)], SEM["z2"] + q, z_next)
        arrived(relay.at[1, rows4(q)], SEM["z1"] + 4 + q)
        send(relay.at[1, rows4(q)], zq.at[to_last, rows4(q)], SEM["z2"] + 4 + q, z_last)

    def rings_z(q):
        arrived(zq.at[from_last, rows4(q)], SEM["z2"] + q)
        if q < 2:
            send(zq.at[from_last, rows4(q)], relay_half.at[0, rows4(q)], SEM["z3"] + q, z_next)
        arrived(zq.at[from_next, rows4(q)], SEM["z2"] + 4 + q)
        if q >= 2:
            send(zq.at[from_next, rows4(q)], relay_half.at[1, rows4(q - 2)], SEM["z3"] + q, z_last)

    def opposite_z(q):
        if q == 0:
            for e in (0, 2, 1, 3):
                side, there = (0, z_next) if e < 2 else (1, z_last)
                arrived(relay_half.at[side, rows4(e % 2)], SEM["z3"] + e)
                send(relay_half.at[side, rows4(e % 2)], zq.at[1, rows4(e)], SEM["z4"] + e, there)
        arrived(zq.at[1, rows4(q)], SEM["z4"] + q)

    def send_x1(q):
        send(cur.at[1, rows4(q)], xq.at[2 * (x % 2), rows4(q)], SEM["x1"] + q, x_next)
        send(cur.at[1, rows4(q)], xq.at[2 * (1 - x % 2), rows4(q)], SEM["x1"] + 4 + q, x_last)

    xq = got.at[pl.ds(3, 3)]
    quad(0, 2, 2, cur.at[0], zq, rings_z, (0, 2, 1, 3), opposite_z, first.at[pl.ds(2, 2)])
    merge_with(next_fourth[...], perm_of(0, 3), first.at[3], first.at[2], cur.at[1], send_x1)

    def rings_x(q):
        arrived(xq.at[2 * (1 - x % 2), rows4(q)], SEM["x1"] + q)
        if q < 2:
            send(xq.at[2 * (1 - x % 2), rows4(q)], xq.at[1, rows4(q)], SEM["x2"] + q, x_next)
        arrived(xq.at[2 * (x % 2), rows4(q)], SEM["x1"] + 4 + q)
        if q >= 2:
            send(xq.at[2 * (x % 2), rows4(q)], xq.at[1, rows4(q)], SEM["x2"] + q, x_last)

    def opposite_x(q):
        arrived(xq.at[1, rows4(q)], SEM["x2"] + q)

    quad(1, 3, 4, cur.at[1], xq, rings_x, (0, 2, 1, 3), opposite_x, first.at[pl.ds(4, 2)])

    yq = got.at[pl.ds(6, 3)]
    o_cols = pl.ds(pl.multiple_of(g * F, F), F)

    @pl.when(inner == 0)
    def _():
        outer_sends = []
        def send_y1(q):
            copy = pltpu.make_async_remote_copy(
                src_ref=cur.at[2, rows4(q)], dst_ref=yq.at[0, rows4(q)], send_sem=ssem.at[SEM["y1"] + q],
                recv_sem=rsem.at[SEM["y1"] + q], device_id=same[Y0], device_id_type=MESH)
            copy.start()
            outer_sends.append(copy)

        merge_with(next_fourth[...], perm_of(0, 5), first.at[5], first.at[4], cur.at[2], send_y1)
        for c in range(2):
            arrived(o_ref.at[0, :, half(c)], SEM["out"] + c)
        for copy in outer_sends:
            copy.wait_send()

    @pl.when(inner == 1)
    def _():
        before = len(sent)

        def send_y2(q):
            send(cur.at[2, rows4(q)], yq.at[2, rows4(q)], SEM["y2"] + q, y_cross)

        merge_with(next_fourth[...], perm_of(0, 5), first.at[5], first.at[4], cur.at[2], send_y2)

        def rings_y(q):
            arrived(yq.at[0, rows4(q)], SEM["y1"] + q)
            send(yq.at[0, rows4(q)], yq.at[1, rows4(q)], SEM["y3"] + q, y_cross)
            arrived(yq.at[2, rows4(q)], SEM["y2"] + q)

        def opposite_y(q):
            arrived(yq.at[1, rows4(q)], SEM["y3"] + q)

        quad(2, 4, 6, cur.at[2], yq, rings_y, (0, 1, 2, 3), opposite_y, first.at[pl.ds(6, 2)])
        ours, theirs = first.at[6], first.at[7]

        def away(src, rows, at, device):
            copy = pltpu.make_async_remote_copy(
                src_ref=src.at[pl.ds(pl.multiple_of(rows, H), H)], dst_ref=o_ref.at[0, :, o_cols],
                send_sem=ssem.at[SEM["away"] + at], recv_sem=rsem.at[SEM["out"] + g],
                device_id=device, device_id_type=MESH)
            return copy

        fourth = next_fourth[...]
        mixing_of(fourth, perm_of(0, 7))
        far_half, my_half = pl.ds(pl.multiple_of(far_rows, H), H), pl.ds(pl.multiple_of(my_rows, H), H)
        ours_far = away(cur.at[3], far_rows, 0, (core(rep, h), far))
        theirs_far = away(cur.at[4], far_rows, 2, (core(chip[Y1], h), far))
        theirs_near = away(cur.at[4], my_rows, 1, (core(chip[Y1], h), h))
        ours_near = away(cur.at[3], my_rows, 3, near)
        mix_rows(0, far_half, theirs, ours, cur.at[3])
        ours_far.start()
        scale = 0.5 / (1.0 + jnp.sum(fourth, axis=1, keepdims=True))
        mix[1] = (onehot_of(perm_of(4, 7)).T + fourth * scale).astype(jnp.bfloat16)
        mix_rows(1, far_half, ours, theirs, cur.at[4])
        theirs_far.start()
        mix_rows(0, my_half, theirs, ours, cur.at[3])

        @pl.when(slot == 0)
        def _():
            home = pltpu.make_async_copy(cur.at[3, my_half], o_ref.at[0, :, o_cols], lsem.at[2])
            home.start()
            home.wait()

        @pl.when(slot == 1)
        def _():
            ours_near.start()

        mix_rows(1, my_half, ours, theirs, cur.at[4])
        ours_far.wait_send()
        theirs_far.wait_send()
        theirs_near.start()

        @pl.when(slot == 0)
        def _():
            arrived(o_ref.at[0, :, pl.ds(pl.multiple_of((1 - g) * F, F), F)], SEM["out"] + 1 - g)

        @pl.when(slot == 1)
        def _():
            for c in range(2):
                arrived(o_ref.at[0, :, half(c)], SEM["out"] + c)
            ours_near.wait_send()

        leaving = [theirs_near]
        for copy in leaving + sent[before:]:
            copy.wait_send()
        del sent[before:]

    for copy in sent:
        copy.wait_send()


def local(weights, perms):
    rows = (N, F)
    return pl.pallas_call(
        kernel,
        out_shape=pltpu.VMEM((1, H, D), jnp.bfloat16),
        in_specs=[pl.BlockSpec(memory_space=pl.ANY), pl.BlockSpec(memory_space=pl.ANY)],
        out_specs=pl.BlockSpec(memory_space=pl.ANY),
        scratch_shapes=[
            pltpu.VMEM((H, D), jnp.bfloat16),
            pltpu.VMEM((5, 2, 8, N), jnp.int32),
            pltpu.VMEM((2, 2, *rows), jnp.bfloat16),
            pltpu.VMEM((8, *rows), jnp.bfloat16),
            pltpu.VMEM((5, *rows), jnp.bfloat16),
            pltpu.VMEM((9, *rows), jnp.bfloat16),
            pltpu.VMEM((2, *rows), jnp.bfloat16),
            pltpu.VMEM((2, H, F), jnp.bfloat16),
            pltpu.VMEM((6, N, N), jnp.float32),
            pltpu.VMEM((6, N, N), jnp.float32),
            pltpu.VMEM((3, N, 2 * N), jnp.float32),
            pltpu.VMEM((3, N, 2 * N), jnp.float32),
            pltpu.VMEM((3, N, N), jnp.float32),
            pltpu.VMEM((3, N, N), jnp.float32),
            pltpu.VMEM((2, N, N), jnp.bfloat16),
            pltpu.VMEM((N, N), jnp.float32),
            pltpu.VMEM((N, N), jnp.float32),
            pltpu.VMEM((2, N, N), jnp.bfloat16),
            pltpu.SemaphoreType.DMA((N_SEM,)),
            pltpu.SemaphoreType.DMA((N_SEM,)),
            pltpu.SemaphoreType.DMA((4,)),
        ],
        compiler_params=pltpu.CompilerParams(
            collective_id=0, has_side_effects=True, vmem_limit_bytes=60 * 1024 * 1024),
    )(weights, perms)


def solution(mesh):
    placed = (P("rep", "slab", None), P("rep", None, None))
    return jax.shard_map(
        local, mesh=mesh, in_specs=placed, out_specs=P("rep", "slab", None), check_vma=False
    )
```
